32 devices in a mesh: gx: 4 (over y, core), gy: 2 (over x), gz: 4 (over z).
Axes of the slice: x: 2, y: 2, z: 4, core: 2. Of those that a mesh axis runs over, the one named last changes fastest.
Arguments:
- density: float32 [32, 32, 512], P('gx', 'gy', 'gz'), may hold values from 0.7 to 1.6
- momentum: float32 [32, 32, 512], P('gx', 'gy', 'gz'), may hold values from -7 to 7
- hydrogen: float32 [32, 32, 512], P('gx', 'gy', 'gz'), may hold values from 0.05 to 1.2
- forced_modes: int32 [96, 3], replicated, may hold values from -3 to 3, as said below
Outputs:
- density_rate: float32 [32, 32, 512], P('gx', 'gy', 'gz')
- momentum_rate: float32 [32, 32, 512], P('gx', 'gy', 'gz')
- hydrogen_rate: float32 [32, 32, 512], P('gx', 'gy', 'gz')
The draws below stay inside these ranges and needn't reach their ends.
Inputs may be any that keep to these rules, and one draw needn't show every extreme that they name: `forced_modes`: each row is a wave vector (kx, ky, kz) with 1 <= kx^2 + ky^2 + kz^2 <= 9; the 96 rows are distinct.
All inputs are finite; a program needn't handle non-finite values.
Results may differ from the reference program's by a relative error of at most 0.0003.
Values sent between devices are 32-bit elements; how exact they have to be, the bound alone decides.
A program may use at most 64 MiB of HBM per device.

```python
import jax
import jax.numpy as jnp
import numpy as np
from jax import lax

KMAX = 3
MODES = 96
NX = 32
NY = 32
NZ = 512


def draw_momentum(key, part):
    keys = jax.random.split(key, 6)
    noise = jnp.clip(0.35 * jax.random.normal(keys[0], (NX, NY, NZ), jnp.float32), -1.4, 1.4)
    amp_low = 0.4
    amp_high = 1.0
    total = noise
    for term in range(4):
        sub = jax.random.split(keys[term + 1], 3)
        wavevec = jax.random.randint(sub[0], (3,), 0, 2).astype(jnp.float32)
        phases = jax.random.uniform(sub[1], (3,), jnp.float32, -jnp.pi, jnp.pi)
        amplitude = jax.random.uniform(sub[2], (), jnp.float32, amp_low, amp_high)
        wave_x = jnp.cos(2.0 * jnp.pi * wavevec[0] * jnp.arange(NX, dtype=jnp.float32) / NX + phases[0])
        wave_y = jnp.cos(2.0 * jnp.pi * wavevec[1] * jnp.arange(NY, dtype=jnp.float32) / NY + phases[1])
        wave_z = jnp.cos(2.0 * jnp.pi * wavevec[2] * jnp.arange(NZ, dtype=jnp.float32) / NZ + phases[2])
        total = total + amplitude * wave_x[:, None, None] * wave_y[None, :, None] * wave_z[None, None, :]
    return total.astype(jnp.float32)


def wave_sheet(key, rows, cols, theta_low, theta_high):
    keys = jax.random.split(key, 3)
    theta = jax.random.uniform(keys[0], (3,), jnp.float32, theta_low, theta_high)
    drift = jax.random.uniform(keys[1], (3,), jnp.float32, -0.2, 0.2)
    phase = jax.random.uniform(keys[2], (3,), jnp.float32, -jnp.pi, jnp.pi)
    across = jnp.arange(rows, dtype=jnp.float32)[:, None]
    along = jnp.arange(cols, dtype=jnp.float32)[None, :]
    total = jnp.zeros((rows, cols), jnp.float32)
    for term in range(3):
        total = total + 0.09 * jnp.cos(theta[term] * along + drift[term] * across + phase[term])
    return total


def draw_hydrogen(key, part):
    keys = jax.random.split(key, 3)
    sheet_y = wave_sheet(keys[0], NX, NY, 0.5, 1.05)
    sheet_z = wave_sheet(keys[1], NX, NZ, 0.5, 1.05)
    rough = jnp.clip(0.02 * jax.random.normal(keys[2], (NX, NY, NZ), jnp.float32), -0.045, 0.045)
    smooth = 0.6 + sheet_y[:, :, None] + sheet_z[:, None, :]
    return (smooth * (1.0 + rough)).astype(jnp.float32)


def draw_forced_modes(key, part):
    grid = np.arange(-3, 4)
    triples = np.stack(np.meshgrid(grid, grid, grid, indexing='ij'), -1).reshape(-1, 3)
    radius = np.sum(triples * triples, axis=1)
    valid = triples[(radius >= 1) & (radius <= 9)].astype(np.int32)
    chosen = jax.random.permutation(key, valid.shape[0])[:MODES]
    return jnp.asarray(valid)[chosen].astype(jnp.int32)


def steps_of(rng, shape, pieces, smallest, high):
    gain = 1.0
    for axis_at, shards_of in pieces:
        heights = jax.random.uniform(jax.random.fold_in(jax.random.fold_in(rng, 6), axis_at), (shards_of,), jnp.float32, smallest / len(pieces), high / len(pieces))
        gain = gain * jnp.repeat(jnp.exp(heights), shape[axis_at] // shards_of).reshape((-1,) + (1,) * (len(shape) - 1 - axis_at))
    return gain


def setup_inputs(seed: int = 0) -> dict:
    streams_of = jax.random.split(jax.random.key(seed), 5)
    density = jnp.clip(0.7 + 0.90000004 * jax.random.uniform(streams_of[0], (NX, NY, NZ), jnp.float32) ** steps_of(streams_of[0], (NX, NY, NZ), ((0, 4), (1, 2), (2, 4)), -0.2, 0.2), 0.7, 1.6)
    momentum = draw_momentum(jax.random.fold_in(streams_of[4], 71), 0)
    hydrogen = draw_hydrogen(jax.random.fold_in(streams_of[4], 71), 0)
    forced_modes = draw_forced_modes(jax.random.fold_in(streams_of[4], 71), 0)
    return dict(density=density, momentum=momentum, hydrogen=hydrogen, forced_modes=forced_modes)


FIRST_COEFFS = (0.8, -0.2, 4.0 / 105.0, -1.0 / 280.0)
SECOND_COEFFS = (1.6, -0.2, 8.0 / 315.0, -1.0 / 560.0)
CENTRE_COEFF = -205.0 / 72.0
VISCOSITY = 0.3
DIFFUSIVITY = 1.5
FORCE_POWER = 0.3
ENERGY_EPS = 1e-6
ACTIVATION = 2.0
HIGHEST = lax.Precision.HIGHEST


def first_diff(field, axis):
    total = jnp.zeros_like(field)
    for offset, weight in enumerate(FIRST_COEFFS, 1):
        total = total + weight * (jnp.roll(field, -offset, axis) - jnp.roll(field, offset, axis))
    return total


def second_diff(field, axis):
    total = CENTRE_COEFF * field
    for offset, weight in enumerate(SECOND_COEFFS, 1):
        total = total + weight * (jnp.roll(field, -offset, axis) + jnp.roll(field, offset, axis))
    return total


def wave_tables(start, local, total):
    position = start + jnp.arange(local, dtype=jnp.int32)
    wavenum = jnp.arange(-KMAX, KMAX + 1, dtype=jnp.int32)
    phase = (wavenum[:, None] * position[None, :]) % total
    angle = (2.0 * jnp.pi / total) * phase.astype(jnp.float32)
    return jnp.cos(angle), jnp.sin(angle)


def reference(density, momentum, hydrogen, forced_modes):
    size_x, size_y, size_z = density.shape
    velocity = momentum / density
    cos_x, sin_x = wave_tables(0, size_x, size_x)
    cos_y, sin_y = wave_tables(0, size_y, size_y)
    cos_z, sin_z = wave_tables(0, size_z, size_z)
    flat = velocity.reshape(size_x * size_y, size_z)
    part_re = jnp.dot(cos_z, flat.T, precision=HIGHEST).reshape(-1, size_x, size_y)
    part_im = jnp.dot(sin_z, flat.T, precision=HIGHEST).reshape(-1, size_x, size_y)
    mid_re = jnp.einsum('axy,by->abx', part_re, cos_y, precision=HIGHEST) - jnp.einsum('axy,by->abx', part_im, sin_y, precision=HIGHEST)
    mid_im = jnp.einsum('axy,by->abx', part_re, sin_y, precision=HIGHEST) + jnp.einsum('axy,by->abx', part_im, cos_y, precision=HIGHEST)
    cube_re = jnp.einsum('abx,cx->cba', mid_re, cos_x, precision=HIGHEST) - jnp.einsum('abx,cx->cba', mid_im, sin_x, precision=HIGHEST)
    cube_im = jnp.einsum('abx,cx->cba', mid_re, sin_x, precision=HIGHEST) + jnp.einsum('abx,cx->cba', mid_im, cos_x, precision=HIGHEST)
    width = 2 * KMAX + 1
    code = (forced_modes[:, 0] + KMAX) * width * width + (forced_modes[:, 1] + KMAX) * width + (forced_modes[:, 2] + KMAX)
    selector = (code[:, None] == jnp.arange(width ** 3, dtype=jnp.int32)[None, :]).astype(jnp.float32)
    ncell = float(size_x * size_y * size_z)
    coef_cos = jnp.dot(selector, cube_re.reshape(-1), precision=HIGHEST) / ncell
    coef_sin = jnp.dot(selector, cube_im.reshape(-1), precision=HIGHEST) / ncell
    energy = jnp.sum(coef_cos * coef_cos + coef_sin * coef_sin)
    spec_re = jnp.dot(selector.T, coef_cos, precision=HIGHEST).reshape(width, width, width)
    spec_im = -jnp.dot(selector.T, coef_sin, precision=HIGHEST).reshape(width, width, width)
    step_re = jnp.einsum('abc,ax->xbc', spec_re, cos_x, precision=HIGHEST) - jnp.einsum('abc,ax->xbc', spec_im, sin_x, precision=HIGHEST)
    step_im = jnp.einsum('abc,ax->xbc', spec_re, sin_x, precision=HIGHEST) + jnp.einsum('abc,ax->xbc', spec_im, cos_x, precision=HIGHEST)
    plane_re = jnp.einsum('xbc,by->xyc', step_re, cos_y, precision=HIGHEST) - jnp.einsum('xbc,by->xyc', step_im, sin_y, precision=HIGHEST)
    plane_im = jnp.einsum('xbc,by->xyc', step_re, sin_y, precision=HIGHEST) + jnp.einsum('xbc,by->xyc', step_im, cos_y, precision=HIGHEST)
    low = 2.0 * (jnp.dot(plane_re.reshape(-1, width), cos_z, precision=HIGHEST) - jnp.dot(plane_im.reshape(-1, width), sin_z, precision=HIGHEST))
    force = FORCE_POWER * low.reshape(size_x, size_y, size_z) / (energy + ENERGY_EPS)
    density_rate = -first_diff(momentum, 0)
    lap_mom = second_diff(momentum, 0) + second_diff(momentum, 1) + second_diff(momentum, 2)
    lap_fuel = second_diff(hydrogen, 0) + second_diff(hydrogen, 1) + second_diff(hydrogen, 2)
    momentum_rate = -first_diff(momentum * velocity + density, 0) + VISCOSITY * lap_mom + density * force
    hydrogen_rate = -first_diff(hydrogen * velocity, 0) + DIFFUSIVITY * lap_fuel - hydrogen * jnp.exp(-ACTIVATION * hydrogen / density)
    return density_rate, momentum_rate, hydrogen_rate
```

```python
import functools
import math

import jax
import jax.numpy as jnp
import numpy as np
from jax import lax
from jax.experimental import pallas as pl
from jax.experimental.pallas import tpu as pltpu
from jax.sharding import PartitionSpec as P

KMAX = 3
WIDTH = 2 * KMAX + 1
HALF = 64
ROWS = KMAX + 1
REACH = 4

FIRST_COEFFS = (0.8, -0.2, 4.0 / 105.0, -1.0 / 280.0)
SECOND_COEFFS = (1.6, -0.2, 8.0 / 315.0, -1.0 / 560.0)
CENTRE_COEFF = -205.0 / 72.0
VISCOSITY = 0.3
DIFFUSIVITY = 1.5
FORCE_POWER = 0.3
ENERGY_EPS = 1e-06
ACTIVATION = 2.0
HIGHEST = lax.Precision.HIGHEST
MESH = pl.DeviceIdType.MESH


def packed_modes():
    reach = range(-KMAX, KMAX + 1)
    cells = [(x, y, z) for z in range(ROWS) for x in reach for y in reach
             if x * x + y * y + z * z <= KMAX * KMAX and (z, x, y) > (0, 0, 0)]
    return cells


def packed_index(place):
    cells = packed_modes()
    result = []
    for part in range(3):
        value = jnp.full(place.shape, cells[0][part], jnp.int32)
        if part == 1:
            value = value + place
        for i in range(1, len(cells)):
            step = cells[i][part] - cells[i - 1][part] - (part == 1)
            if step:
                value = value + jnp.where(place >= i, step, 0)
        result.append(value)
    return result


def tables(local, full):
    size_x, size_y, size_z = local
    full_x, full_y, full_z = full
    k = np.arange(-KMAX, KMAX + 1)
    ang_z = 2.0 * np.pi * (k[:, None] * np.arange(size_z)[None, :]) / full_z
    trig_z = np.zeros((2 * ROWS, size_z))
    trig_z[:ROWS] = np.cos(ang_z[KMAX:])
    trig_z[ROWS:] = np.sin(ang_z[KMAX:])
    ax = k[:, None] * np.arange(size_x)[None, :] / full_x
    ay = k[:, None] * np.arange(size_y)[None, :] / full_y
    ang = np.stack([2.0 * np.pi * (ax[x + KMAX, :, None] + ay[y + KMAX, None, :]) for x, y, _ in packed_modes()])
    ang = ang.reshape(-1, size_x * size_y)
    trig_xy = np.zeros((2 * HALF, size_x * size_y))
    trig_xy[: len(ang)] = np.cos(ang)
    trig_xy[HALF : HALF + len(ang)] = np.sin(ang)
    edge = np.zeros((8, size_z))
    for j in range(REACH):
        edge[j, j] = 1.0
        edge[REACH + j, size_z - REACH + j] = 1.0
    band = np.zeros((size_z, size_z))
    halo = np.zeros((16, size_z))
    for z in range(size_z):
        band[z, z] = 3.0 * CENTRE_COEFF
        for offset, weight in enumerate(SECOND_COEFFS, 1):
            for q in (z - offset, z + offset):
                if 0 <= q < size_z:
                    band[q, z] = weight
                elif q < 0:
                    halo[8 + q, z] = weight
                else:
                    halo[8 + q - size_z, z] = weight
    z_high, z_low = split_host(trig_z)
    xy_high, xy_low = split_host(trig_xy)
    early = np.concatenate([z_high, z_low, xy_high, xy_low, z_high, z_high, z_low, z_low,
                            split_host(np.concatenate([edge, np.zeros_like(edge)], 0))[0]], 0)
    back = np.concatenate([xy_high, xy_low], 1)
    late = np.concatenate([halo, band], 0).astype(np.float32)
    return early, back, late


def split_host(table):
    high = table.astype(np.float32).astype(jnp.bfloat16)
    low = (table - high.astype(np.float64)).astype(np.float32).astype(jnp.bfloat16)
    return high, low


def split(x):
    high = x.astype(jnp.bfloat16).astype(jnp.float32)
    return high, x - high


def dot_split(a, b, contract):
    return lax.dot_general(a.astype(jnp.bfloat16), b.astype(jnp.bfloat16), (contract, ((), ())),
                           preferred_element_type=jnp.float32)


def fold(x):
    rows, lanes = x.shape
    x = x[: rows // 2] + x[rows // 2 :]
    return x[:, : lanes // 2] + x[:, lanes // 2 :]


def dot_nt(a, b):
    return lax.dot_general(a, b, (((1,), (1,)), ((), ())), precision=HIGHEST, preferred_element_type=jnp.float32)


def dot_nn(a, b):
    return lax.dot_general(a, b, (((1,), (0,)), ((), ())), precision=HIGHEST, preferred_element_type=jnp.float32)


def dot_tn(a, b):
    return lax.dot_general(a, b, (((0,), (0,)), ((), ())), precision=HIGHEST, preferred_element_type=jnp.float32)


def tree_sum(parts):
    parts = list(parts)
    while len(parts) > 1:
        parts = [sum(parts[i : i + 2][1:], parts[i]) for i in range(0, len(parts), 2)]
    return parts[0]


def root_places(sizes):
    return [{"gx": x, "gy": 0, "gz": 0} for x in range(min(2, sizes["gx"]))]


def kernel(sizes, local, dens_hbm, mom_hbm, fuel_hbm, modes_hbm, early_hbm, back_hbm, late_hbm,
           drate, mrate, hrate,
           f, modes, early, back, late, edges, sides, ypack, zpack, ztile, own_sum, got_sums, full_sum,
           load_sem, halo_send, halo_recv, z_send, z_recv, sum_send, sum_recv, full_send, full_recv):
    size_x, size_y, size_z = local
    rows = size_x * size_y
    rows_z = 2 * ROWS
    me = {a: lax.axis_index(a) for a in sizes}
    count_x, count_y, count_z = sizes["gx"], sizes["gy"], sizes["gz"]
    total = count_x * count_y * count_z
    roots = root_places(sizes)
    rank_of = lambda p: (p["gz"] * count_x + p["gx"]) * count_y + p["gy"]
    rank = rank_of(me)
    root_ranks = [rank_of(r) for r in roots]
    is_root = functools.reduce(jnp.logical_or, [rank == r for r in root_ranks])

    def place_of(i):
        return {"gx": lax.rem(lax.div(i, count_y), count_x), "gy": lax.rem(i, count_y),
                "gz": lax.div(i, count_x * count_y)}

    def shifted(axis, step):
        return {axis: lax.rem(me[axis] + step % sizes[axis], sizes[axis])}

    own = pl.ds(REACH, size_x)
    loads = [
        pltpu.make_async_copy(src, dst, load_sem.at[i])
        for i, (src, dst) in enumerate([
            (dens_hbm, f.at[0, own]), (mom_hbm, f.at[1, own]), (early_hbm, early),
            (fuel_hbm, f.at[2, own]), (modes_hbm, modes), (late_hbm, late), (back_hbm, back),
        ])
    ]
    for copy in loads:
        copy.start()

    barrier = pltpu.get_barrier_semaphore()
    z_steps = (1, -1)
    z_next = [shifted("gz", step)["gz"] for step in z_steps]
    z_lower = [z < me["gz"] for z in z_next]
    y_steps = (1, -1) if count_y > 2 else (1,)
    sides_used = len(y_steps)

    def greet(place):
        pl.semaphore_signal(barrier, inc=1, device_id=place, device_id_type=MESH)

    for step in (1, -1):
        greet(shifted("gx", step))
    for step in y_steps:
        greet(shifted("gy", step))
    for step, lower in zip(z_steps, z_lower):
        @pl.when(jnp.logical_not(lower))
        def _(step=step):
            greet(shifted("gz", step))

    @pl.when(is_root)
    def _():
        def greet_one(i, carry):
            @pl.when(i != rank)
            def _():
                greet(place_of(i))
            return carry
        lax.fori_loop(0, total, greet_one, 0)

    greeters = 2 + sides_used + len(roots) - is_root.astype(jnp.int32)
    for lower in z_lower:
        greeters = greeters + lower.astype(jnp.int32)

    lane = lax.broadcasted_iota(jnp.int32, (1, 2 * HALF), 1)
    kx, ky, kz = packed_index(lax.rem(lane, HALF))
    turn = jnp.zeros((1, 2 * HALF), jnp.float32)
    for k, axis in ((kx, "gx"), (ky, "gy"), (kz, "gz")):
        part = k.astype(jnp.float32) * me[axis].astype(jnp.float32) / sizes[axis]
        turn = turn + (part - jnp.floor(part))
    level = (lax.broadcasted_iota(jnp.int32, (ROWS, 2 * HALF), 0) == kz).astype(jnp.float32)
    turn = turn - jnp.floor(turn + 0.5)
    cos_p = jnp.cos(2.0 * math.pi * turn)
    sin_p = jnp.sin(2.0 * math.pi * turn)
    sign = jnp.where(lane < HALF, -1.0, 1.0)
    sin_p = sign * sin_p

    loads[0].wait()
    loads[1].wait()
    loads[2].wait()
    flat = lambda i: f[i, own].reshape(rows, size_z)
    vel = flat(1) / flat(0)
    deep = 2 * rows_z
    table_xy = early[deep : deep + 4 * HALF]
    vel_both = jnp.concatenate(split(vel), 0)
    part = fold(dot_split(early[0:deep], vel_both, ((1,), (1,))))
    grid = fold(dot_split(jnp.concatenate(split(part), 0), table_xy, ((1,), (1,))))
    grid = grid * jnp.concatenate([level, level], 0)
    flip = jnp.sum(grid[ROWS:], axis=0, keepdims=True)
    cube = jnp.sum(grid[0:ROWS], axis=0, keepdims=True) + sign * pltpu.roll(flip, HALF, 1)
    cube = cos_p * cube + sin_p * pltpu.roll(cube, HALF, 1)
    own_sum[...] = cube
    got_sums[rank] = cube

    pl.semaphore_wait(barrier, greeters)
    to_root = [
        pltpu.make_async_remote_copy(
            src_ref=own_sum, dst_ref=got_sums.at[rank], send_sem=sum_send.at[i], recv_sem=sum_recv,
            device_id={a: jnp.int32(v) for a, v in place.items()}, device_id_type=MESH)
        for i, place in enumerate(roots)
    ]
    for copy, r in zip(to_root, root_ranks):
        @pl.when(rank != r)
        def _(copy=copy):
            copy.start()

    def send(src, dst, slot, axis, step):
        copy = pltpu.make_async_remote_copy(
            src_ref=src, dst_ref=dst, send_sem=halo_send.at[slot], recv_sem=halo_recv.at[slot],
            device_id=shifted(axis, step), device_id_type=MESH)
        copy.start()
        return copy

    loads[3].wait()
    halos_x = [
        send(f.at[:, pl.ds(size_x, REACH)], f.at[:, pl.ds(0, REACH)], 0, "gx", 1),
        send(f.at[:, pl.ds(REACH, REACH)], f.at[:, pl.ds(size_x + REACH, REACH)], 0, "gx", -1),
    ]
    pieces = []
    for i in range(2):
        ypack[i, :, 0:REACH] = f[1 + i, own, 0:REACH]
        ypack[i, :, REACH : 2 * REACH] = f[1 + i, own, size_y - REACH : size_y]
        high, rest = split(flat(1 + i))
        pieces += [high, *split(rest)]
    edge_at = deep + 4 * HALF + 4 * rows_z
    ends = dot_split(early[edge_at : edge_at + 16], jnp.concatenate(pieces, 0), ((1,), (1,)))[0:8]
    for i in range(2):
        zpack[i] = tree_sum([ends[:, (3 * i + j) * rows : (3 * i + j + 1) * rows] for j in range(3)])
    halos_y = [send(ypack, sides.at[i], 1, "gy", step) for i, step in enumerate(y_steps)]
    halos_z = [
        pltpu.make_async_remote_copy(
            src_ref=zpack, dst_ref=ztile.at[i], send_sem=z_send.at[i], recv_sem=z_recv.at[i],
            device_id=shifted("gz", step), device_id_type=MESH)
        for i, step in enumerate(z_steps)
    ]
    for copy, lower in zip(halos_z, z_lower):
        @pl.when(lower)
        def _(copy=copy):
            copy.start()

    loads[4].wait()
    count = modes.shape[1]
    code = (modes[0:1] * WIDTH + modes[1:2]) * WIDTH + modes[2:3]
    place = lax.rem(lax.broadcasted_iota(jnp.int32, (2 * HALF, 1), 0), HALF)
    px, py, pz = packed_index(place)
    mine = (px * WIDTH + py) * WIDTH + pz
    used = place < len(packed_modes())
    both_ways = jnp.where(used & (mine == code), 1.0, 0.0) + jnp.where(used & (mine == -code), 1.0, 0.0)
    chosen = dot_nt(jnp.ones((8, count), jnp.float32), both_ways)[0:1]

    loads[5].wait()
    lap = [dot_nn(flat(1 + i), late[16 : 16 + size_z]).reshape(size_x, size_y, size_z) for i in range(2)]
    outs = (drate, mrate, hrate)
    mrate[...] = lap[0]
    hrate[...] = lap[1]

    arrived = [f.at[:, pl.ds(0, 2 * REACH)], sides.at[pl.ds(0, sides_used)]]
    def wait_halo(sem, slot):
        pltpu.make_async_copy(arrived[slot], arrived[slot], sem.at[slot]).wait()

    wait_halo(halo_recv, 1)
    for i in range(2):
        edges[i, :, 0:8] = sides[0, i]
        edges[i, :, 8 : 8 + size_y] = f[1 + i, own]
        edges[i, :, 8 + size_y : 16 + size_y] = sides[sides_used - 1, i]
        total_y = outs[1 + i][...]
        for offset, weight in enumerate(SECOND_COEFFS, 1):
            total_y = total_y + weight * (
                edges[i, :, 8 + offset : 8 + offset + size_y] + edges[i, :, 8 - offset : 8 - offset + size_y])
        outs[1 + i][...] = total_y

    wait_halo(halo_recv, 0)
    def planes(x, offset):
        return x[REACH + offset : REACH + offset + size_x]

    def first_diff(x):
        result = None
        for offset, weight in enumerate(FIRST_COEFFS, 1):
            term = weight * (planes(x, offset) - planes(x, -offset))
            result = term if result is None else result + term
        return result

    def second_diff(x):
        return tree_sum([w * (planes(x, o) + planes(x, -o)) for o, w in enumerate(SECOND_COEFFS, 1)])

    mom = f[1]
    dens = f[0]
    fuel = f[2]
    vel_pad = mom / dens
    drate[...] = -first_diff(mom)
    mid_fuel = planes(fuel, 0)
    hrate[...] = (DIFFUSIVITY * (hrate[...] + second_diff(fuel)) - first_diff(fuel * vel_pad)
                  - mid_fuel * jnp.exp(-ACTIVATION * mid_fuel / planes(dens, 0)))
    mrate[...] = VISCOSITY * (mrate[...] + second_diff(mom)) - first_diff(mom * vel_pad + dens)

    from_next = [pltpu.make_async_copy(ztile.at[1 - i], ztile.at[1 - i], z_recv.at[1 - i]) for i in range(2)]
    for copy, got, lower in zip(halos_z, from_next, z_lower):
        @pl.when(jnp.logical_not(lower))
        def _(copy=copy, got=got):
            got.wait()
            copy.start()
    for got, lower in zip(from_next, z_lower):
        @pl.when(lower)
        def _(got=got):
            got.wait()
    for i, gain in enumerate((VISCOSITY, DIFFUSIVITY)):
        tile = jnp.concatenate([ztile[0, i], ztile[1, i]], 0)
        outs[1 + i][...] = outs[1 + i][...] + gain * dot_tn(tile, late[0:16]).reshape(size_x, size_y, size_z)

    loads[6].wait()
    def spread(i):
        return pltpu.make_async_remote_copy(
            src_ref=full_sum, dst_ref=full_sum, send_sem=full_send, recv_sem=full_recv,
            device_id=place_of(i), device_id_type=MESH)

    others = total - len(roots)

    @pl.when(is_root)
    def _():
        got = got_sums.at[pl.ds(0, total - 1)]
        pltpu.make_async_copy(got, got, sum_recv).wait()
        full_sum[...] = tree_sum([got_sums[i] for i in range(total)])

    if others:
        @pl.when(rank == root_ranks[-1])
        def _():
            def send_one(j, carry):
                i = total - 1 - j
                leaf = functools.reduce(jnp.logical_and, [i != r for r in root_ranks])
                @pl.when(leaf)
                def _():
                    spread(i).start()
                return carry
            lax.fori_loop(0, total, send_one, 0)

        @pl.when(jnp.logical_not(is_root))
        def _():
            pltpu.make_async_copy(full_sum, full_sum, full_recv).wait()

    ncell = float(rows * size_z * total)
    cube = full_sum[...]
    coef = cube / ncell
    picked = chosen * coef
    energy = jnp.sum(jnp.sum(picked * coef, axis=1, keepdims=True), axis=0, keepdims=True)
    scale = 2.0 * FORCE_POWER / (energy + ENERGY_EPS)
    local_coef = cos_p * picked - sin_p * pltpu.roll(picked, HALF, 1)
    both = jnp.concatenate([level * local_coef, level * (-sign * pltpu.roll(local_coef, HALF, 1))], 0)
    wave = fold(dot_split(jnp.concatenate(split(both), 0), back[...], ((1,), (0,))))
    high, rest = split(wave)
    waves = jnp.concatenate([high, rest, high, rest], 0).T
    low = dot_split(waves, early[deep + 4 * HALF : deep + 4 * HALF + 4 * rows_z], ((1,), (0,)))
    low = low.reshape(size_x, size_y, size_z)
    mrate[...] = mrate[...] + f[0, own] * (low * scale.reshape(1, 1, 1))
    for slot in range(2):
        wait_halo(halo_send, slot)
    for i in range(2):
        pltpu.make_async_copy(zpack, zpack, z_send.at[i]).wait()
    for i, r in enumerate(root_ranks):
        @pl.when(rank != r)
        def _(i=i):
            pltpu.make_async_copy(own_sum, own_sum, sum_send.at[i]).wait()
    if others:
        @pl.when(rank == root_ranks[-1])
        def _():
            sent = got_sums.at[pl.ds(0, others)]
            pltpu.make_async_copy(sent, sent, full_send).wait()


def write_out(*refs):
    count = len(refs) // 2
    copies = [pltpu.make_async_copy(refs[i], refs[count + i], refs[-1].at[i]) for i in range(count)]
    for copy in copies:
        copy.start()
    for copy in copies:
        copy.wait()


def solution(mesh):
    sizes = {a: mesh.shape[a] for a in ("gx", "gy", "gz")}

    def per_device(density, momentum, hydrogen, forced_modes):
        local = density.shape
        size_x, size_y, size_z = local
        rows = size_x * size_y
        full = (size_x * sizes["gx"], size_y * sizes["gy"], size_z * sizes["gz"])
        early, back, late = tables(local, full)
        modes = forced_modes.T
        total = math.prod(sizes.values())
        any_spec = pl.BlockSpec(memory_space=pl.ANY)
        f32 = jnp.float32
        rates = pl.pallas_call(
            functools.partial(kernel, sizes, local),
            out_shape=[pltpu.VMEM(local, f32)] * 3,
            in_specs=[any_spec] * 7,
            out_specs=[pl.BlockSpec(memory_space=pltpu.VMEM)] * 3,
            scratch_shapes=[
                pltpu.VMEM((3, size_x + 2 * REACH, size_y, size_z), f32),
                pltpu.VMEM(modes.shape, jnp.int32),
                pltpu.VMEM(early.shape, jnp.bfloat16),
                pltpu.VMEM(back.shape, jnp.bfloat16),
                pltpu.VMEM(late.shape, f32),
                pltpu.VMEM((2, size_x, size_y + 16, size_z), f32),
                pltpu.VMEM((2, 2, size_x, 8, size_z), f32),
                pltpu.VMEM((2, size_x, 8, size_z), f32),
                pltpu.VMEM((2, 8, rows), f32),
                pltpu.VMEM((2, 2, 8, rows), f32),
                pltpu.VMEM((1, 2 * HALF), f32),
                pltpu.VMEM((total, 1, 2 * HALF), f32),
                pltpu.VMEM((1, 2 * HALF), f32),
                pltpu.SemaphoreType.DMA((7,)),
                pltpu.SemaphoreType.DMA((2,)),
                pltpu.SemaphoreType.DMA((2,)),
                pltpu.SemaphoreType.DMA((2,)),
                pltpu.SemaphoreType.DMA((2,)),
                pltpu.SemaphoreType.DMA((2,)),
                pltpu.SemaphoreType.DMA,
                pltpu.SemaphoreType.DMA,
                pltpu.SemaphoreType.DMA,
            ],
            compiler_params=pltpu.CompilerParams(collective_id=0, has_side_effects=True),
            name="flame",
        )(density, momentum, hydrogen, modes, jnp.asarray(early), jnp.asarray(back), jnp.asarray(late))
        return tuple(pl.pallas_call(
            write_out,
            out_shape=[jax.ShapeDtypeStruct(local, f32)] * 3,
            in_specs=[pl.BlockSpec(memory_space=pltpu.VMEM)] * 3,
            out_specs=[any_spec] * 3,
            scratch_shapes=[pltpu.SemaphoreType.DMA((3,))],
            name="write",
        )(*[pltpu.with_memory_space_constraint(r, pltpu.VMEM) for r in rates]))

    in_specs = (P("gx", "gy", "gz"), P("gx", "gy", "gz"), P("gx", "gy", "gz"), P())
    out_specs = (P("gx", "gy", "gz"), P("gx", "gy", "gz"), P("gx", "gy", "gz"))
    return jax.shard_map(
        per_device, mesh=mesh, in_specs=in_specs, out_specs=out_specs, check_vma=False
    )
```

```python
import functools
import math

import jax
import jax.numpy as jnp
import numpy as np
from jax import lax
from jax.experimental import pallas as pl
from jax.experimental.pallas import tpu as pltpu
from jax.sharding import PartitionSpec as P

KMAX = 3
WIDTH = 2 * KMAX + 1
HALF = 64
ROWS = KMAX + 1
REACH = 4

FIRST_COEFFS = (0.8, -0.2, 4.0 / 105.0, -1.0 / 280.0)
SECOND_COEFFS = (1.6, -0.2, 8.0 / 315.0, -1.0 / 560.0)
CENTRE_COEFF = -205.0 / 72.0
VISCOSITY = 0.3
DIFFUSIVITY = 1.5
FORCE_POWER = 0.3
ENERGY_EPS = 1e-06
ACTIVATION = 2.0
HIGHEST = lax.Precision.HIGHEST
MESH = pl.DeviceIdType.MESH


def packed_modes():
    reach = range(-KMAX, KMAX + 1)
    cells = [(x, y, z) for z in range(ROWS) for x in reach for y in reach
             if x * x + y * y + z * z <= KMAX * KMAX and (z, x, y) > (0, 0, 0)]
    return cells


def packed_index(place):
    cells = packed_modes()
    result = []
    for part in range(3):
        value = jnp.full(place.shape, cells[0][part], jnp.int32)
        if part == 1:
            value = value + place
        for i in range(1, len(cells)):
            step = cells[i][part] - cells[i - 1][part] - (part == 1)
            if step:
                value = value + jnp.where(place >= i, step, 0)
        result.append(value)
    return result


def tables(local, full):
    size_x, size_y, size_z = local
    full_x, full_y, full_z = full
    k = np.arange(-KMAX, KMAX + 1)
    ang_z = 2.0 * np.pi * (k[:, None] * np.arange(size_z)[None, :]) / full_z
    trig_z = np.zeros((2 * ROWS, size_z))
    trig_z[:ROWS] = np.cos(ang_z[KMAX:])
    trig_z[ROWS:] = np.sin(ang_z[KMAX:])
    ax = k[:, None] * np.arange(size_x)[None, :] / full_x
    ay = k[:, None] * np.arange(size_y)[None, :] / full_y
    ang = np.stack([2.0 * np.pi * (ax[x + KMAX, :, None] + ay[y + KMAX, None, :]) for x, y, _ in packed_modes()])
    ang = ang.reshape(-1, size_x * size_y)
    trig_xy = np.zeros((2 * HALF, size_x * size_y))
    trig_xy[: len(ang)] = np.cos(ang)
    trig_xy[HALF : HALF + len(ang)] = np.sin(ang)
    edge = np.zeros((8, size_z))
    for j in range(REACH):
        edge[j, j] = 1.0
        edge[REACH + j, size_z - REACH + j] = 1.0
    band = np.zeros((size_z, size_z))
    halo = np.zeros((16, size_z))
    for z in range(size_z):
        band[z, z] = 3.0 * CENTRE_COEFF
        for offset, weight in enumerate(SECOND_COEFFS, 1):
            for q in (z - offset, z + offset):
                if 0 <= q < size_z:
                    band[q, z] = weight
                elif q < 0:
                    halo[8 + q, z] = weight
                else:
                    halo[8 + q - size_z, z] = weight
    early = np.concatenate([*split_host(trig_z), *split_host(trig_xy)], 0)
    late = np.concatenate([halo, band, trig_xy.T, edge, trig_z], 0).astype(np.float32)
    return early, late


def split_host(table):
    high = table.astype(np.float32).astype(jnp.bfloat16)
    low = (table - high.astype(np.float64)).astype(np.float32).astype(jnp.bfloat16)
    return high, low


def split(x):
    high = x.astype(jnp.bfloat16).astype(jnp.float32)
    return high, x - high


def dot_split(a, b, contract):
    return lax.dot_general(a.astype(jnp.bfloat16), b.astype(jnp.bfloat16), (contract, ((), ())),
                           preferred_element_type=jnp.float32)


def fold(x):
    rows, lanes = x.shape
    x = x[: rows // 2] + x[rows // 2 :]
    return x[:, : lanes // 2] + x[:, lanes // 2 :]


def sum_blocks(parts, rows):
    return tree_sum([x[i : i + rows] for x in parts for i in range(0, x.shape[0], rows)])


def dot_nt(a, b):
    return lax.dot_general(a, b, (((1,), (1,)), ((), ())), precision=HIGHEST, preferred_element_type=jnp.float32)


def dot_nn(a, b):
    return lax.dot_general(a, b, (((1,), (0,)), ((), ())), precision=HIGHEST, preferred_element_type=jnp.float32)


def dot_tn(a, b):
    return lax.dot_general(a, b, (((0,), (0,)), ((), ())), precision=HIGHEST, preferred_element_type=jnp.float32)


def tree_sum(parts):
    parts = list(parts)
    while len(parts) > 1:
        parts = [sum(parts[i : i + 2][1:], parts[i]) for i in range(0, len(parts), 2)]
    return parts[0]


def root_places(sizes):
    return [{"gx": x, "gy": 0, "gz": 0} for x in range(min(2, sizes["gx"]))]


def kernel(sizes, local, dens_hbm, mom_hbm, fuel_hbm, modes_hbm, early_hbm, late_hbm,
           drate, mrate, hrate,
           f, modes, early, late, turned, edges, sides, ypack, zpack, ztile, own_sum, got_sums, full_sum,
           load_sem, send_sem, halo_recv, z_recv, sum_recv):
    size_x, size_y, size_z = local
    rows = size_x * size_y
    rows_z = 2 * ROWS
    me = {a: lax.axis_index(a) for a in sizes}
    count_x, count_y, count_z = sizes["gx"], sizes["gy"], sizes["gz"]
    total = count_x * count_y * count_z
    roots = root_places(sizes)
    rank_of = lambda p: (p["gz"] * count_x + p["gx"]) * count_y + p["gy"]
    rank = rank_of(me)
    root_ranks = [rank_of(r) for r in roots]
    is_root = functools.reduce(jnp.logical_or, [rank == r for r in root_ranks])

    def place_of(i):
        if isinstance(i, int):
            x, y, z = i // count_y % count_x, i % count_y, i // (count_x * count_y)
            return {"gx": jnp.int32(x), "gy": jnp.int32(y), "gz": jnp.int32(z)}
        return {"gx": lax.rem(lax.div(i, count_y), count_x), "gy": lax.rem(i, count_y),
                "gz": lax.div(i, count_x * count_y)}

    def shifted(axis, step):
        return {axis: lax.rem(me[axis] + step % sizes[axis], sizes[axis])}

    own = pl.ds(REACH, size_x)
    load_early = pltpu.make_async_copy(early_hbm, early, load_sem.at[1])
    load_late = pltpu.make_async_copy(late_hbm, late, load_sem.at[1])
    load_dens = pltpu.make_async_copy(dens_hbm, f.at[0, own], load_sem.at[0])
    load_mom = pltpu.make_async_copy(mom_hbm, f.at[1, own], load_sem.at[0])
    load_fuel = pltpu.make_async_copy(fuel_hbm, f.at[2, own], load_sem.at[0])
    load_modes = pltpu.make_async_copy(modes_hbm, modes, load_sem.at[0])
    load_dens.start()
    load_mom.start()
    load_early.start()

    barrier = pltpu.get_barrier_semaphore()
    z_steps = (1, -1)
    z_next = [shifted("gz", step)["gz"] for step in z_steps]
    z_lower = [z < me["gz"] for z in z_next]
    y_steps = (1, -1) if count_y > 2 else (1,)
    sides_used = len(y_steps)

    def greet(place):
        pl.semaphore_signal(barrier, inc=1, device_id=place, device_id_type=MESH)

    for step in (1, -1):
        greet(shifted("gx", step))
    for step in y_steps:
        greet(shifted("gy", step))
    for step, lower in zip(z_steps, z_lower):
        @pl.when(jnp.logical_not(lower))
        def _(step=step):
            greet(shifted("gz", step))

    @pl.when(is_root)
    def _():
        def greet_one(i, carry):
            @pl.when(i != rank)
            def _():
                greet(place_of(i))
            return carry
        lax.fori_loop(0, total, greet_one, 0)

    greeters = 2 + sides_used + len(roots) - is_root.astype(jnp.int32)
    for lower in z_lower:
        greeters = greeters + lower.astype(jnp.int32)

    lane = lax.broadcasted_iota(jnp.int32, (1, 2 * HALF), 1)
    kx, ky, kz = packed_index(lax.rem(lane, HALF))
    turn = jnp.zeros((1, 2 * HALF), jnp.float32)
    for k, axis in ((kx, "gx"), (ky, "gy"), (kz, "gz")):
        part = k.astype(jnp.float32) * me[axis].astype(jnp.float32) / sizes[axis]
        turn = turn + (part - jnp.floor(part))
    turn = turn - jnp.floor(turn + 0.5)
    cos_p = jnp.cos(2.0 * math.pi * turn)
    sin_p = jnp.sin(2.0 * math.pi * turn)
    sign = jnp.where(lane < HALF, -1.0, 1.0)
    row = lax.broadcasted_iota(jnp.int32, (rows_z, 2 * HALF), 0)
    first = (row == kz).astype(jnp.float32)
    second = (row == kz + ROWS).astype(jnp.float32)
    turn_own = first * cos_p - second * sin_p
    turn_swap = first * (sign * sin_p) + second * (sign * cos_p)

    both_loaded = f.at[pl.ds(0, 2), own]
    pltpu.make_async_copy(both_loaded, both_loaded, load_sem.at[0]).wait()
    load_early.wait()
    load_fuel.start()
    load_late.start()
    flat = lambda i: f[i, own].reshape(rows, size_z)
    vel = flat(1) / flat(0)
    deep = 2 * rows_z
    part = sum_blocks([dot_split(early[0:deep], x, ((1,), (1,))) for x in split(vel)], rows_z)
    part_both = jnp.concatenate(split(part), 0)
    cells = [early[deep + i * HALF : deep + (i + 1) * HALF] for i in range(4)]
    grid, swap = [
        fold(dot_split(part_both, jnp.concatenate([cells[i] for i in order], 0), ((1,), (1,))))
        for order in ((0, 1, 2, 3), (1, 0, 3, 2))
    ]
    cube = jnp.sum(turn_own * grid + turn_swap * swap, axis=0, keepdims=True)
    own_sum[...] = cube
    got_sums[rank] = cube

    pl.semaphore_wait(barrier, greeters)
    def copy_out(src, dst, recv, place):
        return pltpu.make_async_remote_copy(
            src_ref=src, dst_ref=dst, send_sem=send_sem, recv_sem=recv, device_id=place, device_id_type=MESH)

    def spread(i):
        return copy_out(full_sum, full_sum, sum_recv, place_of(i))

    for r in root_ranks:
        @pl.when(rank != r)
        def _(r=r):
            copy_out(own_sum, got_sums.at[rank], sum_recv, place_of(r)).start()

    load_fuel.wait()
    load_modes.start()
    halos_x = [
        copy_out(f.at[:, pl.ds(size_x, REACH)], f.at[:, pl.ds(0, REACH)], halo_recv.at[0], shifted("gx", 1)),
        copy_out(f.at[:, pl.ds(REACH, REACH)], f.at[:, pl.ds(size_x + REACH, REACH)], halo_recv.at[0],
                 shifted("gx", -1)),
    ]
    for copy in halos_x:
        copy.start()
    load_late.wait()
    band_at = 16
    trig_at = band_at + size_z
    edge_at = trig_at + rows
    wave_at = edge_at + 8
    pieces = []
    for i in range(2):
        ypack[i, :, 0:REACH] = f[1 + i, own, 0:REACH]
        ypack[i, :, REACH : 2 * REACH] = f[1 + i, own, size_y - REACH : size_y]
        high, rest = split(flat(1 + i))
        pieces += [high, *split(rest)]
    ends = dot_split(late[edge_at : edge_at + 8], jnp.concatenate(pieces, 0), ((1,), (1,)))
    for i in range(2):
        zpack[i] = tree_sum([ends[:, (3 * i + j) * rows : (3 * i + j + 1) * rows] for j in range(3)])
    halos_y = [copy_out(ypack, sides.at[i], halo_recv.at[1], shifted("gy", step)) for i, step in enumerate(y_steps)]
    halos_z = [copy_out(zpack, ztile.at[i], z_recv.at[i], shifted("gz", step)) for i, step in enumerate(z_steps)]
    for copy, lower in zip(halos_z, z_lower):
        @pl.when(lower)
        def _(copy=copy):
            copy.start()
    for copy in halos_y:
        copy.start()

    lap = [dot_nn(flat(1 + i), late[band_at : band_at + size_z]).reshape(size_x, size_y, size_z) for i in range(2)]
    outs = (drate, mrate, hrate)
    mrate[...] = lap[0]
    hrate[...] = lap[1]

    load_modes.wait()
    count = modes.shape[1]
    code = (modes[0:1] * WIDTH + modes[1:2]) * WIDTH + modes[2:3]
    place = lax.rem(lax.broadcasted_iota(jnp.int32, (2 * HALF, 1), 0), HALF)
    px, py, pz = packed_index(place)
    mine = (px * WIDTH + py) * WIDTH + pz
    used = place < len(packed_modes())
    both_ways = jnp.where(used & (mine == code), 1.0, 0.0) + jnp.where(used & (mine == -code), 1.0, 0.0)
    chosen = dot_nt(jnp.ones((8, count), jnp.float32), both_ways)[0:1]

    ncell = float(rows * size_z * total)
    gain = chosen * (2.0 * FORCE_POWER / ncell)
    cells_xy = late[trig_at : trig_at + rows]
    cells_swap = pltpu.roll(cells_xy, HALF, 1)
    signed = sign * sin_p
    for i, table in enumerate((
            (gain * cos_p) * cells_xy + (gain * signed) * cells_swap,
            (gain * sign * cos_p) * cells_swap - (gain * sign * signed) * cells_xy)):
        high, rest = split(table)
        turned[:, 2 * HALF * i : 2 * HALF * (i + 1)] = high.astype(jnp.bfloat16)
        turned[:, 2 * HALF * (2 + i) : 2 * HALF * (3 + i)] = rest.astype(jnp.bfloat16)

    arrived = [f.at[:, pl.ds(0, 2 * REACH)], sides.at[pl.ds(0, sides_used)]]
    def wait_halo(slot):
        pltpu.make_async_copy(arrived[slot], arrived[slot], halo_recv.at[slot]).wait()

    wait_halo(1)
    for i in range(2):
        edges[i, :, 0:8] = sides[0, i]
        edges[i, :, 8 : 8 + size_y] = f[1 + i, own]
        edges[i, :, 8 + size_y : 16 + size_y] = sides[sides_used - 1, i]
        total_y = outs[1 + i][...]
        for offset, weight in enumerate(SECOND_COEFFS, 1):
            total_y = total_y + weight * (
                edges[i, :, 8 + offset : 8 + offset + size_y] + edges[i, :, 8 - offset : 8 - offset + size_y])
        outs[1 + i][...] = total_y

    wait_halo(0)
    def planes(x, offset):
        return x[REACH + offset : REACH + offset + size_x]

    def first_diff(x):
        result = None
        for offset, weight in enumerate(FIRST_COEFFS, 1):
            term = weight * (planes(x, offset) - planes(x, -offset))
            result = term if result is None else result + term
        return result

    def second_diff(x):
        return tree_sum([w * (planes(x, o) + planes(x, -o)) for o, w in enumerate(SECOND_COEFFS, 1)])

    mom = f[1]
    dens = f[0]
    fuel = f[2]
    vel_pad = mom / dens
    drate[...] = -first_diff(mom)
    mid_fuel = planes(fuel, 0)
    hrate[...] = (DIFFUSIVITY * (hrate[...] + second_diff(fuel)) - first_diff(fuel * vel_pad)
                  - mid_fuel * jnp.exp(-ACTIVATION * mid_fuel / planes(dens, 0)))
    mrate[...] = VISCOSITY * (mrate[...] + second_diff(mom)) - first_diff(mom * vel_pad + dens)

    from_next = [pltpu.make_async_copy(ztile.at[1 - i], ztile.at[1 - i], z_recv.at[1 - i]) for i in range(2)]
    for copy, got, lower in zip(halos_z, from_next, z_lower):
        @pl.when(jnp.logical_not(lower))
        def _(copy=copy, got=got):
            got.wait()
            copy.start()
    for got, lower in zip(from_next, z_lower):
        @pl.when(lower)
        def _(got=got):
            got.wait()
    for i, rate in enumerate((VISCOSITY, DIFFUSIVITY)):
        tile = jnp.concatenate([ztile[0, i], ztile[1, i]], 0)
        outs[1 + i][...] = outs[1 + i][...] + rate * dot_tn(tile, late[0:16]).reshape(size_x, size_y, size_z)

    leaves = [i for i in range(total) if i not in root_ranks]

    @pl.when(is_root)
    def _():
        got = got_sums.at[pl.ds(0, total - 1)]
        pltpu.make_async_copy(got, got, sum_recv).wait()
        full_sum[...] = tree_sum([got_sums[i] for i in range(total)])

    if leaves:
        @pl.when(rank == root_ranks[-1])
        def _():
            for i in reversed(leaves):
                spread(i).start()

        @pl.when(jnp.logical_not(is_root))
        def _():
            pltpu.make_async_copy(full_sum, full_sum, sum_recv).wait()

    cube = full_sum[...]
    coef = cube / ncell
    energy = jnp.sum(chosen * coef * coef, axis=1, keepdims=True)
    scale = 1.0 / (energy + ENERGY_EPS)
    split_cube = split(jnp.concatenate([first * cube, second * cube], 1))
    high, rest = [jnp.concatenate([x] * 4, 0).astype(jnp.bfloat16) for x in split_cube]
    right = jnp.concatenate([high, high, rest], 1)
    wave_high, wave_rest = split(late[wave_at : wave_at + rows_z])
    right_z = jnp.concatenate([wave_high, wave_high, wave_rest, wave_rest], 0)
    use_rest = lax.rem(lax.broadcasted_iota(jnp.int32, (rows // 2, 4 * rows_z), 1), 2 * rows_z) >= rows_z
    for half in range(2):
        here = pl.ds(half * rows // 2, rows // 2)
        left = jnp.concatenate([turned[here], turned[here, 0 : 4 * HALF]], 1)
        high, rest = split(dot_split(left, right, ((1,), (1,))))
        low = dot_split(jnp.where(use_rest, rest, high), right_z, ((1,), (0,)))
        low = low.reshape(size_x // 2, size_y, size_z)
        at = pl.ds(half * size_x // 2, size_x // 2)
        mrate[at] = mrate[at] + f[0, pl.ds(REACH + half * size_x // 2, size_x // 2)] * (low * scale.reshape(1, 1, 1))

    for sent in (arrived[0], arrived[1], ztile.at[:, :]):
        pltpu.make_async_copy(sent, sent, send_sem).wait()
    for r in root_ranks:
        @pl.when(rank != r)
        def _():
            pltpu.make_async_copy(own_sum, own_sum, send_sem).wait()
    if leaves:
        @pl.when(rank == root_ranks[-1])
        def _():
            sent = got_sums.at[pl.ds(0, len(leaves))]
            pltpu.make_async_copy(sent, sent, send_sem).wait()


def write_out(*refs):
    count = len(refs) // 2
    copies = [pltpu.make_async_copy(refs[i], refs[count + i], refs[-1]) for i in range(count)]
    for copy in copies:
        copy.start()
    for copy in copies:
        copy.wait()


def solution(mesh):
    sizes = {a: mesh.shape[a] for a in ("gx", "gy", "gz")}

    def per_device(density, momentum, hydrogen, forced_modes):
        local = density.shape
        size_x, size_y, size_z = local
        rows = size_x * size_y
        full = (size_x * sizes["gx"], size_y * sizes["gy"], size_z * sizes["gz"])
        early, late = tables(local, full)
        modes = forced_modes.T
        total = math.prod(sizes.values())
        any_spec = pl.BlockSpec(memory_space=pl.ANY)
        f32 = jnp.float32
        rates = pl.pallas_call(
            functools.partial(kernel, sizes, local),
            out_shape=[pltpu.VMEM(local, f32)] * 3,
            in_specs=[any_spec] * 6,
            out_specs=[pl.BlockSpec(memory_space=pltpu.VMEM)] * 3,
            scratch_shapes=[
                pltpu.VMEM((3, size_x + 2 * REACH, size_y, size_z), f32),
                pltpu.VMEM(modes.shape, jnp.int32),
                pltpu.VMEM(early.shape, jnp.bfloat16),
                pltpu.VMEM(late.shape, f32),
                pltpu.VMEM((rows, 8 * HALF), jnp.bfloat16),
                pltpu.VMEM((2, size_x, size_y + 16, size_z), f32),
                pltpu.VMEM((2, 2, size_x, 8, size_z), f32),
                pltpu.VMEM((2, size_x, 8, size_z), f32),
                pltpu.VMEM((2, 8, rows), f32),
                pltpu.VMEM((2, 2, 8, rows), f32),
                pltpu.VMEM((1, 2 * HALF), f32),
                pltpu.VMEM((total, 1, 2 * HALF), f32),
                pltpu.VMEM((1, 2 * HALF), f32),
                pltpu.SemaphoreType.DMA((2,)),
                pltpu.SemaphoreType.DMA,
                pltpu.SemaphoreType.DMA((2,)),
                pltpu.SemaphoreType.DMA((2,)),
                pltpu.SemaphoreType.DMA,
            ],
            compiler_params=pltpu.CompilerParams(collective_id=0, has_side_effects=True),
            name="flame",
        )(density, momentum, hydrogen, modes, jnp.asarray(early), jnp.asarray(late))
        return tuple(pl.pallas_call(
            write_out,
            out_shape=[jax.ShapeDtypeStruct(local, f32)] * 3,
            in_specs=[pl.BlockSpec(memory_space=pltpu.VMEM)] * 3,
            out_specs=[any_spec] * 3,
            scratch_shapes=[pltpu.SemaphoreType.DMA],
            name="write",
        )(*[pltpu.with_memory_space_constraint(r, pltpu.VMEM) for r in rates]))

    in_specs = (P("gx", "gy", "gz"), P("gx", "gy", "gz"), P("gx", "gy", "gz"), P())
    out_specs = (P("gx", "gy", "gz"), P("gx", "gy", "gz"), P("gx", "gy", "gz"))
    return jax.shard_map(
        per_device, mesh=mesh, in_specs=in_specs, out_specs=out_specs, check_vma=False
    )
```

```python
import functools
import math

import jax
import jax.numpy as jnp
import numpy as np
from jax import lax
from jax.experimental import pallas as pl
from jax.experimental.pallas import tpu as pltpu
from jax.sharding import PartitionSpec as P

KMAX = 3
WIDTH = 2 * KMAX + 1
HALF = 64
ROWS = KMAX + 1
REACH = 4
LOAD_PLANES = 4

FIRST_COEFFS = (0.8, -0.2, 4.0 / 105.0, -1.0 / 280.0)
SECOND_COEFFS = (1.6, -0.2, 8.0 / 315.0, -1.0 / 560.0)
CENTRE_COEFF = -205.0 / 72.0
VISCOSITY = 0.3
DIFFUSIVITY = 1.5
FORCE_POWER = 0.3
ENERGY_EPS = 1e-06
ACTIVATION = 2.0
HIGHEST = lax.Precision.HIGHEST
MESH = pl.DeviceIdType.MESH


def packed_modes():
    reach = range(-KMAX, KMAX + 1)
    cells = [(x, y, z) for z in range(ROWS) for x in reach for y in reach
             if x * x + y * y + z * z <= KMAX * KMAX and (z, x, y) > (0, 0, 0)]
    return cells


def packed_index(place):
    cells = packed_modes()
    result = []
    for part in range(3):
        value = jnp.full(place.shape, cells[0][part], jnp.int32)
        if part == 1:
            value = value + place
        for i in range(1, len(cells)):
            step = cells[i][part] - cells[i - 1][part] - (part == 1)
            if step:
                value = value + jnp.where(place >= i, step, 0)
        result.append(value)
    return result


def tables(size_z):
    edge = np.zeros((8, size_z))
    for j in range(REACH):
        edge[j, j] = 1.0
        edge[REACH + j, size_z - REACH + j] = 1.0
    band = np.zeros((size_z, size_z))
    halo = np.zeros((16, size_z))
    for z in range(size_z):
        band[z, z] = 3.0 * CENTRE_COEFF
        for offset, weight in enumerate(SECOND_COEFFS, 1):
            for q in (z - offset, z + offset):
                if 0 <= q < size_z:
                    band[q, z] = weight
                elif q < 0:
                    halo[8 + q, z] = weight
                else:
                    halo[8 + q - size_z, z] = weight
    return np.concatenate([halo, band, edge], 0).astype(np.float32)


def polynomial(x, coeffs):
    result = coeffs[-1]
    for c in reversed(coeffs[:-1]):
        result = result * x + c
    return result


SIN_COEFFS = [(-1) ** n * (math.pi / 2) ** (2 * n + 1) / math.factorial(2 * n + 1) for n in range(5)]
COS_COEFFS = [(-1) ** n * (math.pi / 2) ** (2 * n) / math.factorial(2 * n) for n in range(6)]


def cos_sin(quarters):
    turns = jnp.floor(quarters + 0.5)
    d = quarters - turns
    square = d * d
    s = d * polynomial(square, SIN_COEFFS)
    c = polynomial(square, COS_COEFFS)
    half = jnp.floor(0.5 * turns)
    odd = turns - 2.0 * half
    turned = half - 2.0 * jnp.floor(0.5 * half)
    sin_sign = 1.0 - 2.0 * turned
    cos_sign = sin_sign - 2.0 * odd * sin_sign
    swap = odd > 0.5
    return jnp.where(swap, s, c) * cos_sign, jnp.where(swap, c, s) * sin_sign


def split(x):
    high = x.astype(jnp.bfloat16).astype(jnp.float32)
    return high, x - high


def dot_split(a, b, contract):
    return lax.dot_general(a.astype(jnp.bfloat16), b.astype(jnp.bfloat16), (contract, ((), ())),
                           preferred_element_type=jnp.float32)


def column_sum(x):
    x = tree_sum([x[i : i + 8] for i in range(0, x.shape[0], 8)])
    return jnp.sum(x, axis=0, keepdims=True)


def dot_nt(a, b):
    return lax.dot_general(a, b, (((1,), (1,)), ((), ())), precision=HIGHEST, preferred_element_type=jnp.float32)


def dot_nn(a, b):
    return lax.dot_general(a, b, (((1,), (0,)), ((), ())), precision=HIGHEST, preferred_element_type=jnp.float32)


def dot_tn(a, b):
    return lax.dot_general(a, b, (((0,), (0,)), ((), ())), precision=HIGHEST, preferred_element_type=jnp.float32)


def tree_sum(parts):
    parts = list(parts)
    while len(parts) > 1:
        parts = [sum(parts[i : i + 2][1:], parts[i]) for i in range(0, len(parts), 2)]
    return parts[0]


def root_places(sizes):
    return [{"gx": x, "gy": 0, "gz": 0} for x in range(min(2, sizes["gx"]))]


def kernel(sizes, local, dens_hbm, mom_hbm, fuel_hbm, modes_hbm, late_hbm,
           drate, mrate, hrate,
           f, modes, late, cells, along, along_low, across, across_low, edges, sides, ypack, zpack, ztile, own_sum, got_sums, full_sum,
           load_sem, send_sem, halo_recv, z_recv, sum_recv, z_ready):
    size_x, size_y, size_z = local
    rows = size_x * size_y
    me = {a: lax.axis_index(a) for a in sizes}
    count_x, count_y, count_z = sizes["gx"], sizes["gy"], sizes["gz"]
    total = count_x * count_y * count_z
    roots = root_places(sizes)
    rank_of = lambda p: (p["gz"] * count_x + p["gx"]) * count_y + p["gy"]
    rank = rank_of(me)
    root_ranks = [rank_of(r) for r in roots]
    is_root = functools.reduce(jnp.logical_or, [rank == r for r in root_ranks])

    def place_of(i):
        if isinstance(i, int):
            x, y, z = i // count_y % count_x, i % count_y, i // (count_x * count_y)
            return {"gx": jnp.int32(x), "gy": jnp.int32(y), "gz": jnp.int32(z)}
        return {"gx": lax.rem(lax.div(i, count_y), count_x), "gy": lax.rem(i, count_y),
                "gz": lax.div(i, count_x * count_y)}

    def shifted(axis, step):
        return {axis: lax.rem(me[axis] + step % sizes[axis], sizes[axis])}

    own = pl.ds(REACH, size_x)
    load_late = pltpu.make_async_copy(late_hbm, late, load_sem.at[1])
    for at in range(0, size_x, LOAD_PLANES):
        for i, src in enumerate((dens_hbm, mom_hbm)):
            pltpu.make_async_copy(
                src.at[pl.ds(at, LOAD_PLANES)], f.at[i, pl.ds(REACH + at, LOAD_PLANES)], load_sem.at[0]).start()
    load_fuel = pltpu.make_async_copy(fuel_hbm, f.at[2, own], load_sem.at[0])
    load_modes = pltpu.make_async_copy(modes_hbm, modes, load_sem.at[0])

    barrier = pltpu.get_barrier_semaphore()
    z_steps = (1, -1)
    z_next = [shifted("gz", step)["gz"] for step in z_steps]
    z_lower = [z < me["gz"] for z in z_next]
    y_steps = (1, -1) if count_y > 2 else (1,)
    sides_used = len(y_steps)

    def greet(place):
        pl.semaphore_signal(barrier, inc=1, device_id=place, device_id_type=MESH)

    for step in (1, -1):
        greet(shifted("gx", step))
    for step in y_steps:
        greet(shifted("gy", step))
    for step, lower in zip(z_steps, z_lower):
        @pl.when(jnp.logical_not(lower))
        def _(step=step):
            greet(shifted("gz", step))

    @pl.when(is_root)
    def _():
        def greet_one(i, carry):
            @pl.when(i != rank)
            def _():
                greet(place_of(i))
            return carry
        lax.fori_loop(0, total, greet_one, 0)

    greeters = 2 + sides_used + len(roots) - is_root.astype(jnp.int32)
    for lower in z_lower:
        greeters = greeters + lower.astype(jnp.int32)

    lane = lax.broadcasted_iota(jnp.int32, (1, 2 * HALF), 1)
    kx, ky, kz = packed_index(lax.rem(lane, HALF))
    quarter = (lane >= HALF).astype(jnp.float32)
    kx, ky, kz = [k.astype(jnp.float32) for k in (kx, ky, kz)]

    def quarters(k, place, axis, size):
        part = k * place.astype(jnp.float32) / (size * sizes[axis])
        return 4.0 * (part - jnp.floor(part))

    shift = quarters(kz, me["gz"] * size_z, "gz", size_z) - quarter
    rows_y = me["gy"] * size_y + lax.broadcasted_iota(jnp.int32, (size_y, 1), 0)
    angle_y = quarters(ky, rows_y, "gy", size_y) + shift
    for x in range(size_x):
        c, s = cos_sin(angle_y + quarters(kx, me["gx"] * size_x + x, "gx", size_x))
        cells[x * size_y : (x + 1) * size_y, 0 : 2 * HALF] = c
        cells[x * size_y : (x + 1) * size_y, 2 * HALF : 4 * HALF] = -s
    for z in range(0, size_z, 16):
        rows_at = z + lax.broadcasted_iota(jnp.int32, (16, 1), 0)
        for i, x in enumerate(cos_sin(quarters(kz, rows_at, "gz", size_z))):
            high, rest = split(x)
            along[z : z + 16, 2 * HALF * i : 2 * HALF * (i + 1)] = high.astype(jnp.bfloat16)
            along_low[z : z + 16, 2 * HALF * i : 2 * HALF * (i + 1)] = rest.astype(jnp.bfloat16)

    both_loaded = f.at[pl.ds(0, 2), own]
    pltpu.make_async_copy(both_loaded, both_loaded, load_sem.at[0]).wait()
    load_fuel.start()
    load_late.start()
    flat = lambda i: f[i, own].reshape(rows, size_z)
    high, rest = split(flat(1) / flat(0))
    part = (dot_split(jnp.concatenate([high, rest], 1), jnp.concatenate([along[...], along[...]], 0), ((1,), (0,)))
            + dot_split(high, along_low[...], ((1,), (0,)))) * cells[...]
    cube = column_sum(part[:, 0 : 2 * HALF] + part[:, 2 * HALF : 4 * HALF])
    own_sum[...] = cube
    got_sums[rank] = cube

    pl.semaphore_wait(barrier, greeters)
    def copy_out(src, dst, recv, place):
        return pltpu.make_async_remote_copy(
            src_ref=src, dst_ref=dst, send_sem=send_sem, recv_sem=recv, device_id=place, device_id_type=MESH)

    def spread(i):
        return copy_out(full_sum, full_sum, sum_recv, place_of(i))

    for r in root_ranks:
        @pl.when(rank != r)
        def _(r=r):
            copy_out(own_sum, got_sums.at[rank], sum_recv, place_of(r)).start()

    for step, lower in zip(z_steps, z_lower):
        @pl.when(lower)
        def _(step=step):
            pl.semaphore_signal(z_ready, inc=1, device_id=shifted("gz", step), device_id_type=MESH)

    load_fuel.wait()
    load_modes.start()
    halos_x = [
        copy_out(f.at[:, pl.ds(size_x, REACH)], f.at[:, pl.ds(0, REACH)], halo_recv.at[0], shifted("gx", 1)),
        copy_out(f.at[:, pl.ds(REACH, REACH)], f.at[:, pl.ds(size_x + REACH, REACH)], halo_recv.at[0],
                 shifted("gx", -1)),
    ]
    for copy in halos_x:
        copy.start()
    load_late.wait()
    band_at = 16
    edge_at = band_at + size_z
    pieces = []
    for i in range(2):
        ypack[i, :, 0:REACH] = f[1 + i, own, 0:REACH]
        ypack[i, :, REACH : 2 * REACH] = f[1 + i, own, size_y - REACH : size_y]
        high, rest = split(flat(1 + i))
        pieces += [high, *split(rest)]
    ends = dot_split(late[edge_at : edge_at + 8], jnp.concatenate(pieces, 0), ((1,), (1,)))
    for i in range(2):
        zpack[i] = tree_sum([ends[:, (3 * i + j) * rows : (3 * i + j + 1) * rows] for j in range(3)])
    halos_y = [copy_out(ypack, sides.at[i], halo_recv.at[1], shifted("gy", step)) for i, step in enumerate(y_steps)]
    halos_z = [copy_out(zpack, ztile.at[i], z_recv.at[i], shifted("gz", step)) for i, step in enumerate(z_steps)]
    for copy, lower in zip(halos_z, z_lower):
        @pl.when(lower)
        def _(copy=copy):
            copy.start()
    for copy in halos_y:
        copy.start()

    lap = [dot_nn(flat(1 + i), late[band_at : band_at + size_z]).reshape(size_x, size_y, size_z) for i in range(2)]
    outs = (drate, mrate, hrate)
    mrate[...] = lap[0]
    hrate[...] = lap[1]

    load_modes.wait()
    count = modes.shape[1]
    code = (modes[0:1] * WIDTH + modes[1:2]) * WIDTH + modes[2:3]
    place = lax.rem(lax.broadcasted_iota(jnp.int32, (2 * HALF, 1), 0), HALF)
    px, py, pz = packed_index(place)
    mine = (px * WIDTH + py) * WIDTH + pz
    used = place < len(packed_modes())
    both_ways = jnp.where(used & (mine == code), 1.0, 0.0) + jnp.where(used & (mine == -code), 1.0, 0.0)
    chosen = dot_nt(jnp.ones((8, count), jnp.float32), both_ways)[0:1]

    ncell = float(rows * size_z * total)
    gain = chosen * (2.0 * FORCE_POWER / ncell)
    for i in range(2):
        here = pl.ds(2 * HALF * i, 2 * HALF)
        across[here] = along[:, here].astype(jnp.float32).T.astype(jnp.bfloat16)
        across_low[here] = along_low[:, here].astype(jnp.float32).T.astype(jnp.bfloat16)

    arrived = [f.at[:, pl.ds(0, 2 * REACH)], sides.at[pl.ds(0, sides_used)]]
    def wait_halo(slot):
        pltpu.make_async_copy(arrived[slot], arrived[slot], halo_recv.at[slot]).wait()

    higher = sum(jnp.logical_not(lower).astype(jnp.int32) for lower in z_lower)

    @pl.when(higher > 0)
    def _():
        pl.semaphore_wait(z_ready, higher)

    for copy, lower in zip(halos_z, z_lower):
        @pl.when(jnp.logical_not(lower))
        def _(copy=copy):
            copy.start()

    wait_halo(1)
    for i in range(2):
        edges[i, :, 0:8] = sides[0, i]
        edges[i, :, 8 : 8 + size_y] = f[1 + i, own]
        edges[i, :, 8 + size_y : 16 + size_y] = sides[sides_used - 1, i]
        total_y = outs[1 + i][...]
        for offset, weight in enumerate(SECOND_COEFFS, 1):
            total_y = total_y + weight * (
                edges[i, :, 8 + offset : 8 + offset + size_y] + edges[i, :, 8 - offset : 8 - offset + size_y])
        outs[1 + i][...] = total_y

    wait_halo(0)
    def planes(x, offset):
        return x[REACH + offset : REACH + offset + size_x]

    def first_diff(x):
        result = None
        for offset, weight in enumerate(FIRST_COEFFS, 1):
            term = weight * (planes(x, offset) - planes(x, -offset))
            result = term if result is None else result + term
        return result

    def second_diff(x):
        return tree_sum([w * (planes(x, o) + planes(x, -o)) for o, w in enumerate(SECOND_COEFFS, 1)])

    mom = f[1]
    dens = f[0]
    fuel = f[2]
    vel_pad = mom / dens
    drate[...] = -first_diff(mom)
    mid_fuel = planes(fuel, 0)
    hrate[...] = (DIFFUSIVITY * (hrate[...] + second_diff(fuel)) - first_diff(fuel * vel_pad)
                  - mid_fuel * jnp.exp(-ACTIVATION * mid_fuel / planes(dens, 0)))
    mrate[...] = VISCOSITY * (mrate[...] + second_diff(mom)) - first_diff(mom * vel_pad + dens)

    for i in range(2):
        pltpu.make_async_copy(ztile.at[i], ztile.at[i], z_recv.at[i]).wait()
    for i, rate in enumerate((VISCOSITY, DIFFUSIVITY)):
        tile = jnp.concatenate([ztile[0, i], ztile[1, i]], 0)
        outs[1 + i][...] = outs[1 + i][...] + rate * dot_tn(tile, late[0:16]).reshape(size_x, size_y, size_z)

    leaves = [i for i in range(total) if i not in root_ranks]

    @pl.when(is_root)
    def _():
        got = got_sums.at[pl.ds(0, total - 1)]
        pltpu.make_async_copy(got, got, sum_recv).wait()
        full_sum[...] = tree_sum([got_sums[i] for i in range(total)])

    if leaves:
        @pl.when(rank == root_ranks[-1])
        def _():
            for i in reversed(leaves):
                spread(i).start()

        @pl.when(jnp.logical_not(is_root))
        def _():
            pltpu.make_async_copy(full_sum, full_sum, sum_recv).wait()

    cube = full_sum[...]
    coef = cube / ncell
    energy = jnp.sum(chosen * coef * coef, axis=1, keepdims=True)
    scale = 1.0 / (energy + ENERGY_EPS)
    lit = gain * cube
    high, rest = split(cells[...] * jnp.concatenate([lit, lit], 1))
    both = dot_split(high, jnp.concatenate([across[...], across_low[...]], 1), ((1,), (0,)))
    low = both[:, 0:size_z] + both[:, size_z:] + dot_split(rest, across[...], ((1,), (0,)))
    low = low.reshape(size_x, size_y, size_z)
    mrate[...] = mrate[...] + f[0, own] * (low * scale.reshape(1, 1, 1))

    for sent in (arrived[0], arrived[1], ztile.at[:, :]):
        pltpu.make_async_copy(sent, sent, send_sem).wait()
    for r in root_ranks:
        @pl.when(rank != r)
        def _():
            pltpu.make_async_copy(own_sum, own_sum, send_sem).wait()
    if leaves:
        @pl.when(rank == root_ranks[-1])
        def _():
            sent = got_sums.at[pl.ds(0, len(leaves))]
            pltpu.make_async_copy(sent, sent, send_sem).wait()


def write_out(*refs):
    count = len(refs) // 2
    copies = [pltpu.make_async_copy(refs[i], refs[count + i], refs[-1]) for i in range(count)]
    for copy in copies:
        copy.start()
    for copy in copies:
        copy.wait()


def solution(mesh):
    sizes = {a: mesh.shape[a] for a in ("gx", "gy", "gz")}

    def per_device(density, momentum, hydrogen, forced_modes):
        local = density.shape
        size_x, size_y, size_z = local
        rows = size_x * size_y
        late = tables(size_z)
        modes = forced_modes.T
        total = math.prod(sizes.values())
        any_spec = pl.BlockSpec(memory_space=pl.ANY)
        f32 = jnp.float32
        rates = pl.pallas_call(
            functools.partial(kernel, sizes, local),
            out_shape=[pltpu.VMEM(local, f32)] * 3,
            in_specs=[any_spec] * 5,
            out_specs=[pl.BlockSpec(memory_space=pltpu.VMEM)] * 3,
            scratch_shapes=[
                pltpu.VMEM((3, size_x + 2 * REACH, size_y, size_z), f32),
                pltpu.VMEM(modes.shape, jnp.int32),
                pltpu.VMEM(late.shape, f32),
                pltpu.VMEM((rows, 4 * HALF), f32),
                pltpu.VMEM((size_z, 4 * HALF), jnp.bfloat16),
                pltpu.VMEM((size_z, 4 * HALF), jnp.bfloat16),
                pltpu.VMEM((4 * HALF, size_z), jnp.bfloat16),
                pltpu.VMEM((4 * HALF, size_z), jnp.bfloat16),
                pltpu.VMEM((2, size_x, size_y + 16, size_z), f32),
                pltpu.VMEM((2, 2, size_x, 8, size_z), f32),
                pltpu.VMEM((2, size_x, 8, size_z), f32),
                pltpu.VMEM((2, 8, rows), f32),
                pltpu.VMEM((2, 2, 8, rows), f32),
                pltpu.VMEM((1, 2 * HALF), f32),
                pltpu.VMEM((total, 1, 2 * HALF), f32),
                pltpu.VMEM((1, 2 * HALF), f32),
                pltpu.SemaphoreType.DMA((2,)),
                pltpu.SemaphoreType.DMA,
                pltpu.SemaphoreType.DMA((2,)),
                pltpu.SemaphoreType.DMA((2,)),
                pltpu.SemaphoreType.DMA,
                pltpu.SemaphoreType.REGULAR,
            ],
            compiler_params=pltpu.CompilerParams(collective_id=0, has_side_effects=True),
            name="flame",
        )(density, momentum, hydrogen, modes, jnp.asarray(late))
        return tuple(pl.pallas_call(
            write_out,
            out_shape=[jax.ShapeDtypeStruct(local, f32)] * 3,
            in_specs=[pl.BlockSpec(memory_space=pltpu.VMEM)] * 3,
            out_specs=[any_spec] * 3,
            scratch_shapes=[pltpu.SemaphoreType.DMA],
            name="write",
        )(*[pltpu.with_memory_space_constraint(r, pltpu.VMEM) for r in rates]))

    in_specs = (P("gx", "gy", "gz"), P("gx", "gy", "gz"), P("gx", "gy", "gz"), P())
    out_specs = (P("gx", "gy", "gz"), P("gx", "gy", "gz"), P("gx", "gy", "gz"))
    return jax.shard_map(
        per_device, mesh=mesh, in_specs=in_specs, out_specs=out_specs, check_vma=False
    )
```

```python
import functools
import math

import jax
import jax.numpy as jnp
import numpy as np
from jax import lax
from jax.experimental import pallas as pl
from jax.experimental.pallas import tpu as pltpu
from jax.sharding import PartitionSpec as P

KMAX = 3
WIDTH = 2 * KMAX + 1
HALF = 64
ROWS = KMAX + 1
REACH = 4
LOAD_PLANES = 4

FIRST_COEFFS = (0.8, -0.2, 4.0 / 105.0, -1.0 / 280.0)
SECOND_COEFFS = (1.6, -0.2, 8.0 / 315.0, -1.0 / 560.0)
CENTRE_COEFF = -205.0 / 72.0
VISCOSITY = 0.3
DIFFUSIVITY = 1.5
FORCE_POWER = 0.3
ENERGY_EPS = 1e-06
ACTIVATION = 2.0
HIGHEST = lax.Precision.HIGHEST
MESH = pl.DeviceIdType.MESH


def packed_modes():
    reach = range(-KMAX, KMAX + 1)
    cells = [(x, y, z) for z in range(ROWS) for x in reach for y in reach
             if x * x + y * y + z * z <= KMAX * KMAX and (z, x, y) > (0, 0, 0)]
    return cells


def packed_index(place):
    cells = packed_modes()
    result = []
    for part in range(3):
        value = jnp.full(place.shape, cells[0][part], jnp.int32)
        if part == 1:
            value = value + place
        for i in range(1, len(cells)):
            step = cells[i][part] - cells[i - 1][part] - (part == 1)
            if step:
                value = value + jnp.where(place >= i, step, 0)
        result.append(value)
    return result


def tables(size_z):
    band = np.zeros((size_z, size_z))
    halo = np.zeros((16, size_z))
    for z in range(size_z):
        band[z, z] = 3.0 * CENTRE_COEFF
        for offset, weight in enumerate(SECOND_COEFFS, 1):
            for q in (z - offset, z + offset):
                if 0 <= q < size_z:
                    band[q, z] = weight
                elif q < 0:
                    halo[8 + q, z] = weight
                else:
                    halo[8 + q - size_z, z] = weight
    return np.concatenate([halo, band], 0).astype(np.float32)


def polynomial(x, coeffs):
    result = coeffs[-1]
    for c in reversed(coeffs[:-1]):
        result = result * x + c
    return result


SIN_COEFFS = [(-1) ** n * (math.pi / 2) ** (2 * n + 1) / math.factorial(2 * n + 1) for n in range(5)]
COS_COEFFS = [(-1) ** n * (math.pi / 2) ** (2 * n) / math.factorial(2 * n) for n in range(6)]


def cos_sin(quarters):
    turns = jnp.floor(quarters + 0.5)
    d = quarters - turns
    square = d * d
    s = d * polynomial(square, SIN_COEFFS)
    c = polynomial(square, COS_COEFFS)
    half = jnp.floor(0.5 * turns)
    odd = turns - 2.0 * half
    turned = half - 2.0 * jnp.floor(0.5 * half)
    sin_sign = 1.0 - 2.0 * turned
    cos_sign = sin_sign - 2.0 * odd * sin_sign
    swap = odd > 0.5
    return jnp.where(swap, s, c) * cos_sign, jnp.where(swap, c, s) * sin_sign


def split(x):
    high = x.astype(jnp.bfloat16).astype(jnp.float32)
    return high, x - high


def dot_split(a, b, contract):
    return lax.dot_general(a.astype(jnp.bfloat16), b.astype(jnp.bfloat16), (contract, ((), ())),
                           preferred_element_type=jnp.float32)


def column_sum(x):
    x = tree_sum([x[i : i + 8] for i in range(0, x.shape[0], 8)])
    return jnp.sum(x, axis=0, keepdims=True)


def dot_nt(a, b):
    return lax.dot_general(a, b, (((1,), (1,)), ((), ())), precision=HIGHEST, preferred_element_type=jnp.float32)


def dot_nn(a, b):
    return lax.dot_general(a, b, (((1,), (0,)), ((), ())), precision=HIGHEST, preferred_element_type=jnp.float32)


def dot_tn(a, b):
    return lax.dot_general(a, b, (((0,), (0,)), ((), ())), precision=HIGHEST, preferred_element_type=jnp.float32)


def tree_sum(parts):
    parts = list(parts)
    while len(parts) > 1:
        parts = [sum(parts[i : i + 2][1:], parts[i]) for i in range(0, len(parts), 2)]
    return parts[0]


def root_places(sizes):
    places = [(0, 0), (1, 0), (1, max(0, sizes["gz"] // 2 - 1))]
    return [{"gx": x, "gy": 0, "gz": z} for i, (x, z) in enumerate(places) if (x, z) not in places[:i]]


def kernel(sizes, local, dens_hbm, mom_hbm, fuel_hbm, modes_hbm, late_hbm,
           drate, mrate, hrate,
           f, modes, late, cells, along, along_low, across, across_low, edges, sides, ypack, zpack, ztile, own_sum, got_sums, full_sum,
           load_sem, send_sem, halo_recv, z_recv, sum_recv, z_ready, measure):
    size_x, size_y, size_z = local
    rows = size_x * size_y
    me = {a: lax.axis_index(a) for a in sizes}
    count_x, count_y, count_z = sizes["gx"], sizes["gy"], sizes["gz"]
    total = count_x * count_y * count_z
    roots = root_places(sizes)
    rank_of = lambda p: (p["gz"] * count_x + p["gx"]) * count_y + p["gy"]
    rank = rank_of(me)
    root_ranks = [rank_of(r) for r in roots]
    is_root = functools.reduce(jnp.logical_or, [rank == r for r in root_ranks])

    def place_of(i):
        if isinstance(i, int):
            x, y, z = i // count_y % count_x, i % count_y, i // (count_x * count_y)
            return {"gx": jnp.int32(x), "gy": jnp.int32(y), "gz": jnp.int32(z)}
        return {"gx": lax.rem(lax.div(i, count_y), count_x), "gy": lax.rem(i, count_y),
                "gz": lax.div(i, count_x * count_y)}

    def shifted(axis, step):
        return {axis: lax.rem(me[axis] + step % sizes[axis], sizes[axis])}

    own = pl.ds(REACH, size_x)
    load_late = pltpu.make_async_copy(late_hbm, late, load_sem)
    for at in range(0, size_x, LOAD_PLANES):
        for i, src in enumerate((dens_hbm, mom_hbm)):
            pltpu.make_async_copy(
                src.at[pl.ds(at, LOAD_PLANES)], f.at[i, pl.ds(REACH + at, LOAD_PLANES)], load_sem).start()
    load_fuel = pltpu.make_async_copy(fuel_hbm, f.at[2, own], load_sem)
    load_modes = pltpu.make_async_copy(modes_hbm, modes, load_sem)

    barrier = pltpu.get_barrier_semaphore()
    z_steps = (1, -1)
    z_next = [shifted("gz", step)["gz"] for step in z_steps]
    z_lower = [z < me["gz"] for z in z_next]
    y_steps = (1, -1) if count_y > 2 else (1,)
    sides_used = len(y_steps)

    def greet(place):
        pl.semaphore_signal(barrier, inc=1, device_id=place, device_id_type=MESH)

    for step in (1, -1):
        greet(shifted("gx", step))
    for step in y_steps:
        greet(shifted("gy", step))
    for step, lower in zip(z_steps, z_lower):
        @pl.when(jnp.logical_not(lower))
        def _(step=step):
            greet(shifted("gz", step))

    @pl.when(is_root)
    def _():
        def greet_one(i, carry):
            @pl.when(i != rank)
            def _():
                greet(place_of(i))
            return carry
        lax.fori_loop(0, total, greet_one, 0)

    greeters = 2 + sides_used + len(roots) - is_root.astype(jnp.int32)
    for lower in z_lower:
        greeters = greeters + lower.astype(jnp.int32)

    lane = lax.broadcasted_iota(jnp.int32, (1, 2 * HALF), 1)
    kx, ky, kz = packed_index(lax.rem(lane, HALF))
    quarter = (lane >= HALF).astype(jnp.float32)
    kx, ky, kz = [k.astype(jnp.float32) for k in (kx, ky, kz)]

    def quarters(k, place, axis, size):
        part = k * place.astype(jnp.float32) / (size * sizes[axis])
        return 4.0 * (part - jnp.floor(part))

    shift = quarters(kz, me["gz"] * size_z, "gz", size_z) - quarter
    rows_y = me["gy"] * size_y + lax.broadcasted_iota(jnp.int32, (size_y, 1), 0)
    angle_y = quarters(ky, rows_y, "gy", size_y) + shift
    for x in range(size_x):
        c, s = cos_sin(angle_y + quarters(kx, me["gx"] * size_x + x, "gx", size_x))
        cells[x * size_y : (x + 1) * size_y, 0 : 2 * HALF] = c
        cells[x * size_y : (x + 1) * size_y, 2 * HALF : 4 * HALF] = -s
    for z in range(0, size_z, 16):
        rows_at = z + lax.broadcasted_iota(jnp.int32, (16, 1), 0)
        for i, x in enumerate(cos_sin(quarters(kz, rows_at, "gz", size_z))):
            high, rest = split(x)
            along[z : z + 16, 2 * HALF * i : 2 * HALF * (i + 1)] = high.astype(jnp.bfloat16)
            along_low[z : z + 16, 2 * HALF * i : 2 * HALF * (i + 1)] = rest.astype(jnp.bfloat16)

    both_loaded = f.at[pl.ds(0, 2), own]
    pltpu.make_async_copy(both_loaded, both_loaded, load_sem).wait()
    load_fuel.start()
    flat = lambda i: f[i, own].reshape(rows, size_z)
    high, rest = split(flat(1) / flat(0))
    part = dot_split(jnp.concatenate([high, rest], 1), jnp.concatenate([along[...], along[...]], 0), ((1,), (0,)))
    part = part * cells[...] + dot_split(high, along_low[...], ((1,), (0,))) * cells[...]
    cube = column_sum(part[:, 0 : 2 * HALF] + part[:, 2 * HALF : 4 * HALF])
    own_sum[...] = cube
    got_sums[rank] = cube

    pl.semaphore_wait(barrier, greeters)
    def copy_out(src, dst, recv, place):
        return pltpu.make_async_remote_copy(
            src_ref=src, dst_ref=dst, send_sem=send_sem, recv_sem=recv, device_id=place, device_id_type=MESH)

    def spread(i):
        return copy_out(full_sum, full_sum, sum_recv, place_of(i))

    for r in root_ranks:
        @pl.when(rank != r)
        def _(r=r):
            copy_out(own_sum, got_sums.at[rank], sum_recv, place_of(r)).start()

    for step, lower in zip(z_steps, z_lower):
        @pl.when(lower)
        def _(step=step):
            pl.semaphore_signal(z_ready, inc=1, device_id=shifted("gz", step), device_id_type=MESH)

    load_fuel.wait()
    load_late.start()
    halos_x = [
        copy_out(f.at[:, pl.ds(size_x, REACH)], f.at[:, pl.ds(0, REACH)], halo_recv, shifted("gx", 1)),
        copy_out(f.at[:, pl.ds(REACH, REACH)], f.at[:, pl.ds(size_x + REACH, REACH)], halo_recv,
                 shifted("gx", -1)),
    ]
    for copy in halos_x:
        copy.start()
    band_at = 16
    pieces = []
    for i in range(2):
        ypack[i, :, 0:REACH] = f[1 + i, own, 0:REACH]
        ypack[i, :, REACH : 2 * REACH] = f[1 + i, own, size_y - REACH : size_y]
        high, rest = split(flat(1 + i))
        pieces += [high, *split(rest)]
    place = lax.broadcasted_iota(jnp.int32, (8, size_z), 0)
    place = jnp.where(place < REACH, place, place + size_z - 2 * REACH)
    edge = (lax.broadcasted_iota(jnp.int32, (8, size_z), 1) == place).astype(jnp.float32)
    ends = dot_split(edge, jnp.concatenate(pieces, 0), ((1,), (1,)))
    for i in range(2):
        zpack[i] = tree_sum([ends[:, (3 * i + j) * rows : (3 * i + j + 1) * rows] for j in range(3)])
    halos_y = [copy_out(ypack, sides.at[i], halo_recv, shifted("gy", step)) for i, step in enumerate(y_steps)]
    halos_z = [copy_out(zpack, ztile.at[i], z_recv, shifted("gz", step)) for i, step in enumerate(z_steps)]
    for copy, lower in zip(halos_z, z_lower):
        @pl.when(lower)
        def _(copy=copy):
            copy.start()
    for copy in halos_y:
        copy.start()

    load_late.wait()
    load_modes.start()
    lap = [dot_nn(flat(1 + i), late[band_at : band_at + size_z]).reshape(size_x, size_y, size_z) for i in range(2)]
    outs = (drate, mrate, hrate)
    mrate[...] = lap[0]
    hrate[...] = lap[1]

    load_modes.wait()
    count = modes.shape[1]
    code = (modes[0:1] * WIDTH + modes[1:2]) * WIDTH + modes[2:3]
    place = lax.rem(lax.broadcasted_iota(jnp.int32, (2 * HALF, 1), 0), HALF)
    px, py, pz = packed_index(place)
    mine = (px * WIDTH + py) * WIDTH + pz
    used = place < len(packed_modes())
    both_ways = jnp.where(used & (mine == code), 1.0, 0.0) + jnp.where(used & (mine == -code), 1.0, 0.0)
    chosen = dot_nt(jnp.ones((8, count), jnp.float32), both_ways)[0:1]

    ncell = float(rows * size_z * total)
    gain = chosen * (2.0 * FORCE_POWER / ncell)
    for i in range(2):
        here = pl.ds(2 * HALF * i, 2 * HALF)
        across[here] = along[:, here].astype(jnp.float32).T.astype(jnp.bfloat16)
        across_low[here] = along_low[:, here].astype(jnp.float32).T.astype(jnp.bfloat16)

    arrived = [f.at[:, pl.ds(0, 2 * REACH)], sides.at[pl.ds(0, sides_used)]]
    higher = sum(jnp.logical_not(lower).astype(jnp.int32) for lower in z_lower)

    @pl.when(higher > 0)
    def _():
        pl.semaphore_wait(z_ready, higher)

    for copy, lower in zip(halos_z, z_lower):
        @pl.when(jnp.logical_not(lower))
        def _(copy=copy):
            copy.start()

    pltpu.make_async_copy(measure, measure, halo_recv).wait()
    for i in range(2):
        edges[i, :, 0:8] = sides[0, i]
        edges[i, :, 8 : 8 + size_y] = f[1 + i, own]
        edges[i, :, 8 + size_y : 16 + size_y] = sides[sides_used - 1, i]
        total_y = outs[1 + i][...]
        for offset, weight in enumerate(SECOND_COEFFS, 1):
            total_y = total_y + weight * (
                edges[i, :, 8 + offset : 8 + offset + size_y] + edges[i, :, 8 - offset : 8 - offset + size_y])
        outs[1 + i][...] = total_y

    def planes(x, offset):
        return x[REACH + offset : REACH + offset + size_x]

    def first_diff(x):
        result = None
        for offset, weight in enumerate(FIRST_COEFFS, 1):
            term = weight * (planes(x, offset) - planes(x, -offset))
            result = term if result is None else result + term
        return result

    def second_diff(x):
        return tree_sum([w * (planes(x, o) + planes(x, -o)) for o, w in enumerate(SECOND_COEFFS, 1)])

    mom = f[1]
    dens = f[0]
    fuel = f[2]
    vel_pad = mom / dens
    drate[...] = -first_diff(mom)
    mid_fuel = planes(fuel, 0)
    hrate[...] = (DIFFUSIVITY * (hrate[...] + second_diff(fuel)) - first_diff(fuel * vel_pad)
                  - mid_fuel * jnp.exp(-ACTIVATION * mid_fuel / planes(dens, 0)))
    mrate[...] = VISCOSITY * (mrate[...] + second_diff(mom)) - first_diff(mom * vel_pad + dens)

    pltpu.make_async_copy(ztile, ztile, z_recv).wait()
    for i, rate in enumerate((VISCOSITY, DIFFUSIVITY)):
        tile = jnp.concatenate([ztile[0, i], ztile[1, i]], 0)
        outs[1 + i][...] = outs[1 + i][...] + rate * dot_tn(tile, late[0:16]).reshape(size_x, size_y, size_z)

    leaves = [i for i in range(total) if i not in root_ranks]

    @pl.when(is_root)
    def _():
        got = got_sums.at[pl.ds(0, total - 1)]
        pltpu.make_async_copy(got, got, sum_recv).wait()
        full_sum[...] = tree_sum([got_sums[i] for i in range(total)])

    if leaves:
        @pl.when(rank == root_ranks[-1])
        def _():
            for i in reversed(leaves):
                spread(i).start()

        @pl.when(jnp.logical_not(is_root))
        def _():
            pltpu.make_async_copy(full_sum, full_sum, sum_recv).wait()

    cube = full_sum[...]
    coef = cube / ncell
    energy = jnp.sum(chosen * coef * coef, axis=1, keepdims=True)
    scale = 1.0 / (energy + ENERGY_EPS)
    lit = gain * cube
    high, rest = split(cells[...] * jnp.concatenate([lit, lit], 1))
    both = dot_split(high, jnp.concatenate([across[...], across_low[...]], 1), ((1,), (0,)))
    weight = flat(0) * scale
    low = weight * (both[:, 0:size_z] + both[:, size_z:]) + weight * dot_split(rest, across[...], ((1,), (0,)))
    mrate[...] = mrate[...] + low.reshape(size_x, size_y, size_z)

    for sent in (arrived[0], arrived[1], ztile.at[:, :]):
        pltpu.make_async_copy(sent, sent, send_sem).wait()
    for r in root_ranks:
        @pl.when(rank != r)
        def _():
            pltpu.make_async_copy(own_sum, own_sum, send_sem).wait()
    if leaves:
        @pl.when(rank == root_ranks[-1])
        def _():
            sent = got_sums.at[pl.ds(0, len(leaves))]
            pltpu.make_async_copy(sent, sent, send_sem).wait()


def write_out(*refs):
    count = len(refs) // 2
    copies = [pltpu.make_async_copy(refs[i], refs[count + i], refs[-1]) for i in range(count)]
    for copy in copies:
        copy.start()
    for copy in copies:
        copy.wait()


def solution(mesh):
    sizes = {a: mesh.shape[a] for a in ("gx", "gy", "gz")}

    def per_device(density, momentum, hydrogen, forced_modes):
        local = density.shape
        size_x, size_y, size_z = local
        rows = size_x * size_y
        late = tables(size_z)
        modes = forced_modes.T
        total = math.prod(sizes.values())
        halo_bytes = 4 * (3 * 2 * REACH * size_y + (1 + (sizes["gy"] > 2)) * 2 * size_x * 8) * size_z
        any_spec = pl.BlockSpec(memory_space=pl.ANY)
        f32 = jnp.float32
        rates = pl.pallas_call(
            functools.partial(kernel, sizes, local),
            out_shape=[pltpu.VMEM(local, f32)] * 3,
            in_specs=[any_spec] * 5,
            out_specs=[pl.BlockSpec(memory_space=pltpu.VMEM)] * 3,
            scratch_shapes=[
                pltpu.VMEM((3, size_x + 2 * REACH, size_y, size_z), f32),
                pltpu.VMEM(modes.shape, jnp.int32),
                pltpu.VMEM(late.shape, f32),
                pltpu.VMEM((rows, 4 * HALF), f32),
                pltpu.VMEM((size_z, 4 * HALF), jnp.bfloat16),
                pltpu.VMEM((size_z, 4 * HALF), jnp.bfloat16),
                pltpu.VMEM((4 * HALF, size_z), jnp.bfloat16),
                pltpu.VMEM((4 * HALF, size_z), jnp.bfloat16),
                pltpu.VMEM((2, size_x, size_y + 16, size_z), f32),
                pltpu.VMEM((2, 2, size_x, 8, size_z), f32),
                pltpu.VMEM((2, size_x, 8, size_z), f32),
                pltpu.VMEM((2, 8, rows), f32),
                pltpu.VMEM((2, 2, 8, rows), f32),
                pltpu.VMEM((1, 2 * HALF), f32),
                pltpu.VMEM((total, 1, 2 * HALF), f32),
                pltpu.VMEM((1, 2 * HALF), f32),
                pltpu.SemaphoreType.DMA,
                pltpu.SemaphoreType.DMA,
                pltpu.SemaphoreType.DMA,
                pltpu.SemaphoreType.DMA,
                pltpu.SemaphoreType.DMA,
                pltpu.SemaphoreType.REGULAR,
                pltpu.VMEM((halo_bytes // 4096, 8, 128), f32),
            ],
            compiler_params=pltpu.CompilerParams(collective_id=0, has_side_effects=True),
            name="flame",
        )(density, momentum, hydrogen, modes, jnp.asarray(late))
        return tuple(pl.pallas_call(
            write_out,
            out_shape=[jax.ShapeDtypeStruct(local, f32)] * 3,
            in_specs=[pl.BlockSpec(memory_space=pltpu.VMEM)] * 3,
            out_specs=[any_spec] * 3,
            scratch_shapes=[pltpu.SemaphoreType.DMA],
            name="write",
        )(*[pltpu.with_memory_space_constraint(r, pltpu.VMEM) for r in rates]))

    in_specs = (P("gx", "gy", "gz"), P("gx", "gy", "gz"), P("gx", "gy", "gz"), P())
    out_specs = (P("gx", "gy", "gz"), P("gx", "gy", "gz"), P("gx", "gy", "gz"))
    return jax.shard_map(
        per_device, mesh=mesh, in_specs=in_specs, out_specs=out_specs, check_vma=False
    )
```

```python
import functools
import math

import jax
import jax.numpy as jnp
import numpy as np
from jax import lax
from jax.experimental import pallas as pl
from jax.experimental.pallas import tpu as pltpu
from jax.sharding import PartitionSpec as P

KMAX = 3
WIDTH = 2 * KMAX + 1
HALF = 64
ROWS = KMAX + 1
REACH = 4
LOAD_PLANES = 4

FIRST_COEFFS = (0.8, -0.2, 4.0 / 105.0, -1.0 / 280.0)
SECOND_COEFFS = (1.6, -0.2, 8.0 / 315.0, -1.0 / 560.0)
CENTRE_COEFF = -205.0 / 72.0
VISCOSITY = 0.3
DIFFUSIVITY = 1.5
FORCE_POWER = 0.3
ENERGY_EPS = 1e-06
ACTIVATION = 2.0
HIGHEST = lax.Precision.HIGHEST
MESH = pl.DeviceIdType.MESH


def packed_modes():
    reach = range(-KMAX, KMAX + 1)
    cells = [(x, y, z) for z in range(ROWS) for x in reach for y in reach
             if x * x + y * y + z * z <= KMAX * KMAX and (z, x, y) > (0, 0, 0)]
    return cells


def packed_index(place):
    cells = packed_modes()
    result = []
    for part in range(3):
        value = jnp.full(place.shape, cells[0][part], jnp.int32)
        if part == 1:
            value = value + place
        for i in range(1, len(cells)):
            step = cells[i][part] - cells[i - 1][part] - (part == 1)
            if step:
                value = value + jnp.where(place >= i, step, 0)
        result.append(value)
    return result


def tables(size_z):
    band = np.zeros((size_z, size_z))
    halo = np.zeros((16, size_z))
    for z in range(size_z):
        band[z, z] = 3.0 * CENTRE_COEFF
        for offset, weight in enumerate(SECOND_COEFFS, 1):
            for q in (z - offset, z + offset):
                if 0 <= q < size_z:
                    band[q, z] = weight
                elif q < 0:
                    halo[8 + q, z] = weight
                else:
                    halo[8 + q - size_z, z] = weight
    return np.concatenate([halo, band], 0).astype(np.float32)


def polynomial(x, coeffs):
    result = coeffs[-1]
    for c in reversed(coeffs[:-1]):
        result = result * x + c
    return result


SIN_COEFFS = [(-1) ** n * (math.pi / 2) ** (2 * n + 1) / math.factorial(2 * n + 1) for n in range(5)]
COS_COEFFS = [(-1) ** n * (math.pi / 2) ** (2 * n) / math.factorial(2 * n) for n in range(6)]


def cos_sin(quarters):
    turns = jnp.floor(quarters + 0.5)
    d = quarters - turns
    square = d * d
    s = d * polynomial(square, SIN_COEFFS)
    c = polynomial(square, COS_COEFFS)
    half = jnp.floor(0.5 * turns)
    odd = turns - 2.0 * half
    turned = half - 2.0 * jnp.floor(0.5 * half)
    sin_sign = 1.0 - 2.0 * turned
    cos_sign = sin_sign - 2.0 * odd * sin_sign
    swap = odd > 0.5
    return jnp.where(swap, s, c) * cos_sign, jnp.where(swap, c, s) * sin_sign


def split(x):
    high = x.astype(jnp.bfloat16).astype(jnp.float32)
    return high, x - high


def dot_split(a, b, contract):
    return lax.dot_general(a.astype(jnp.bfloat16), b.astype(jnp.bfloat16), (contract, ((), ())),
                           preferred_element_type=jnp.float32)


def column_sum(x):
    x = tree_sum([x[i : i + 8] for i in range(0, x.shape[0], 8)])
    return jnp.sum(x, axis=0, keepdims=True)


def dot_nt(a, b):
    return lax.dot_general(a, b, (((1,), (1,)), ((), ())), precision=HIGHEST, preferred_element_type=jnp.float32)


def dot_nn(a, b):
    return lax.dot_general(a, b, (((1,), (0,)), ((), ())), precision=HIGHEST, preferred_element_type=jnp.float32)


def dot_tn(a, b):
    return lax.dot_general(a, b, (((0,), (0,)), ((), ())), precision=HIGHEST, preferred_element_type=jnp.float32)


def tree_sum(parts):
    parts = list(parts)
    while len(parts) > 1:
        parts = [sum(parts[i : i + 2][1:], parts[i]) for i in range(0, len(parts), 2)]
    return parts[0]


def root_places(sizes):
    places = [(0, 0), (1, 0), (1, max(0, sizes["gz"] // 2 - 1))]
    return [{"gx": x, "gy": 0, "gz": z} for i, (x, z) in enumerate(places) if (x, z) not in places[:i]]


def kernel(sizes, local, dens_hbm, mom_hbm, fuel_hbm, modes_hbm, late_hbm,
           drate, mrate, hrate,
           f, modes, late, cells, along, along_low, across, across_low, edges, sides, ypack, zpack, ztile, own_sum, got_sums, full_sum,
           load_sem, send_sem, halo_recv, z_recv, sum_recv, z_ready, measure):
    size_x, size_y, size_z = local
    rows = size_x * size_y
    me = {a: lax.axis_index(a) for a in sizes}
    count_x, count_y, count_z = sizes["gx"], sizes["gy"], sizes["gz"]
    total = count_x * count_y * count_z
    roots = root_places(sizes)
    rank_of = lambda p: (p["gz"] * count_x + p["gx"]) * count_y + p["gy"]
    rank = rank_of(me)
    root_ranks = [rank_of(r) for r in roots]
    is_root = functools.reduce(jnp.logical_or, [rank == r for r in root_ranks])

    def place_of(i):
        if isinstance(i, int):
            x, y, z = i // count_y % count_x, i % count_y, i // (count_x * count_y)
            return {"gx": jnp.int32(x), "gy": jnp.int32(y), "gz": jnp.int32(z)}
        return {"gx": lax.rem(lax.div(i, count_y), count_x), "gy": lax.rem(i, count_y),
                "gz": lax.div(i, count_x * count_y)}

    def shifted(axis, step):
        return {axis: lax.rem(me[axis] + step % sizes[axis], sizes[axis])}

    own = pl.ds(REACH, size_x)
    load_late = pltpu.make_async_copy(late_hbm, late, load_sem.at[1])
    for at in range(0, size_x, LOAD_PLANES):
        for i, src in enumerate((dens_hbm, mom_hbm)):
            pltpu.make_async_copy(
                src.at[pl.ds(at, LOAD_PLANES)], f.at[i, pl.ds(REACH + at, LOAD_PLANES)], load_sem.at[0]).start()
    load_fuel = pltpu.make_async_copy(fuel_hbm, f.at[2, own], load_sem.at[1])
    load_modes = pltpu.make_async_copy(modes_hbm, modes, load_sem.at[2])

    barrier = pltpu.get_barrier_semaphore()
    z_steps = (1, -1)
    z_next = [shifted("gz", step)["gz"] for step in z_steps]
    z_lower = [z < me["gz"] for z in z_next]
    y_steps = (1, -1) if count_y > 2 else (1,)
    sides_used = len(y_steps)

    def greet(place):
        pl.semaphore_signal(barrier, inc=1, device_id=place, device_id_type=MESH)

    for step in (1, -1):
        greet(shifted("gx", step))
    for step in y_steps:
        greet(shifted("gy", step))
    for step, lower in zip(z_steps, z_lower):
        @pl.when(jnp.logical_not(lower))
        def _(step=step):
            greet(shifted("gz", step))

    @pl.when(is_root)
    def _():
        def greet_one(i, carry):
            @pl.when(i != rank)
            def _():
                greet(place_of(i))
            return carry
        lax.fori_loop(0, total, greet_one, 0)

    greeters = 2 + sides_used + len(roots) - is_root.astype(jnp.int32)
    for lower in z_lower:
        greeters = greeters + lower.astype(jnp.int32)

    lane = lax.broadcasted_iota(jnp.int32, (1, 2 * HALF), 1)
    kx, ky, kz = packed_index(lax.rem(lane, HALF))
    quarter = (lane >= HALF).astype(jnp.float32)
    kx, ky, kz = [k.astype(jnp.float32) for k in (kx, ky, kz)]

    def quarters(k, place, axis, size):
        part = k * place.astype(jnp.float32) / (size * sizes[axis])
        return 4.0 * (part - jnp.floor(part))

    shift = quarters(kz, me["gz"] * size_z, "gz", size_z) - quarter
    rows_y = me["gy"] * size_y + lax.broadcasted_iota(jnp.int32, (size_y, 1), 0)
    angle_y = quarters(ky, rows_y, "gy", size_y) + shift
    for x in range(size_x):
        c, s = cos_sin(angle_y + quarters(kx, me["gx"] * size_x + x, "gx", size_x))
        cells[x * size_y : (x + 1) * size_y, 0 : 2 * HALF] = c
        cells[x * size_y : (x + 1) * size_y, 2 * HALF : 4 * HALF] = -s
    for z in range(0, size_z, 16):
        rows_at = z + lax.broadcasted_iota(jnp.int32, (16, 1), 0)
        for i, x in enumerate(cos_sin(quarters(kz, rows_at, "gz", size_z))):
            high, rest = split(x)
            along[z : z + 16, 2 * HALF * i : 2 * HALF * (i + 1)] = high.astype(jnp.bfloat16)
            along_low[z : z + 16, 2 * HALF * i : 2 * HALF * (i + 1)] = rest.astype(jnp.bfloat16)

    load_fuel.start()
    load_late.start()
    load_modes.start()
    both_loaded = f.at[pl.ds(0, 2), own]
    pltpu.make_async_copy(both_loaded, both_loaded, load_sem.at[0]).wait()
    flat = lambda i: f[i, own].reshape(rows, size_z)
    high, rest = split(flat(1) / flat(0))
    part = dot_split(jnp.concatenate([high, rest], 1), jnp.concatenate([along[...], along[...]], 0), ((1,), (0,)))
    part = part * cells[...] + dot_split(high, along_low[...], ((1,), (0,))) * cells[...]
    cube = column_sum(part[:, 0 : 2 * HALF] + part[:, 2 * HALF : 4 * HALF])
    own_sum[...] = cube
    got_sums[rank] = cube

    pl.semaphore_wait(barrier, greeters)
    def copy_out(src, dst, recv, place):
        return pltpu.make_async_remote_copy(
            src_ref=src, dst_ref=dst, send_sem=send_sem, recv_sem=recv, device_id=place, device_id_type=MESH)

    def spread(i):
        return copy_out(full_sum, full_sum, sum_recv, place_of(i))

    for r in root_ranks:
        @pl.when(rank != r)
        def _(r=r):
            copy_out(own_sum, got_sums.at[rank], sum_recv, place_of(r)).start()

    for step, lower in zip(z_steps, z_lower):
        @pl.when(lower)
        def _(step=step):
            pl.semaphore_signal(z_ready, inc=1, device_id=shifted("gz", step), device_id_type=MESH)

    both_loaded = measure.at[pl.ds(0, (fuel_hbm.size + late_hbm.size) // 1024)]
    pltpu.make_async_copy(both_loaded, both_loaded, load_sem.at[1]).wait()
    halos_x = [
        copy_out(f.at[:, pl.ds(size_x, REACH)], f.at[:, pl.ds(0, REACH)], halo_recv, shifted("gx", 1)),
        copy_out(f.at[:, pl.ds(REACH, REACH)], f.at[:, pl.ds(size_x + REACH, REACH)], halo_recv,
                 shifted("gx", -1)),
    ]
    for copy in halos_x:
        copy.start()
    band_at = 16
    pieces = []
    for i in range(2):
        ypack[i, :, 0:REACH] = f[1 + i, own, 0:REACH]
        ypack[i, :, REACH : 2 * REACH] = f[1 + i, own, size_y - REACH : size_y]
        high, rest = split(flat(1 + i))
        pieces += [high, *split(rest)]
    place = lax.broadcasted_iota(jnp.int32, (8, size_z), 0)
    place = jnp.where(place < REACH, place, place + size_z - 2 * REACH)
    edge = (lax.broadcasted_iota(jnp.int32, (8, size_z), 1) == place).astype(jnp.float32)
    ends = dot_split(edge, jnp.concatenate(pieces, 0), ((1,), (1,)))
    for i in range(2):
        zpack[i] = tree_sum([ends[:, (3 * i + j) * rows : (3 * i + j + 1) * rows] for j in range(3)])
    halos_y = [copy_out(ypack, sides.at[i], halo_recv, shifted("gy", step)) for i, step in enumerate(y_steps)]
    halos_z = [copy_out(zpack, ztile.at[i], z_recv, shifted("gz", step)) for i, step in enumerate(z_steps)]
    for copy, lower in zip(halos_z, z_lower):
        @pl.when(lower)
        def _(copy=copy):
            copy.start()
    for copy in halos_y:
        copy.start()

    lap = [dot_nn(flat(1 + i), late[band_at : band_at + size_z]).reshape(size_x, size_y, size_z) for i in range(2)]
    outs = (drate, mrate, hrate)
    mrate[...] = lap[0]
    hrate[...] = lap[1]

    load_modes.wait()
    count = modes.shape[1]
    code = (modes[0:1] * WIDTH + modes[1:2]) * WIDTH + modes[2:3]
    place = lax.rem(lax.broadcasted_iota(jnp.int32, (2 * HALF, 1), 0), HALF)
    px, py, pz = packed_index(place)
    mine = (px * WIDTH + py) * WIDTH + pz
    used = place < len(packed_modes())
    both_ways = jnp.where(used & (mine == code), 1.0, 0.0) + jnp.where(used & (mine == -code), 1.0, 0.0)
    chosen = dot_nt(jnp.ones((8, count), jnp.float32), both_ways)[0:1]

    ncell = float(rows * size_z * total)
    gain = chosen * (2.0 * FORCE_POWER / ncell)
    for i in range(2):
        here = pl.ds(2 * HALF * i, 2 * HALF)
        across[here] = along[:, here].astype(jnp.float32).T.astype(jnp.bfloat16)
        across_low[here] = along_low[:, here].astype(jnp.float32).T.astype(jnp.bfloat16)

    arrived = [f.at[:, pl.ds(0, 2 * REACH)], sides.at[pl.ds(0, sides_used)]]
    higher = sum(jnp.logical_not(lower).astype(jnp.int32) for lower in z_lower)

    @pl.when(higher > 0)
    def _():
        pl.semaphore_wait(z_ready, higher)

    for copy, lower in zip(halos_z, z_lower):
        @pl.when(jnp.logical_not(lower))
        def _(copy=copy):
            copy.start()

    pltpu.make_async_copy(measure, measure, halo_recv).wait()
    for i in range(2):
        edges[i, :, 0:8] = sides[0, i]
        edges[i, :, 8 : 8 + size_y] = f[1 + i, own]
        edges[i, :, 8 + size_y : 16 + size_y] = sides[sides_used - 1, i]
        total_y = outs[1 + i][...]
        for offset, weight in enumerate(SECOND_COEFFS, 1):
            total_y = total_y + weight * (
                edges[i, :, 8 + offset : 8 + offset + size_y] + edges[i, :, 8 - offset : 8 - offset + size_y])
        outs[1 + i][...] = total_y

    def planes(x, offset):
        return x[REACH + offset : REACH + offset + size_x]

    def first_diff(x):
        result = None
        for offset, weight in enumerate(FIRST_COEFFS, 1):
            term = weight * (planes(x, offset) - planes(x, -offset))
            result = term if result is None else result + term
        return result

    def second_diff(x):
        return tree_sum([w * (planes(x, o) + planes(x, -o)) for o, w in enumerate(SECOND_COEFFS, 1)])

    mom = f[1]
    dens = f[0]
    fuel = f[2]
    vel_pad = mom / dens
    drate[...] = -first_diff(mom)
    mid_fuel = planes(fuel, 0)
    hrate[...] = (DIFFUSIVITY * (hrate[...] + second_diff(fuel)) - first_diff(fuel * vel_pad)
                  - mid_fuel * jnp.exp(-ACTIVATION * mid_fuel / planes(dens, 0)))
    mrate[...] = VISCOSITY * (mrate[...] + second_diff(mom)) - first_diff(mom * vel_pad + dens)

    pltpu.make_async_copy(ztile, ztile, z_recv).wait()
    for i, rate in enumerate((VISCOSITY, DIFFUSIVITY)):
        tile = jnp.concatenate([ztile[0, i], ztile[1, i]], 0)
        outs[1 + i][...] = outs[1 + i][...] + rate * dot_tn(tile, late[0:16]).reshape(size_x, size_y, size_z)

    leaves = [i for i in range(total) if i not in root_ranks]

    @pl.when(is_root)
    def _():
        got = got_sums.at[pl.ds(0, total - 1)]
        pltpu.make_async_copy(got, got, sum_recv).wait()
        full_sum[...] = tree_sum([got_sums[i] for i in range(total)])

    if leaves:
        @pl.when(rank == root_ranks[-1])
        def _():
            for i in reversed(leaves):
                spread(i).start()

        @pl.when(jnp.logical_not(is_root))
        def _():
            pltpu.make_async_copy(full_sum, full_sum, sum_recv).wait()

    cube = full_sum[...]
    coef = cube / ncell
    energy = jnp.sum(chosen * coef * coef, axis=1, keepdims=True)
    scale = 1.0 / (energy + ENERGY_EPS)
    lit = gain * cube
    high, rest = split(cells[...] * jnp.concatenate([lit, lit], 1))
    both = dot_split(high, jnp.concatenate([across[...], across_low[...]], 1), ((1,), (0,)))
    weight = flat(0) * scale
    low = weight * (both[:, 0:size_z] + both[:, size_z:]) + weight * dot_split(rest, across[...], ((1,), (0,)))
    mrate[...] = mrate[...] + low.reshape(size_x, size_y, size_z)

    for sent in (arrived[0], arrived[1], ztile.at[:, :]):
        pltpu.make_async_copy(sent, sent, send_sem).wait()
    for r in root_ranks:
        @pl.when(rank != r)
        def _():
            pltpu.make_async_copy(own_sum, own_sum, send_sem).wait()
    if leaves:
        @pl.when(rank == root_ranks[-1])
        def _():
            sent = got_sums.at[pl.ds(0, len(leaves))]
            pltpu.make_async_copy(sent, sent, send_sem).wait()


def write_out(*refs):
    count = len(refs) // 2
    copies = [pltpu.make_async_copy(refs[i], refs[count + i], refs[-1]) for i in range(count)]
    for copy in copies:
        copy.start()
    for copy in copies:
        copy.wait()


def solution(mesh):
    sizes = {a: mesh.shape[a] for a in ("gx", "gy", "gz")}

    def per_device(density, momentum, hydrogen, forced_modes):
        local = density.shape
        size_x, size_y, size_z = local
        rows = size_x * size_y
        late = tables(size_z)
        modes = forced_modes.T
        total = math.prod(sizes.values())
        halo_bytes = 4 * (3 * 2 * REACH * size_y + (1 + (sizes["gy"] > 2)) * 2 * size_x * 8) * size_z
        any_spec = pl.BlockSpec(memory_space=pl.ANY)
        f32 = jnp.float32
        rates = pl.pallas_call(
            functools.partial(kernel, sizes, local),
            out_shape=[pltpu.VMEM(local, f32)] * 3,
            in_specs=[any_spec] * 5,
            out_specs=[pl.BlockSpec(memory_space=pltpu.VMEM)] * 3,
            scratch_shapes=[
                pltpu.VMEM((3, size_x + 2 * REACH, size_y, size_z), f32),
                pltpu.VMEM(modes.shape, jnp.int32),
                pltpu.VMEM(late.shape, f32),
                pltpu.VMEM((rows, 4 * HALF), f32),
                pltpu.VMEM((size_z, 4 * HALF), jnp.bfloat16),
                pltpu.VMEM((size_z, 4 * HALF), jnp.bfloat16),
                pltpu.VMEM((4 * HALF, size_z), jnp.bfloat16),
                pltpu.VMEM((4 * HALF, size_z), jnp.bfloat16),
                pltpu.VMEM((2, size_x, size_y + 16, size_z), f32),
                pltpu.VMEM((2, 2, size_x, 8, size_z), f32),
                pltpu.VMEM((2, size_x, 8, size_z), f32),
                pltpu.VMEM((2, 8, rows), f32),
                pltpu.VMEM((2, 2, 8, rows), f32),
                pltpu.VMEM((1, 2 * HALF), f32),
                pltpu.VMEM((total, 1, 2 * HALF), f32),
                pltpu.VMEM((1, 2 * HALF), f32),
                pltpu.SemaphoreType.DMA((3,)),
                pltpu.SemaphoreType.DMA,
                pltpu.SemaphoreType.DMA,
                pltpu.SemaphoreType.DMA,
                pltpu.SemaphoreType.DMA,
                pltpu.SemaphoreType.REGULAR,
                pltpu.VMEM((halo_bytes // 4096, 8, 128), f32),
            ],
            compiler_params=pltpu.CompilerParams(collective_id=0, has_side_effects=True),
            name="flame",
        )(density, momentum, hydrogen, modes, jnp.asarray(late))
        return tuple(pl.pallas_call(
            write_out,
            out_shape=[jax.ShapeDtypeStruct(local, f32)] * 3,
            in_specs=[pl.BlockSpec(memory_space=pltpu.VMEM)] * 3,
            out_specs=[any_spec] * 3,
            scratch_shapes=[pltpu.SemaphoreType.DMA],
            name="write",
        )(*[pltpu.with_memory_space_constraint(r, pltpu.VMEM) for r in rates]))

    in_specs = (P("gx", "gy", "gz"), P("gx", "gy", "gz"), P("gx", "gy", "gz"), P())
    out_specs = (P("gx", "gy", "gz"), P("gx", "gy", "gz"), P("gx", "gy", "gz"))
    return jax.shard_map(
        per_device, mesh=mesh, in_specs=in_specs, out_specs=out_specs, check_vma=False
    )
```

```python
import functools
import math

import jax
import jax.numpy as jnp
import numpy as np
from jax import lax
from jax.experimental import pallas as pl
from jax.experimental.pallas import tpu as pltpu
from jax.sharding import PartitionSpec as P

KMAX = 3
WIDTH = 2 * KMAX + 1
HALF = 64
ROWS = KMAX + 1
REACH = 4
LOAD_PLANES = 4

FIRST_COEFFS = (0.8, -0.2, 4.0 / 105.0, -1.0 / 280.0)
SECOND_COEFFS = (1.6, -0.2, 8.0 / 315.0, -1.0 / 560.0)
CENTRE_COEFF = -205.0 / 72.0
VISCOSITY = 0.3
DIFFUSIVITY = 1.5
FORCE_POWER = 0.3
ENERGY_EPS = 1e-06
ACTIVATION = 2.0
HIGHEST = lax.Precision.HIGHEST
MESH = pl.DeviceIdType.MESH


def packed_modes():
    reach = range(-KMAX, KMAX + 1)
    cells = [(x, y, z) for z in range(ROWS) for x in reach for y in reach
             if x * x + y * y + z * z <= KMAX * KMAX and (z, x, y) > (0, 0, 0)]
    return cells


def packed_index(place):
    cells = packed_modes()
    result = []
    for part in range(3):
        value = jnp.full(place.shape, cells[0][part], jnp.int32)
        if part == 1:
            value = value + place
        for i in range(1, len(cells)):
            step = cells[i][part] - cells[i - 1][part] - (part == 1)
            if step:
                value = value + jnp.where(place >= i, step, 0)
        result.append(value)
    return result


def tables(size_z):
    band = np.zeros((size_z, size_z))
    halo = np.zeros((16, size_z))
    for z in range(size_z):
        band[z, z] = 3.0 * CENTRE_COEFF
        for offset, weight in enumerate(SECOND_COEFFS, 1):
            for q in (z - offset, z + offset):
                if 0 <= q < size_z:
                    band[q, z] = weight
                elif q < 0:
                    halo[8 + q, z] = weight
                else:
                    halo[8 + q - size_z, z] = weight
    return np.concatenate([halo, band], 0).astype(np.float32)


def polynomial(x, coeffs):
    result = coeffs[-1]
    for c in reversed(coeffs[:-1]):
        result = result * x + c
    return result


SIN_COEFFS = [(-1) ** n * (math.pi / 2) ** (2 * n + 1) / math.factorial(2 * n + 1) for n in range(5)]
COS_COEFFS = [(-1) ** n * (math.pi / 2) ** (2 * n) / math.factorial(2 * n) for n in range(6)]


def cos_sin(quarters):
    turns = jnp.floor(quarters + 0.5)
    d = quarters - turns
    square = d * d
    s = d * polynomial(square, SIN_COEFFS)
    c = polynomial(square, COS_COEFFS)
    half = jnp.floor(0.5 * turns)
    odd = turns - 2.0 * half
    turned = half - 2.0 * jnp.floor(0.5 * half)
    sin_sign = 1.0 - 2.0 * turned
    cos_sign = sin_sign - 2.0 * odd * sin_sign
    swap = odd > 0.5
    return jnp.where(swap, s, c) * cos_sign, jnp.where(swap, c, s) * sin_sign


def split(x):
    high = x.astype(jnp.bfloat16).astype(jnp.float32)
    return high, x - high


def dot_split(a, b, contract):
    return lax.dot_general(a.astype(jnp.bfloat16), b.astype(jnp.bfloat16), (contract, ((), ())),
                           preferred_element_type=jnp.float32)


def column_sum(x):
    x = tree_sum([x[i : i + 8] for i in range(0, x.shape[0], 8)])
    return jnp.sum(x, axis=0, keepdims=True)


def dot_nt(a, b):
    return lax.dot_general(a, b, (((1,), (1,)), ((), ())), precision=HIGHEST, preferred_element_type=jnp.float32)


def dot_nn(a, b):
    return lax.dot_general(a, b, (((1,), (0,)), ((), ())), precision=HIGHEST, preferred_element_type=jnp.float32)


def dot_tn(a, b):
    return lax.dot_general(a, b, (((0,), (0,)), ((), ())), precision=HIGHEST, preferred_element_type=jnp.float32)


def tree_sum(parts):
    parts = list(parts)
    while len(parts) > 1:
        parts = [sum(parts[i : i + 2][1:], parts[i]) for i in range(0, len(parts), 2)]
    return parts[0]


def root_places(sizes):
    places = [(0, 0), (1, 0), (1, max(0, sizes["gz"] // 2 - 1))]
    return [{"gx": x, "gy": 0, "gz": z} for i, (x, z) in enumerate(places) if (x, z) not in places[:i]]


def kernel(sizes, local, dens_hbm, mom_hbm, fuel_hbm, modes_hbm, late_hbm,
           drate, mrate, hrate,
           f, modes, late, cells, along, along_low, across, across_low, edges, sides, ypack, zpack, ztile, own_sum, got_sums, full_sum,
           halo_recv, z_recv, sum_recv, z_ready, measure, load_sem, send_sem):
    size_x, size_y, size_z = local
    rows = size_x * size_y
    me = {a: lax.axis_index(a) for a in sizes}
    count_x, count_y, count_z = sizes["gx"], sizes["gy"], sizes["gz"]
    total = count_x * count_y * count_z
    roots = root_places(sizes)
    rank_of = lambda p: (p["gz"] * count_x + p["gx"]) * count_y + p["gy"]
    rank = rank_of(me)
    root_ranks = [rank_of(r) for r in roots]
    is_root = functools.reduce(jnp.logical_or, [rank == r for r in root_ranks])

    def place_of(i):
        if isinstance(i, int):
            x, y, z = i // count_y % count_x, i % count_y, i // (count_x * count_y)
            return {"gx": jnp.int32(x), "gy": jnp.int32(y), "gz": jnp.int32(z)}
        return {"gx": lax.rem(lax.div(i, count_y), count_x), "gy": lax.rem(i, count_y),
                "gz": lax.div(i, count_x * count_y)}

    def shifted(axis, step):
        return {axis: lax.rem(me[axis] + step % sizes[axis], sizes[axis])}

    own = pl.ds(REACH, size_x)
    load_late = pltpu.make_async_copy(late_hbm, late, load_sem.at[1])
    for at in range(0, size_x, LOAD_PLANES):
        for i, src in enumerate((dens_hbm, mom_hbm)):
            pltpu.make_async_copy(
                src.at[pl.ds(at, LOAD_PLANES)], f.at[i, pl.ds(REACH + at, LOAD_PLANES)], load_sem.at[0]).start()
    load_fuel = pltpu.make_async_copy(fuel_hbm, f.at[2, own], load_sem.at[1])
    load_modes = pltpu.make_async_copy(modes_hbm, modes, load_sem.at[2])

    barrier = pltpu.get_barrier_semaphore()
    z_steps = (1, -1)
    z_next = [shifted("gz", step)["gz"] for step in z_steps]
    z_lower = [z < me["gz"] for z in z_next]
    y_steps = (1, -1) if count_y > 2 else (1,)
    sides_used = len(y_steps)

    def greet(place):
        pl.semaphore_signal(barrier, inc=1, device_id=place, device_id_type=MESH)

    for step in (1, -1):
        greet(shifted("gx", step))
    for step in y_steps:
        greet(shifted("gy", step))
    for step, lower in zip(z_steps, z_lower):
        @pl.when(jnp.logical_not(lower))
        def _(step=step):
            greet(shifted("gz", step))

    @pl.when(is_root)
    def _():
        def greet_one(i, carry):
            @pl.when(i != rank)
            def _():
                greet(place_of(i))
            return carry
        lax.fori_loop(0, total, greet_one, 0)

    greeters = 2 + sides_used + len(roots) - is_root.astype(jnp.int32)
    for lower in z_lower:
        greeters = greeters + lower.astype(jnp.int32)

    lane = lax.broadcasted_iota(jnp.int32, (1, 2 * HALF), 1)
    kx, ky, kz = packed_index(lax.rem(lane, HALF))
    quarter = (lane >= HALF).astype(jnp.float32)
    kx, ky, kz = [k.astype(jnp.float32) for k in (kx, ky, kz)]

    def quarters(k, place, axis, size):
        part = k * place.astype(jnp.float32) / (size * sizes[axis])
        return 4.0 * (part - jnp.floor(part))

    shift = quarters(kz, me["gz"] * size_z, "gz", size_z) - quarter
    rows_y = me["gy"] * size_y + lax.broadcasted_iota(jnp.int32, (size_y, 1), 0)
    angle_y = quarters(ky, rows_y, "gy", size_y) + shift
    for x in range(size_x):
        c, s = cos_sin(angle_y + quarters(kx, me["gx"] * size_x + x, "gx", size_x))
        cells[x * size_y : (x + 1) * size_y, 0 : 2 * HALF] = c
        cells[x * size_y : (x + 1) * size_y, 2 * HALF : 4 * HALF] = -s
    for z in range(0, size_z, 16):
        rows_at = z + lax.broadcasted_iota(jnp.int32, (16, 1), 0)
        for i, x in enumerate(cos_sin(quarters(kz, rows_at, "gz", size_z))):
            high, rest = split(x)
            along[z : z + 16, 2 * HALF * i : 2 * HALF * (i + 1)] = high.astype(jnp.bfloat16)
            along_low[z : z + 16, 2 * HALF * i : 2 * HALF * (i + 1)] = rest.astype(jnp.bfloat16)

    load_fuel.start()
    load_late.start()
    load_modes.start()
    both_loaded = f.at[pl.ds(0, 2), own]
    pltpu.make_async_copy(both_loaded, both_loaded, load_sem.at[0]).wait()
    flat = lambda i: f[i, own].reshape(rows, size_z)
    high, rest = split(flat(1) / flat(0))
    part = dot_split(jnp.concatenate([high, rest], 1), jnp.concatenate([along[...], along[...]], 0), ((1,), (0,)))
    part = part * cells[...] + dot_split(high, along_low[...], ((1,), (0,))) * cells[...]
    cube = column_sum(part[:, 0 : 2 * HALF] + part[:, 2 * HALF : 4 * HALF])
    own_sum[...] = cube
    got_sums[rank] = cube

    pl.semaphore_wait(barrier, greeters)
    def copy_out(src, dst, recv, place):
        return pltpu.make_async_remote_copy(
            src_ref=src, dst_ref=dst, send_sem=send_sem, recv_sem=recv, device_id=place, device_id_type=MESH)

    def spread(i):
        return copy_out(full_sum, full_sum, sum_recv, place_of(i))

    for r in root_ranks:
        @pl.when(rank != r)
        def _(r=r):
            copy_out(own_sum, got_sums.at[rank], sum_recv, place_of(r)).start()

    for step, lower in zip(z_steps, z_lower):
        @pl.when(lower)
        def _(step=step):
            pl.semaphore_signal(z_ready, inc=1, device_id=shifted("gz", step), device_id_type=MESH)

    both_loaded = measure.at[pl.ds(0, (fuel_hbm.size + late_hbm.size) // 1024)]
    pltpu.make_async_copy(both_loaded, both_loaded, load_sem.at[1]).wait()
    halos_x = [
        copy_out(f.at[:, pl.ds(size_x, REACH)], f.at[:, pl.ds(0, REACH)], halo_recv, shifted("gx", 1)),
        copy_out(f.at[:, pl.ds(REACH, REACH)], f.at[:, pl.ds(size_x + REACH, REACH)], halo_recv,
                 shifted("gx", -1)),
    ]
    for copy in halos_x:
        copy.start()
    band_at = 16
    pieces = []
    for i in range(2):
        ypack[i, :, 0:REACH] = f[1 + i, own, 0:REACH]
        ypack[i, :, REACH : 2 * REACH] = f[1 + i, own, size_y - REACH : size_y]
        high, rest = split(flat(1 + i))
        pieces += [high, *split(rest)]
    place = lax.broadcasted_iota(jnp.int32, (8, size_z), 0)
    place = jnp.where(place < REACH, place, place + size_z - 2 * REACH)
    edge = (lax.broadcasted_iota(jnp.int32, (8, size_z), 1) == place).astype(jnp.float32)
    ends = dot_split(edge, jnp.concatenate(pieces, 0), ((1,), (1,)))
    for i in range(2):
        zpack[i] = tree_sum([ends[:, (3 * i + j) * rows : (3 * i + j + 1) * rows] for j in range(3)])
    halos_y = [copy_out(ypack, sides.at[i], halo_recv, shifted("gy", step)) for i, step in enumerate(y_steps)]
    halos_z = [copy_out(zpack, ztile.at[i], z_recv, shifted("gz", step)) for i, step in enumerate(z_steps)]
    for copy, lower in zip(halos_z, z_lower):
        @pl.when(lower)
        def _(copy=copy):
            copy.start()
    for copy in halos_y:
        copy.start()

    lap = [dot_nn(flat(1 + i), late[band_at : band_at + size_z]).reshape(size_x, size_y, size_z) for i in range(2)]
    outs = (drate, mrate, hrate)
    mrate[...] = lap[0]
    hrate[...] = lap[1]

    load_modes.wait()
    count = modes.shape[1]
    code = (modes[0:1] * WIDTH + modes[1:2]) * WIDTH + modes[2:3]
    place = lax.rem(lax.broadcasted_iota(jnp.int32, (2 * HALF, 1), 0), HALF)
    px, py, pz = packed_index(place)
    mine = (px * WIDTH + py) * WIDTH + pz
    used = place < len(packed_modes())
    both_ways = jnp.where(used & (mine == code), 1.0, 0.0) + jnp.where(used & (mine == -code), 1.0, 0.0)
    chosen = dot_nt(jnp.ones((8, count), jnp.float32), both_ways)[0:1]

    ncell = float(rows * size_z * total)
    gain = chosen * (2.0 * FORCE_POWER / ncell)
    for i in range(2):
        here = pl.ds(2 * HALF * i, 2 * HALF)
        across[here] = along[:, here].astype(jnp.float32).T.astype(jnp.bfloat16)
        across_low[here] = along_low[:, here].astype(jnp.float32).T.astype(jnp.bfloat16)

    arrived = [f.at[:, pl.ds(0, 2 * REACH)], sides.at[pl.ds(0, sides_used)]]
    higher = sum(jnp.logical_not(lower).astype(jnp.int32) for lower in z_lower)

    @pl.when(higher > 0)
    def _():
        pl.semaphore_wait(z_ready, higher)

    for copy, lower in zip(halos_z, z_lower):
        @pl.when(jnp.logical_not(lower))
        def _(copy=copy):
            copy.start()

    pltpu.make_async_copy(measure, measure, halo_recv).wait()
    for i in range(2):
        edges[i, :, 0:8] = sides[0, i]
        edges[i, :, 8 : 8 + size_y] = f[1 + i, own]
        edges[i, :, 8 + size_y : 16 + size_y] = sides[sides_used - 1, i]
        total_y = outs[1 + i][...]
        for offset, weight in enumerate(SECOND_COEFFS, 1):
            total_y = total_y + weight * (
                edges[i, :, 8 + offset : 8 + offset + size_y] + edges[i, :, 8 - offset : 8 - offset + size_y])
        outs[1 + i][...] = total_y

    def planes(x, offset):
        return x[REACH + offset : REACH + offset + size_x]

    def first_diff(x):
        result = None
        for offset, weight in enumerate(FIRST_COEFFS, 1):
            term = weight * (planes(x, offset) - planes(x, -offset))
            result = term if result is None else result + term
        return result

    def second_diff(x):
        return tree_sum([w * (planes(x, o) + planes(x, -o)) for o, w in enumerate(SECOND_COEFFS, 1)])

    mom = f[1]
    dens = f[0]
    fuel = f[2]
    vel_pad = mom / dens
    drate[...] = -first_diff(mom)
    mid_fuel = planes(fuel, 0)
    hrate[...] = (DIFFUSIVITY * (hrate[...] + second_diff(fuel)) - first_diff(fuel * vel_pad)
                  - mid_fuel * jnp.exp(-ACTIVATION * mid_fuel / planes(dens, 0)))
    mrate[...] = VISCOSITY * (mrate[...] + second_diff(mom)) - first_diff(mom * vel_pad + dens)

    pltpu.make_async_copy(ztile, ztile, z_recv).wait()
    for i, rate in enumerate((VISCOSITY, DIFFUSIVITY)):
        tile = jnp.concatenate([ztile[0, i], ztile[1, i]], 0)
        outs[1 + i][...] = outs[1 + i][...] + rate * dot_tn(tile, late[0:16]).reshape(size_x, size_y, size_z)

    leaves = [i for i in range(total) if i not in root_ranks]

    @pl.when(is_root)
    def _():
        got = got_sums.at[pl.ds(0, total - 1)]
        pltpu.make_async_copy(got, got, sum_recv).wait()

    @pl.when(jnp.logical_not(is_root))
    def _():
        pltpu.make_async_copy(full_sum, full_sum, sum_recv).wait()

    cube = jnp.where(is_root, tree_sum([got_sums[i] for i in range(total)]), full_sum[...])

    @pl.when(rank == root_ranks[-1])
    def _():
        full_sum[...] = cube
        for i in reversed(leaves):
            spread(i).start()

    coef = cube / ncell
    energy = jnp.sum(chosen * coef * coef, axis=1, keepdims=True)
    scale = 1.0 / (energy + ENERGY_EPS)
    lit = gain * cube
    high, rest = split(cells[...] * jnp.concatenate([lit, lit], 1))
    both = dot_split(high, jnp.concatenate([across[...], across_low[...]], 1), ((1,), (0,)))
    weight = flat(0) * scale
    low = weight * (both[:, 0:size_z] + both[:, size_z:]) + weight * dot_split(rest, across[...], ((1,), (0,)))
    mrate[...] = mrate[...] + low.reshape(size_x, size_y, size_z)

    for sent in (arrived[0], arrived[1], ztile.at[:, :]):
        pltpu.make_async_copy(sent, sent, send_sem).wait()
    for r in root_ranks:
        @pl.when(rank != r)
        def _():
            pltpu.make_async_copy(own_sum, own_sum, send_sem).wait()
    if leaves:
        @pl.when(rank == root_ranks[-1])
        def _():
            sent = got_sums.at[pl.ds(0, len(leaves))]
            pltpu.make_async_copy(sent, sent, send_sem).wait()


def scoped_kernel(sizes, local, *refs):
    pl.run_scoped(functools.partial(kernel, sizes, local, *refs),
                  pltpu.SemaphoreType.DMA((3,)), pltpu.SemaphoreType.DMA)


def write_out(*refs):
    count = len(refs) // 2
    copies = [pltpu.make_async_copy(refs[i], refs[count + i], refs[-1]) for i in range(count)]
    for copy in copies:
        copy.start()
    for copy in copies:
        copy.wait()


def solution(mesh):
    sizes = {a: mesh.shape[a] for a in ("gx", "gy", "gz")}

    def per_device(density, momentum, hydrogen, forced_modes):
        local = density.shape
        size_x, size_y, size_z = local
        rows = size_x * size_y
        late = tables(size_z)
        modes = forced_modes.T
        total = math.prod(sizes.values())
        halo_bytes = 4 * (3 * 2 * REACH * size_y + (1 + (sizes["gy"] > 2)) * 2 * size_x * 8) * size_z
        any_spec = pl.BlockSpec(memory_space=pl.ANY)
        f32 = jnp.float32
        rates = pl.pallas_call(
            functools.partial(scoped_kernel, sizes, local),
            out_shape=[pltpu.VMEM(local, f32)] * 3,
            in_specs=[any_spec] * 5,
            out_specs=[pl.BlockSpec(memory_space=pltpu.VMEM)] * 3,
            scratch_shapes=[
                pltpu.VMEM((3, size_x + 2 * REACH, size_y, size_z), f32),
                pltpu.VMEM(modes.shape, jnp.int32),
                pltpu.VMEM(late.shape, f32),
                pltpu.VMEM((rows, 4 * HALF), f32),
                pltpu.VMEM((size_z, 4 * HALF), jnp.bfloat16),
                pltpu.VMEM((size_z, 4 * HALF), jnp.bfloat16),
                pltpu.VMEM((4 * HALF, size_z), jnp.bfloat16),
                pltpu.VMEM((4 * HALF, size_z), jnp.bfloat16),
                pltpu.VMEM((2, size_x, size_y + 16, size_z), f32),
                pltpu.VMEM((2, 2, size_x, 8, size_z), f32),
                pltpu.VMEM((2, size_x, 8, size_z), f32),
                pltpu.VMEM((2, 8, rows), f32),
                pltpu.VMEM((2, 2, 8, rows), f32),
                pltpu.VMEM((1, 2 * HALF), f32),
                pltpu.VMEM((total, 1, 2 * HALF), f32),
                pltpu.VMEM((1, 2 * HALF), f32),
                pltpu.SemaphoreType.DMA,
                pltpu.SemaphoreType.DMA,
                pltpu.SemaphoreType.DMA,
                pltpu.SemaphoreType.REGULAR,
                pltpu.VMEM((halo_bytes // 4096, 8, 128), f32),
            ],
            compiler_params=pltpu.CompilerParams(collective_id=0, has_side_effects=True),
            name="flame",
        )(density, momentum, hydrogen, modes, jnp.asarray(late))
        return tuple(pl.pallas_call(
            write_out,
            out_shape=[jax.ShapeDtypeStruct(local, f32)] * 3,
            in_specs=[pl.BlockSpec(memory_space=pltpu.VMEM)] * 3,
            out_specs=[any_spec] * 3,
            scratch_shapes=[pltpu.SemaphoreType.DMA],
            name="write",
        )(*[pltpu.with_memory_space_constraint(r, pltpu.VMEM) for r in rates]))

    in_specs = (P("gx", "gy", "gz"), P("gx", "gy", "gz"), P("gx", "gy", "gz"), P())
    out_specs = (P("gx", "gy", "gz"), P("gx", "gy", "gz"), P("gx", "gy", "gz"))
    return jax.shard_map(
        per_device, mesh=mesh, in_specs=in_specs, out_specs=out_specs, check_vma=False
    )
```

```python
import functools
import math

import jax
import jax.numpy as jnp
import numpy as np
from jax import lax
from jax.experimental import pallas as pl
from jax.experimental.pallas import tpu as pltpu
from jax.sharding import PartitionSpec as P

KMAX = 3
WIDTH = 2 * KMAX + 1
HALF = 64
ROWS = KMAX + 1
REACH = 4
LOAD_PLANES = 4

FIRST_COEFFS = (0.8, -0.2, 4.0 / 105.0, -1.0 / 280.0)
SECOND_COEFFS = (1.6, -0.2, 8.0 / 315.0, -1.0 / 560.0)
CENTRE_COEFF = -205.0 / 72.0
VISCOSITY = 0.3
DIFFUSIVITY = 1.5
FORCE_POWER = 0.3
ENERGY_EPS = 1e-06
ACTIVATION = 2.0
HIGHEST = lax.Precision.HIGHEST
MESH = pl.DeviceIdType.MESH


def packed_modes():
    reach = range(-KMAX, KMAX + 1)
    cells = [(x, y, z) for z in range(ROWS) for x in reach for y in reach
             if x * x + y * y + z * z <= KMAX * KMAX and (z, x, y) > (0, 0, 0)]
    return cells


def packed_index(place):
    cells = packed_modes()
    result = []
    for part in range(3):
        value = jnp.full(place.shape, cells[0][part], jnp.int32)
        if part == 1:
            value = value + place
        for i in range(1, len(cells)):
            step = cells[i][part] - cells[i - 1][part] - (part == 1)
            if step:
                value = value + jnp.where(place >= i, step, 0)
        result.append(value)
    return result


def tables(size_z):
    band = np.zeros((size_z, size_z))
    halo = np.zeros((16, size_z))
    for z in range(size_z):
        band[z, z] = 3.0 * CENTRE_COEFF
        for offset, weight in enumerate(SECOND_COEFFS, 1):
            for q in (z - offset, z + offset):
                if 0 <= q < size_z:
                    band[q, z] = weight
                elif q < 0:
                    halo[8 + q, z] = weight
                else:
                    halo[8 + q - size_z, z] = weight
    return np.concatenate([halo, band], 0).astype(np.float32)


def polynomial(x, coeffs):
    result = coeffs[-1]
    for c in reversed(coeffs[:-1]):
        result = result * x + c
    return result


SIN_COEFFS = [(-1) ** n * (math.pi / 2) ** (2 * n + 1) / math.factorial(2 * n + 1) for n in range(5)]
COS_COEFFS = [(-1) ** n * (math.pi / 2) ** (2 * n) / math.factorial(2 * n) for n in range(6)]


def cos_sin(quarters):
    turns = jnp.floor(quarters + 0.5)
    d = quarters - turns
    square = d * d
    s = d * polynomial(square, SIN_COEFFS)
    c = polynomial(square, COS_COEFFS)
    half = jnp.floor(0.5 * turns)
    odd = turns - 2.0 * half
    turned = half - 2.0 * jnp.floor(0.5 * half)
    sin_sign = 1.0 - 2.0 * turned
    cos_sign = sin_sign - 2.0 * odd * sin_sign
    swap = odd > 0.5
    return jnp.where(swap, s, c) * cos_sign, jnp.where(swap, c, s) * sin_sign


def split(x):
    high = x.astype(jnp.bfloat16).astype(jnp.float32)
    return high, x - high


def dot_split(a, b, contract):
    return lax.dot_general(a.astype(jnp.bfloat16), b.astype(jnp.bfloat16), (contract, ((), ())),
                           preferred_element_type=jnp.float32)


def column_sum(x):
    x = tree_sum([x[i : i + 8] for i in range(0, x.shape[0], 8)])
    return jnp.sum(x, axis=0, keepdims=True)


def dot_nt(a, b):
    return lax.dot_general(a, b, (((1,), (1,)), ((), ())), precision=HIGHEST, preferred_element_type=jnp.float32)


def dot_nn(a, b):
    return lax.dot_general(a, b, (((1,), (0,)), ((), ())), precision=HIGHEST, preferred_element_type=jnp.float32)


def dot_tn(a, b):
    return lax.dot_general(a, b, (((0,), (0,)), ((), ())), precision=HIGHEST, preferred_element_type=jnp.float32)


def tree_sum(parts):
    parts = list(parts)
    while len(parts) > 1:
        parts = [sum(parts[i : i + 2][1:], parts[i]) for i in range(0, len(parts), 2)]
    return parts[0]


def root_places(sizes):
    places = [(0, 0), (1, 0), (1, max(0, sizes["gz"] // 2 - 1))]
    return [{"gx": x, "gy": 0, "gz": z} for i, (x, z) in enumerate(places) if (x, z) not in places[:i]]


def kernel(sizes, local, dens_hbm, mom_hbm, fuel_hbm, modes_hbm, late_hbm,
           drate, mrate, hrate,
           f, modes, late, cells, along, along_low, across, across_low, edges, sides, ypack, zpack, ztile, own_sum, got_sums, full_sum,
           load_sem, send_sem, halo_recv, z_recv, sum_recv, z_ready, measure):
    size_x, size_y, size_z = local
    rows = size_x * size_y
    me = {a: lax.axis_index(a) for a in sizes}
    count_x, count_y, count_z = sizes["gx"], sizes["gy"], sizes["gz"]
    total = count_x * count_y * count_z
    roots = root_places(sizes)
    rank_of = lambda p: (p["gz"] * count_x + p["gx"]) * count_y + p["gy"]
    rank = rank_of(me)
    root_ranks = [rank_of(r) for r in roots]
    is_root = functools.reduce(jnp.logical_or, [rank == r for r in root_ranks])

    def place_of(i):
        if isinstance(i, int):
            x, y, z = i // count_y % count_x, i % count_y, i // (count_x * count_y)
            return {"gx": jnp.int32(x), "gy": jnp.int32(y), "gz": jnp.int32(z)}
        return {"gx": lax.rem(lax.div(i, count_y), count_x), "gy": lax.rem(i, count_y),
                "gz": lax.div(i, count_x * count_y)}

    def shifted(axis, step):
        return {axis: lax.rem(me[axis] + step % sizes[axis], sizes[axis])}

    own = pl.ds(REACH, size_x)
    load_late = pltpu.make_async_copy(late_hbm, late, load_sem)
    for at in range(0, size_x, LOAD_PLANES):
        for i, src in enumerate((dens_hbm, mom_hbm)):
            pltpu.make_async_copy(
                src.at[pl.ds(at, LOAD_PLANES)], f.at[i, pl.ds(REACH + at, LOAD_PLANES)], load_sem).start()
    load_fuel = pltpu.make_async_copy(fuel_hbm, f.at[2, own], load_sem)
    load_modes = pltpu.make_async_copy(modes_hbm, modes, load_sem)

    barrier = pltpu.get_barrier_semaphore()
    z_steps = (1, -1)
    z_next = [shifted("gz", step)["gz"] for step in z_steps]
    z_lower = [z < me["gz"] for z in z_next]
    y_steps = (1, -1) if count_y > 2 else (1,)
    sides_used = len(y_steps)

    def greet(place):
        pl.semaphore_signal(barrier, inc=1, device_id=place, device_id_type=MESH)

    for step in (1, -1):
        greet(shifted("gx", step))
    for step in y_steps:
        greet(shifted("gy", step))
    for step, lower in zip(z_steps, z_lower):
        @pl.when(jnp.logical_not(lower))
        def _(step=step):
            greet(shifted("gz", step))

    @pl.when(is_root)
    def _():
        def greet_one(i, carry):
            @pl.when(i != rank)
            def _():
                greet(place_of(i))
            return carry
        lax.fori_loop(0, total, greet_one, 0)

    greeters = 2 + sides_used + len(roots) - is_root.astype(jnp.int32)
    for lower in z_lower:
        greeters = greeters + lower.astype(jnp.int32)

    lane = lax.broadcasted_iota(jnp.int32, (1, 2 * HALF), 1)
    kx, ky, kz = packed_index(lax.rem(lane, HALF))
    quarter = (lane >= HALF).astype(jnp.float32)
    kx, ky, kz = [k.astype(jnp.float32) for k in (kx, ky, kz)]

    def quarters(k, place, axis, size):
        part = k * place.astype(jnp.float32) / (size * sizes[axis])
        return 4.0 * (part - jnp.floor(part))

    shift = quarters(kz, me["gz"] * size_z, "gz", size_z) - quarter
    rows_y = me["gy"] * size_y + lax.broadcasted_iota(jnp.int32, (size_y, 1), 0)
    angle_y = quarters(ky, rows_y, "gy", size_y) + shift
    for x in range(size_x):
        c, s = cos_sin(angle_y + quarters(kx, me["gx"] * size_x + x, "gx", size_x))
        cells[x * size_y : (x + 1) * size_y, 0 : 2 * HALF] = c
        cells[x * size_y : (x + 1) * size_y, 2 * HALF : 4 * HALF] = -s
    for z in range(0, size_z, 16):
        rows_at = z + lax.broadcasted_iota(jnp.int32, (16, 1), 0)
        for i, x in enumerate(cos_sin(quarters(kz, rows_at, "gz", size_z))):
            high, rest = split(x)
            along[z : z + 16, 2 * HALF * i : 2 * HALF * (i + 1)] = high.astype(jnp.bfloat16)
            along_low[z : z + 16, 2 * HALF * i : 2 * HALF * (i + 1)] = rest.astype(jnp.bfloat16)

    both_loaded = f.at[pl.ds(0, 2), own]
    pltpu.make_async_copy(both_loaded, both_loaded, load_sem).wait()
    load_fuel.start()
    load_late.start()
    flat = lambda i: f[i, own].reshape(rows, size_z)
    high, rest = split(flat(1) / flat(0))
    part = dot_split(jnp.concatenate([high, rest], 1), jnp.concatenate([along[...], along[...]], 0), ((1,), (0,)))
    part = part * cells[...] + dot_split(high, along_low[...], ((1,), (0,))) * cells[...]
    cube = column_sum(part[:, 0 : 2 * HALF] + part[:, 2 * HALF : 4 * HALF])
    own_sum[...] = cube
    got_sums[rank] = cube

    pl.semaphore_wait(barrier, greeters)
    def copy_out(src, dst, recv, place):
        return pltpu.make_async_remote_copy(
            src_ref=src, dst_ref=dst, send_sem=send_sem, recv_sem=recv, device_id=place, device_id_type=MESH)

    def spread(i):
        return copy_out(full_sum, full_sum, sum_recv, place_of(i))

    for r in root_ranks:
        @pl.when(rank != r)
        def _(r=r):
            copy_out(own_sum, got_sums.at[rank], sum_recv, place_of(r)).start()

    for step, lower in zip(z_steps, z_lower):
        @pl.when(lower)
        def _(step=step):
            pl.semaphore_signal(z_ready, inc=1, device_id=shifted("gz", step), device_id_type=MESH)

    both_loaded = measure.at[pl.ds(0, (fuel_hbm.size + late_hbm.size) // 1024)]
    pltpu.make_async_copy(both_loaded, both_loaded, load_sem).wait()
    load_modes.start()
    halos_x = [
        copy_out(f.at[:, pl.ds(size_x, REACH)], f.at[:, pl.ds(0, REACH)], halo_recv, shifted("gx", 1)),
        copy_out(f.at[:, pl.ds(REACH, REACH)], f.at[:, pl.ds(size_x + REACH, REACH)], halo_recv,
                 shifted("gx", -1)),
    ]
    for copy in halos_x:
        copy.start()
    band_at = 16
    pieces = []
    for i in range(2):
        ypack[i, :, 0:REACH] = f[1 + i, own, 0:REACH]
        ypack[i, :, REACH : 2 * REACH] = f[1 + i, own, size_y - REACH : size_y]
        high, rest = split(flat(1 + i))
        pieces += [high, *split(rest)]
    place = lax.broadcasted_iota(jnp.int32, (8, size_z), 0)
    place = jnp.where(place < REACH, place, place + size_z - 2 * REACH)
    edge = (lax.broadcasted_iota(jnp.int32, (8, size_z), 1) == place).astype(jnp.float32)
    ends = dot_split(edge, jnp.concatenate(pieces, 0), ((1,), (1,)))
    for i in range(2):
        zpack[i] = tree_sum([ends[:, (3 * i + j) * rows : (3 * i + j + 1) * rows] for j in range(3)])
    halos_y = [copy_out(ypack, sides.at[i], halo_recv, shifted("gy", step)) for i, step in enumerate(y_steps)]
    halos_z = [copy_out(zpack, ztile.at[i], z_recv, shifted("gz", step)) for i, step in enumerate(z_steps)]
    for copy, lower in zip(halos_z, z_lower):
        @pl.when(lower)
        def _(copy=copy):
            copy.start()
    for copy in halos_y:
        copy.start()

    lap = [dot_nn(flat(1 + i), late[band_at : band_at + size_z]).reshape(size_x, size_y, size_z) for i in range(2)]
    outs = (drate, mrate, hrate)
    mrate[...] = lap[0]
    hrate[...] = lap[1]

    load_modes.wait()
    count = modes.shape[1]
    code = (modes[0:1] * WIDTH + modes[1:2]) * WIDTH + modes[2:3]
    place = lax.rem(lax.broadcasted_iota(jnp.int32, (2 * HALF, 1), 0), HALF)
    px, py, pz = packed_index(place)
    mine = (px * WIDTH + py) * WIDTH + pz
    used = place < len(packed_modes())
    both_ways = jnp.where(used & (mine == code), 1.0, 0.0) + jnp.where(used & (mine == -code), 1.0, 0.0)
    chosen = dot_nt(jnp.ones((8, count), jnp.float32), both_ways)[0:1]

    ncell = float(rows * size_z * total)
    gain = chosen * (2.0 * FORCE_POWER / ncell)
    for i in range(2):
        here = pl.ds(2 * HALF * i, 2 * HALF)
        across[here] = along[:, here].astype(jnp.float32).T.astype(jnp.bfloat16)
        across_low[here] = along_low[:, here].astype(jnp.float32).T.astype(jnp.bfloat16)

    arrived = [f.at[:, pl.ds(0, 2 * REACH)], sides.at[pl.ds(0, sides_used)]]
    higher = sum(jnp.logical_not(lower).astype(jnp.int32) for lower in z_lower)

    @pl.when(higher > 0)
    def _():
        pl.semaphore_wait(z_ready, higher)

    for copy, lower in zip(halos_z, z_lower):
        @pl.when(jnp.logical_not(lower))
        def _(copy=copy):
            copy.start()

    pltpu.make_async_copy(measure, measure, halo_recv).wait()
    for i in range(2):
        edges[i, :, 0:8] = sides[0, i]
        edges[i, :, 8 : 8 + size_y] = f[1 + i, own]
        edges[i, :, 8 + size_y : 16 + size_y] = sides[sides_used - 1, i]
        total_y = outs[1 + i][...]
        for offset, weight in enumerate(SECOND_COEFFS, 1):
            total_y = total_y + weight * (
                edges[i, :, 8 + offset : 8 + offset + size_y] + edges[i, :, 8 - offset : 8 - offset + size_y])
        outs[1 + i][...] = total_y

    def planes(x, offset):
        return x[REACH + offset : REACH + offset + size_x]

    def first_diff(x):
        result = None
        for offset, weight in enumerate(FIRST_COEFFS, 1):
            term = weight * (planes(x, offset) - planes(x, -offset))
            result = term if result is None else result + term
        return result

    def second_diff(x):
        return tree_sum([w * (planes(x, o) + planes(x, -o)) for o, w in enumerate(SECOND_COEFFS, 1)])

    mom = f[1]
    dens = f[0]
    fuel = f[2]
    vel_pad = mom / dens
    drate[...] = -first_diff(mom)
    mid_fuel = planes(fuel, 0)
    hrate[...] = (DIFFUSIVITY * (hrate[...] + second_diff(fuel)) - first_diff(fuel * vel_pad)
                  - mid_fuel * jnp.exp(-ACTIVATION * mid_fuel / planes(dens, 0)))
    mrate[...] = VISCOSITY * (mrate[...] + second_diff(mom)) - first_diff(mom * vel_pad + dens)

    pltpu.make_async_copy(ztile, ztile, z_recv).wait()
    for i, rate in enumerate((VISCOSITY, DIFFUSIVITY)):
        tile = jnp.concatenate([ztile[0, i], ztile[1, i]], 0)
        outs[1 + i][...] = outs[1 + i][...] + rate * dot_tn(tile, late[0:16]).reshape(size_x, size_y, size_z)

    leaves = [i for i in range(total) if i not in root_ranks]

    @pl.when(is_root)
    def _():
        got = got_sums.at[pl.ds(0, total - 1)]
        pltpu.make_async_copy(got, got, sum_recv).wait()

    @pl.when(jnp.logical_not(is_root))
    def _():
        pltpu.make_async_copy(full_sum, full_sum, sum_recv).wait()

    cube = jnp.where(is_root, tree_sum([got_sums[i] for i in range(total)]), full_sum[...])

    @pl.when(rank == root_ranks[-1])
    def _():
        full_sum[...] = cube
        for i in reversed(leaves):
            spread(i).start()

    coef = cube / ncell
    energy = jnp.sum(chosen * coef * coef, axis=1, keepdims=True)
    scale = 1.0 / (energy + ENERGY_EPS)
    lit = gain * cube
    high, rest = split(cells[...] * jnp.concatenate([lit, lit], 1))
    both = dot_split(high, jnp.concatenate([across[...], across_low[...]], 1), ((1,), (0,)))
    weight = flat(0) * scale
    low = weight * (both[:, 0:size_z] + both[:, size_z:]) + weight * dot_split(rest, across[...], ((1,), (0,)))
    mrate[...] = mrate[...] + low.reshape(size_x, size_y, size_z)

    for sent in (arrived[0], arrived[1], ztile.at[:, :]):
        pltpu.make_async_copy(sent, sent, send_sem).wait()
    for r in root_ranks:
        @pl.when(rank != r)
        def _():
            pltpu.make_async_copy(own_sum, own_sum, send_sem).wait()
    if leaves:
        @pl.when(rank == root_ranks[-1])
        def _():
            sent = got_sums.at[pl.ds(0, len(leaves))]
            pltpu.make_async_copy(sent, sent, send_sem).wait()


def write_out(*refs):
    count = len(refs) // 2
    copies = [pltpu.make_async_copy(refs[i], refs[count + i], refs[-1]) for i in range(count)]
    for copy in copies:
        copy.start()
    for copy in copies:
        copy.wait()


def solution(mesh):
    sizes = {a: mesh.shape[a] for a in ("gx", "gy", "gz")}

    def per_device(density, momentum, hydrogen, forced_modes):
        local = density.shape
        size_x, size_y, size_z = local
        rows = size_x * size_y
        late = tables(size_z)
        modes = forced_modes.T
        total = math.prod(sizes.values())
        halo_bytes = 4 * (3 * 2 * REACH * size_y + (1 + (sizes["gy"] > 2)) * 2 * size_x * 8) * size_z
        any_spec = pl.BlockSpec(memory_space=pl.ANY)
        f32 = jnp.float32
        rates = pl.pallas_call(
            functools.partial(kernel, sizes, local),
            out_shape=[pltpu.VMEM(local, f32)] * 3,
            in_specs=[any_spec] * 5,
            out_specs=[pl.BlockSpec(memory_space=pltpu.VMEM)] * 3,
            scratch_shapes=[
                pltpu.VMEM((3, size_x + 2 * REACH, size_y, size_z), f32),
                pltpu.VMEM(modes.shape, jnp.int32),
                pltpu.VMEM(late.shape, f32),
                pltpu.VMEM((rows, 4 * HALF), f32),
                pltpu.VMEM((size_z, 4 * HALF), jnp.bfloat16),
                pltpu.VMEM((size_z, 4 * HALF), jnp.bfloat16),
                pltpu.VMEM((4 * HALF, size_z), jnp.bfloat16),
                pltpu.VMEM((4 * HALF, size_z), jnp.bfloat16),
                pltpu.VMEM((2, size_x, size_y + 16, size_z), f32),
                pltpu.VMEM((2, 2, size_x, 8, size_z), f32),
                pltpu.VMEM((2, size_x, 8, size_z), f32),
                pltpu.VMEM((2, 8, rows), f32),
                pltpu.VMEM((2, 2, 8, rows), f32),
                pltpu.VMEM((1, 2 * HALF), f32),
                pltpu.VMEM((total, 1, 2 * HALF), f32),
                pltpu.VMEM((1, 2 * HALF), f32),
                pltpu.SemaphoreType.DMA,
                pltpu.SemaphoreType.DMA,
                pltpu.SemaphoreType.DMA,
                pltpu.SemaphoreType.DMA,
                pltpu.SemaphoreType.DMA,
                pltpu.SemaphoreType.REGULAR,
                pltpu.VMEM((halo_bytes // 4096, 8, 128), f32),
            ],
            compiler_params=pltpu.CompilerParams(collective_id=0, has_side_effects=True),
            name="flame",
        )(density, momentum, hydrogen, modes, jnp.asarray(late))
        return tuple(pl.pallas_call(
            write_out,
            out_shape=[jax.ShapeDtypeStruct(local, f32)] * 3,
            in_specs=[pl.BlockSpec(memory_space=pltpu.VMEM)] * 3,
            out_specs=[any_spec] * 3,
            scratch_shapes=[pltpu.SemaphoreType.DMA],
            name="write",
        )(*[pltpu.with_memory_space_constraint(r, pltpu.VMEM) for r in rates]))

    in_specs = (P("gx", "gy", "gz"), P("gx", "gy", "gz"), P("gx", "gy", "gz"), P())
    out_specs = (P("gx", "gy", "gz"), P("gx", "gy", "gz"), P("gx", "gy", "gz"))
    return jax.shard_map(
        per_device, mesh=mesh, in_specs=in_specs, out_specs=out_specs, check_vma=False
    )
```

```python
import functools
import math

import jax
import jax.numpy as jnp
import numpy as np
from jax import lax
from jax.experimental import pallas as pl
from jax.experimental.pallas import tpu as pltpu
from jax.sharding import PartitionSpec as P

KMAX = 3
WIDTH = 2 * KMAX + 1
HALF = 64
ROWS = KMAX + 1
REACH = 4
LOAD_PLANES = 4

FIRST_COEFFS = (0.8, -0.2, 4.0 / 105.0, -1.0 / 280.0)
SECOND_COEFFS = (1.6, -0.2, 8.0 / 315.0, -1.0 / 560.0)
CENTRE_COEFF = -205.0 / 72.0
VISCOSITY = 0.3
DIFFUSIVITY = 1.5
FORCE_POWER = 0.3
ENERGY_EPS = 1e-06
ACTIVATION = 2.0
HIGHEST = lax.Precision.HIGHEST
MESH = pl.DeviceIdType.MESH


def packed_modes():
    reach = range(-KMAX, KMAX + 1)
    cells = [(x, y, z) for z in range(ROWS) for x in reach for y in reach
             if x * x + y * y + z * z <= KMAX * KMAX and (z, x, y) > (0, 0, 0)]
    return cells


def packed_index(place):
    cells = packed_modes()
    result = []
    for part in range(3):
        value = jnp.full(place.shape, cells[0][part], jnp.int32)
        if part == 1:
            value = value + place
        for i in range(1, len(cells)):
            step = cells[i][part] - cells[i - 1][part] - (part == 1)
            if step:
                value = value + jnp.where(place >= i, step, 0)
        result.append(value)
    return result


def tables(size_z):
    band = np.zeros((size_z, size_z))
    halo = np.zeros((16, size_z))
    for z in range(size_z):
        band[z, z] = 3.0 * CENTRE_COEFF
        for offset, weight in enumerate(SECOND_COEFFS, 1):
            for q in (z - offset, z + offset):
                if 0 <= q < size_z:
                    band[q, z] = weight
                elif q < 0:
                    halo[8 + q, z] = weight
                else:
                    halo[8 + q - size_z, z] = weight
    return np.concatenate([halo, band], 0).astype(np.float32)


def polynomial(x, coeffs):
    result = coeffs[-1]
    for c in reversed(coeffs[:-1]):
        result = result * x + c
    return result


SIN_COEFFS = [(-1) ** n * (math.pi / 2) ** (2 * n + 1) / math.factorial(2 * n + 1) for n in range(5)]
COS_COEFFS = [(-1) ** n * (math.pi / 2) ** (2 * n) / math.factorial(2 * n) for n in range(6)]


def cos_sin(quarters):
    turns = jnp.floor(quarters + 0.5)
    d = quarters - turns
    square = d * d
    s = d * polynomial(square, SIN_COEFFS)
    c = polynomial(square, COS_COEFFS)
    half = jnp.floor(0.5 * turns)
    odd = turns - 2.0 * half
    turned = half - 2.0 * jnp.floor(0.5 * half)
    sin_sign = 1.0 - 2.0 * turned
    cos_sign = sin_sign - 2.0 * odd * sin_sign
    swap = odd > 0.5
    return jnp.where(swap, s, c) * cos_sign, jnp.where(swap, c, s) * sin_sign


def split(x):
    high = x.astype(jnp.bfloat16).astype(jnp.float32)
    return high, x - high


def dot_split(a, b, contract):
    return lax.dot_general(a.astype(jnp.bfloat16), b.astype(jnp.bfloat16), (contract, ((), ())),
                           preferred_element_type=jnp.float32)


def column_sum(x):
    x = tree_sum([x[i : i + 8] for i in range(0, x.shape[0], 8)])
    return jnp.sum(x, axis=0, keepdims=True)


def dot_nt(a, b):
    return lax.dot_general(a, b, (((1,), (1,)), ((), ())), precision=HIGHEST, preferred_element_type=jnp.float32)


def dot_nn(a, b):
    return lax.dot_general(a, b, (((1,), (0,)), ((), ())), precision=HIGHEST, preferred_element_type=jnp.float32)


def dot_tn(a, b):
    return lax.dot_general(a, b, (((0,), (0,)), ((), ())), precision=HIGHEST, preferred_element_type=jnp.float32)


def tree_sum(parts):
    parts = list(parts)
    while len(parts) > 1:
        parts = [sum(parts[i : i + 2][1:], parts[i]) for i in range(0, len(parts), 2)]
    return parts[0]


def root_places(sizes):
    places = [(0, 0), (1, 0), (1, max(0, sizes["gz"] // 2 - 1))]
    return [{"gx": x, "gy": 0, "gz": z} for i, (x, z) in enumerate(places) if (x, z) not in places[:i]]


def kernel(sizes, local, dens_hbm, mom_hbm, fuel_hbm, modes_hbm, late_hbm,
           drate, mrate, hrate, dens_out, cells, across, across_low, chosen_out, total_out,
           f, modes, late, along, along_low, edges, sides, ypack, zpack, ztile, own_sum, got_sums, full_sum,
           load_sem, send_sem, halo_recv, z_recv, sum_recv, z_ready, measure):
    size_x, size_y, size_z = local
    rows = size_x * size_y
    me = {a: lax.axis_index(a) for a in sizes}
    count_x, count_y, count_z = sizes["gx"], sizes["gy"], sizes["gz"]
    total = count_x * count_y * count_z
    roots = root_places(sizes)
    rank_of = lambda p: (p["gz"] * count_x + p["gx"]) * count_y + p["gy"]
    rank = rank_of(me)
    root_ranks = [rank_of(r) for r in roots]
    is_root = functools.reduce(jnp.logical_or, [rank == r for r in root_ranks])

    def place_of(i):
        if isinstance(i, int):
            x, y, z = i // count_y % count_x, i % count_y, i // (count_x * count_y)
            return {"gx": jnp.int32(x), "gy": jnp.int32(y), "gz": jnp.int32(z)}
        return {"gx": lax.rem(lax.div(i, count_y), count_x), "gy": lax.rem(i, count_y),
                "gz": lax.div(i, count_x * count_y)}

    def shifted(axis, step):
        return {axis: lax.rem(me[axis] + step % sizes[axis], sizes[axis])}

    own = pl.ds(REACH, size_x)
    load_late = pltpu.make_async_copy(late_hbm, late, load_sem)
    for at in range(0, size_x, LOAD_PLANES):
        for i, src in enumerate((dens_hbm, mom_hbm)):
            pltpu.make_async_copy(
                src.at[pl.ds(at, LOAD_PLANES)], f.at[i, pl.ds(REACH + at, LOAD_PLANES)], load_sem).start()
    load_fuel = pltpu.make_async_copy(fuel_hbm, f.at[2, own], load_sem)
    load_modes = pltpu.make_async_copy(modes_hbm, modes, load_sem)

    barrier = pltpu.get_barrier_semaphore()
    z_steps = (1, -1)
    z_next = [shifted("gz", step)["gz"] for step in z_steps]
    z_lower = [z < me["gz"] for z in z_next]
    y_steps = (1, -1) if count_y > 2 else (1,)
    sides_used = len(y_steps)

    def greet(place):
        pl.semaphore_signal(barrier, inc=1, device_id=place, device_id_type=MESH)

    for step in (1, -1):
        greet(shifted("gx", step))
    for step in y_steps:
        greet(shifted("gy", step))
    for step, lower in zip(z_steps, z_lower):
        @pl.when(jnp.logical_not(lower))
        def _(step=step):
            greet(shifted("gz", step))

    @pl.when(is_root)
    def _():
        def greet_one(i, carry):
            @pl.when(i != rank)
            def _():
                greet(place_of(i))
            return carry
        lax.fori_loop(0, total, greet_one, 0)

    greeters = 2 + sides_used + len(roots) - is_root.astype(jnp.int32)
    for lower in z_lower:
        greeters = greeters + lower.astype(jnp.int32)

    lane = lax.broadcasted_iota(jnp.int32, (1, 2 * HALF), 1)
    kx, ky, kz = packed_index(lax.rem(lane, HALF))
    quarter = (lane >= HALF).astype(jnp.float32)
    kx, ky, kz = [k.astype(jnp.float32) for k in (kx, ky, kz)]

    def quarters(k, place, axis, size):
        part = k * place.astype(jnp.float32) / (size * sizes[axis])
        return 4.0 * (part - jnp.floor(part))

    shift = quarters(kz, me["gz"] * size_z, "gz", size_z) - quarter
    rows_y = me["gy"] * size_y + lax.broadcasted_iota(jnp.int32, (size_y, 1), 0)
    angle_y = quarters(ky, rows_y, "gy", size_y) + shift
    for x in range(size_x):
        c, s = cos_sin(angle_y + quarters(kx, me["gx"] * size_x + x, "gx", size_x))
        cells[x * size_y : (x + 1) * size_y, 0 : 2 * HALF] = c
        cells[x * size_y : (x + 1) * size_y, 2 * HALF : 4 * HALF] = -s
    for z in range(0, size_z, 16):
        rows_at = z + lax.broadcasted_iota(jnp.int32, (16, 1), 0)
        for i, x in enumerate(cos_sin(quarters(kz, rows_at, "gz", size_z))):
            high, rest = split(x)
            along[z : z + 16, 2 * HALF * i : 2 * HALF * (i + 1)] = high.astype(jnp.bfloat16)
            along_low[z : z + 16, 2 * HALF * i : 2 * HALF * (i + 1)] = rest.astype(jnp.bfloat16)

    both_loaded = f.at[pl.ds(0, 2), own]
    pltpu.make_async_copy(both_loaded, both_loaded, load_sem).wait()
    load_fuel.start()
    load_late.start()
    flat = lambda i: f[i, own].reshape(rows, size_z)
    high, rest = split(flat(1) / flat(0))
    part = dot_split(jnp.concatenate([high, rest], 1), jnp.concatenate([along[...], along[...]], 0), ((1,), (0,)))
    part = part * cells[...] + dot_split(high, along_low[...], ((1,), (0,))) * cells[...]
    cube = column_sum(part[:, 0 : 2 * HALF] + part[:, 2 * HALF : 4 * HALF])
    own_sum[...] = cube
    got_sums[rank] = cube

    pl.semaphore_wait(barrier, greeters)
    def copy_out(src, dst, recv, place):
        return pltpu.make_async_remote_copy(
            src_ref=src, dst_ref=dst, send_sem=send_sem, recv_sem=recv, device_id=place, device_id_type=MESH)

    def spread(i):
        return copy_out(full_sum, full_sum, sum_recv, place_of(i))

    for r in root_ranks:
        @pl.when(rank != r)
        def _(r=r):
            copy_out(own_sum, got_sums.at[rank], sum_recv, place_of(r)).start()

    for step, lower in zip(z_steps, z_lower):
        @pl.when(lower)
        def _(step=step):
            pl.semaphore_signal(z_ready, inc=1, device_id=shifted("gz", step), device_id_type=MESH)

    both_loaded = measure.at[pl.ds(0, (fuel_hbm.size + late_hbm.size) // 1024)]
    pltpu.make_async_copy(both_loaded, both_loaded, load_sem).wait()
    load_modes.start()
    halos_x = [
        copy_out(f.at[:, pl.ds(size_x, REACH)], f.at[:, pl.ds(0, REACH)], halo_recv, shifted("gx", 1)),
        copy_out(f.at[:, pl.ds(REACH, REACH)], f.at[:, pl.ds(size_x + REACH, REACH)], halo_recv,
                 shifted("gx", -1)),
    ]
    for copy in halos_x:
        copy.start()
    band_at = 16
    pieces = []
    for i in range(2):
        ypack[i, :, 0:REACH] = f[1 + i, own, 0:REACH]
        ypack[i, :, REACH : 2 * REACH] = f[1 + i, own, size_y - REACH : size_y]
        high, rest = split(flat(1 + i))
        pieces += [high, *split(rest)]
    place = lax.broadcasted_iota(jnp.int32, (8, size_z), 0)
    place = jnp.where(place < REACH, place, place + size_z - 2 * REACH)
    edge = (lax.broadcasted_iota(jnp.int32, (8, size_z), 1) == place).astype(jnp.float32)
    ends = dot_split(edge, jnp.concatenate(pieces, 0), ((1,), (1,)))
    for i in range(2):
        zpack[i] = tree_sum([ends[:, (3 * i + j) * rows : (3 * i + j + 1) * rows] for j in range(3)])
    halos_y = [copy_out(ypack, sides.at[i], halo_recv, shifted("gy", step)) for i, step in enumerate(y_steps)]
    halos_z = [copy_out(zpack, ztile.at[i], z_recv, shifted("gz", step)) for i, step in enumerate(z_steps)]
    for copy, lower in zip(halos_z, z_lower):
        @pl.when(lower)
        def _(copy=copy):
            copy.start()
    for copy in halos_y:
        copy.start()

    lap = [dot_nn(flat(1 + i), late[band_at : band_at + size_z]).reshape(size_x, size_y, size_z) for i in range(2)]
    outs = (drate, mrate, hrate)
    mrate[...] = lap[0]
    hrate[...] = lap[1]

    load_modes.wait()
    count = modes.shape[1]
    code = (modes[0:1] * WIDTH + modes[1:2]) * WIDTH + modes[2:3]
    place = lax.rem(lax.broadcasted_iota(jnp.int32, (2 * HALF, 1), 0), HALF)
    px, py, pz = packed_index(place)
    mine = (px * WIDTH + py) * WIDTH + pz
    used = place < len(packed_modes())
    both_ways = jnp.where(used & (mine == code), 1.0, 0.0) + jnp.where(used & (mine == -code), 1.0, 0.0)
    chosen = dot_nt(jnp.ones((8, count), jnp.float32), both_ways)[0:1]

    chosen_out[...] = chosen
    dens_out[...] = f[0, own]
    for i in range(2):
        here = pl.ds(2 * HALF * i, 2 * HALF)
        across[here] = along[:, here].astype(jnp.float32).T.astype(jnp.bfloat16)
        across_low[here] = along_low[:, here].astype(jnp.float32).T.astype(jnp.bfloat16)

    arrived = [f.at[:, pl.ds(0, 2 * REACH)], sides.at[pl.ds(0, sides_used)]]
    higher = sum(jnp.logical_not(lower).astype(jnp.int32) for lower in z_lower)

    @pl.when(higher > 0)
    def _():
        pl.semaphore_wait(z_ready, higher)

    for copy, lower in zip(halos_z, z_lower):
        @pl.when(jnp.logical_not(lower))
        def _(copy=copy):
            copy.start()

    pltpu.make_async_copy(measure, measure, halo_recv).wait()
    for i in range(2):
        edges[i, :, 0:8] = sides[0, i]
        edges[i, :, 8 : 8 + size_y] = f[1 + i, own]
        edges[i, :, 8 + size_y : 16 + size_y] = sides[sides_used - 1, i]
        total_y = outs[1 + i][...]
        for offset, weight in enumerate(SECOND_COEFFS, 1):
            total_y = total_y + weight * (
                edges[i, :, 8 + offset : 8 + offset + size_y] + edges[i, :, 8 - offset : 8 - offset + size_y])
        outs[1 + i][...] = total_y

    def planes(x, offset):
        return x[REACH + offset : REACH + offset + size_x]

    def first_diff(x):
        result = None
        for offset, weight in enumerate(FIRST_COEFFS, 1):
            term = weight * (planes(x, offset) - planes(x, -offset))
            result = term if result is None else result + term
        return result

    def second_diff(x):
        return tree_sum([w * (planes(x, o) + planes(x, -o)) for o, w in enumerate(SECOND_COEFFS, 1)])

    mom = f[1]
    dens = f[0]
    fuel = f[2]
    vel_pad = mom / dens
    drate[...] = -first_diff(mom)
    mid_fuel = planes(fuel, 0)
    hrate[...] = (DIFFUSIVITY * (hrate[...] + second_diff(fuel)) - first_diff(fuel * vel_pad)
                  - mid_fuel * jnp.exp(-ACTIVATION * mid_fuel / planes(dens, 0)))
    mrate[...] = VISCOSITY * (mrate[...] + second_diff(mom)) - first_diff(mom * vel_pad + dens)

    pltpu.make_async_copy(ztile, ztile, z_recv).wait()
    for i, rate in enumerate((VISCOSITY, DIFFUSIVITY)):
        tile = jnp.concatenate([ztile[0, i], ztile[1, i]], 0)
        outs[1 + i][...] = outs[1 + i][...] + rate * dot_tn(tile, late[0:16]).reshape(size_x, size_y, size_z)

    leaves = [i for i in range(total) if i not in root_ranks]

    @pl.when(is_root)
    def _():
        got = got_sums.at[pl.ds(0, total - 1)]
        pltpu.make_async_copy(got, got, sum_recv).wait()

    @pl.when(jnp.logical_not(is_root))
    def _():
        pltpu.make_async_copy(full_sum, full_sum, sum_recv).wait()

    cube = jnp.where(is_root, tree_sum([got_sums[i] for i in range(total)]), full_sum[...])

    @pl.when(rank == root_ranks[-1])
    def _():
        full_sum[...] = cube
        for i in reversed(leaves):
            spread(i).start()

    total_out[...] = cube
    for sent in (arrived[0], arrived[1], ztile.at[:, :]):
        pltpu.make_async_copy(sent, sent, send_sem).wait()
    for r in root_ranks:
        @pl.when(rank != r)
        def _():
            pltpu.make_async_copy(own_sum, own_sum, send_sem).wait()
    if leaves:
        @pl.when(rank == root_ranks[-1])
        def _():
            sent = got_sums.at[pl.ds(0, len(leaves))]
            pltpu.make_async_copy(sent, sent, send_sem).wait()


def finish(ncell, drate, mrate, hrate, dens, cells, across, across_low, chosen, total,
           drate_hbm, mrate_hbm, hrate_hbm, result, sem):
    size_x, size_y, size_z = dens.shape
    rows = size_x * size_y
    early = [pltpu.make_async_copy(drate, drate_hbm, sem), pltpu.make_async_copy(hrate, hrate_hbm, sem)]
    for copy in early:
        copy.start()
    coef = total[...] / ncell
    energy = jnp.sum(chosen[...] * coef * coef, axis=1, keepdims=True)
    scale = 1.0 / (energy + ENERGY_EPS)
    lit = chosen[...] * (2.0 * FORCE_POWER / ncell) * total[...]
    high, rest = split(cells[...] * jnp.concatenate([lit, lit], 1))
    both = dot_split(high, jnp.concatenate([across[...], across_low[...]], 1), ((1,), (0,)))
    weight = dens[...].reshape(rows, size_z) * scale
    low = weight * (both[:, 0:size_z] + both[:, size_z:]) + weight * dot_split(rest, across[...], ((1,), (0,)))
    low = low.reshape(size_x, size_y, size_z)
    for at in range(0, size_x, size_x // 2):
        here = pl.ds(at, size_x // 2)
        result[here] = mrate[here] + low[at : at + size_x // 2]
        pltpu.make_async_copy(result.at[here], mrate_hbm.at[here], sem).start()
    for copy in early:
        copy.wait()
    pltpu.make_async_copy(result, mrate_hbm, sem).wait()


def solution(mesh):
    sizes = {a: mesh.shape[a] for a in ("gx", "gy", "gz")}

    def per_device(density, momentum, hydrogen, forced_modes):
        local = density.shape
        size_x, size_y, size_z = local
        rows = size_x * size_y
        late = tables(size_z)
        modes = forced_modes.T
        total = math.prod(sizes.values())
        halo_bytes = 4 * (3 * 2 * REACH * size_y + (1 + (sizes["gy"] > 2)) * 2 * size_x * 8) * size_z
        any_spec = pl.BlockSpec(memory_space=pl.ANY)
        f32 = jnp.float32
        rates = pl.pallas_call(
            functools.partial(kernel, sizes, local),
            out_shape=[pltpu.VMEM(local, f32)] * 4 + [
                pltpu.VMEM((rows, 4 * HALF), f32),
                pltpu.VMEM((4 * HALF, size_z), jnp.bfloat16),
                pltpu.VMEM((4 * HALF, size_z), jnp.bfloat16),
                pltpu.VMEM((1, 2 * HALF), f32),
                pltpu.VMEM((1, 2 * HALF), f32),
            ],
            in_specs=[any_spec] * 5,
            out_specs=[pl.BlockSpec(memory_space=pltpu.VMEM)] * 9,
            scratch_shapes=[
                pltpu.VMEM((3, size_x + 2 * REACH, size_y, size_z), f32),
                pltpu.VMEM(modes.shape, jnp.int32),
                pltpu.VMEM(late.shape, f32),
                pltpu.VMEM((size_z, 4 * HALF), jnp.bfloat16),
                pltpu.VMEM((size_z, 4 * HALF), jnp.bfloat16),
                pltpu.VMEM((2, size_x, size_y + 16, size_z), f32),
                pltpu.VMEM((2, 2, size_x, 8, size_z), f32),
                pltpu.VMEM((2, size_x, 8, size_z), f32),
                pltpu.VMEM((2, 8, rows), f32),
                pltpu.VMEM((2, 2, 8, rows), f32),
                pltpu.VMEM((1, 2 * HALF), f32),
                pltpu.VMEM((total, 1, 2 * HALF), f32),
                pltpu.VMEM((1, 2 * HALF), f32),
                pltpu.SemaphoreType.DMA,
                pltpu.SemaphoreType.DMA,
                pltpu.SemaphoreType.DMA,
                pltpu.SemaphoreType.DMA,
                pltpu.SemaphoreType.DMA,
                pltpu.SemaphoreType.REGULAR,
                pltpu.VMEM((halo_bytes // 4096, 8, 128), f32),
            ],
            compiler_params=pltpu.CompilerParams(collective_id=0, has_side_effects=True),
            name="flame",
        )(density, momentum, hydrogen, modes, jnp.asarray(late))
        return tuple(pl.pallas_call(
            functools.partial(finish, float(rows * size_z * total)),
            out_shape=[jax.ShapeDtypeStruct(local, f32)] * 3,
            in_specs=[pl.BlockSpec(memory_space=pltpu.VMEM)] * 9,
            out_specs=[any_spec] * 3,
            scratch_shapes=[pltpu.VMEM(local, f32), pltpu.SemaphoreType.DMA],
            name="write",
        )(*[pltpu.with_memory_space_constraint(r, pltpu.VMEM) for r in rates]))

    in_specs = (P("gx", "gy", "gz"), P("gx", "gy", "gz"), P("gx", "gy", "gz"), P())
    out_specs = (P("gx", "gy", "gz"), P("gx", "gy", "gz"), P("gx", "gy", "gz"))
    return jax.shard_map(
        per_device, mesh=mesh, in_specs=in_specs, out_specs=out_specs, check_vma=False
    )
```

```python
import functools
import math

import jax
import jax.numpy as jnp
import numpy as np
from jax import lax
from jax.experimental import pallas as pl
from jax.experimental.pallas import tpu as pltpu
from jax.sharding import PartitionSpec as P

KMAX = 3
WIDTH = 2 * KMAX + 1
HALF = 64
ROWS = KMAX + 1
REACH = 4
LOAD_PLANES = 4

FIRST_COEFFS = (0.8, -0.2, 4.0 / 105.0, -1.0 / 280.0)
SECOND_COEFFS = (1.6, -0.2, 8.0 / 315.0, -1.0 / 560.0)
CENTRE_COEFF = -205.0 / 72.0
VISCOSITY = 0.3
DIFFUSIVITY = 1.5
FORCE_POWER = 0.3
ENERGY_EPS = 1e-06
ACTIVATION = 2.0
HIGHEST = lax.Precision.HIGHEST
MESH = pl.DeviceIdType.MESH


def packed_modes():
    reach = range(-KMAX, KMAX + 1)
    cells = [(x, y, z) for z in range(ROWS) for x in reach for y in reach
             if x * x + y * y + z * z <= KMAX * KMAX and (z, x, y) > (0, 0, 0)]
    return cells


def packed_index(place):
    cells = packed_modes()
    result = []
    for part in range(3):
        value = jnp.full(place.shape, cells[0][part], jnp.int32)
        if part == 1:
            value = value + place
        for i in range(1, len(cells)):
            step = cells[i][part] - cells[i - 1][part] - (part == 1)
            if step:
                value = value + jnp.where(place >= i, step, 0)
        result.append(value)
    return result


def tables(size_z):
    band = np.zeros((size_z, size_z))
    halo = np.zeros((16, size_z))
    for z in range(size_z):
        band[z, z] = 3.0 * CENTRE_COEFF
        for offset, weight in enumerate(SECOND_COEFFS, 1):
            for q in (z - offset, z + offset):
                if 0 <= q < size_z:
                    band[q, z] = weight
                elif q < 0:
                    halo[8 + q, z] = weight
                else:
                    halo[8 + q - size_z, z] = weight
    return np.concatenate([halo, band], 0).astype(np.float32)


def polynomial(x, coeffs):
    result = coeffs[-1]
    for c in reversed(coeffs[:-1]):
        result = result * x + c
    return result


SIN_COEFFS = [(-1) ** n * (math.pi / 2) ** (2 * n + 1) / math.factorial(2 * n + 1) for n in range(5)]
COS_COEFFS = [(-1) ** n * (math.pi / 2) ** (2 * n) / math.factorial(2 * n) for n in range(6)]


def cos_sin(quarters):
    turns = jnp.floor(quarters + 0.5)
    d = quarters - turns
    square = d * d
    s = d * polynomial(square, SIN_COEFFS)
    c = polynomial(square, COS_COEFFS)
    half = jnp.floor(0.5 * turns)
    odd = turns - 2.0 * half
    turned = half - 2.0 * jnp.floor(0.5 * half)
    sin_sign = 1.0 - 2.0 * turned
    cos_sign = sin_sign - 2.0 * odd * sin_sign
    swap = odd > 0.5
    return jnp.where(swap, s, c) * cos_sign, jnp.where(swap, c, s) * sin_sign


def split(x):
    high = x.astype(jnp.bfloat16).astype(jnp.float32)
    return high, x - high


def dot_split(a, b, contract):
    return lax.dot_general(a.astype(jnp.bfloat16), b.astype(jnp.bfloat16), (contract, ((), ())),
                           preferred_element_type=jnp.float32)


def column_sum(x):
    x = tree_sum([x[i : i + 8] for i in range(0, x.shape[0], 8)])
    return jnp.sum(x, axis=0, keepdims=True)


def dot_nt(a, b):
    return lax.dot_general(a, b, (((1,), (1,)), ((), ())), precision=HIGHEST, preferred_element_type=jnp.float32)


def dot_nn(a, b):
    return lax.dot_general(a, b, (((1,), (0,)), ((), ())), precision=HIGHEST, preferred_element_type=jnp.float32)


def dot_tn(a, b):
    return lax.dot_general(a, b, (((0,), (0,)), ((), ())), precision=HIGHEST, preferred_element_type=jnp.float32)


def tree_sum(parts):
    parts = list(parts)
    while len(parts) > 1:
        parts = [sum(parts[i : i + 2][1:], parts[i]) for i in range(0, len(parts), 2)]
    return parts[0]


def root_places(sizes):
    places = [(0, 0), (1, 0), (1, max(0, sizes["gz"] // 2 - 1))]
    return [{"gx": x, "gy": 0, "gz": z} for i, (x, z) in enumerate(places) if (x, z) not in places[:i]]


def kernel(sizes, local, dens_hbm, mom_hbm, fuel_hbm, modes_hbm, late_hbm,
           drate, mrate, hrate, dens_out, cells, across, across_low, chosen_out, total_out,
           f, modes, late, along, along_low, edges, sides, ypack, zpack, ztile, own_sum, got_sums, full_sum,
           load_sem, send_sem, halo_recv, z_recv, sum_recv, z_ready, measure):
    size_x, size_y, size_z = local
    rows = size_x * size_y
    me = {a: lax.axis_index(a) for a in sizes}
    count_x, count_y, count_z = sizes["gx"], sizes["gy"], sizes["gz"]
    total = count_x * count_y * count_z
    roots = root_places(sizes)
    rank_of = lambda p: (p["gz"] * count_x + p["gx"]) * count_y + p["gy"]
    rank = rank_of(me)
    root_ranks = [rank_of(r) for r in roots]
    is_root = functools.reduce(jnp.logical_or, [rank == r for r in root_ranks])

    def place_of(i):
        if isinstance(i, int):
            x, y, z = i // count_y % count_x, i % count_y, i // (count_x * count_y)
            return {"gx": jnp.int32(x), "gy": jnp.int32(y), "gz": jnp.int32(z)}
        return {"gx": lax.rem(lax.div(i, count_y), count_x), "gy": lax.rem(i, count_y),
                "gz": lax.div(i, count_x * count_y)}

    def shifted(axis, step):
        return {axis: lax.rem(me[axis] + step % sizes[axis], sizes[axis])}

    own = pl.ds(REACH, size_x)
    load_late = pltpu.make_async_copy(late_hbm, late, load_sem)
    for at in range(0, size_x, LOAD_PLANES):
        for i, src in enumerate((dens_hbm, mom_hbm)):
            pltpu.make_async_copy(
                src.at[pl.ds(at, LOAD_PLANES)], f.at[i, pl.ds(REACH + at, LOAD_PLANES)], load_sem).start()
    load_fuel = pltpu.make_async_copy(fuel_hbm, f.at[2, own], load_sem)
    load_modes = pltpu.make_async_copy(modes_hbm, modes, load_sem)

    barrier = pltpu.get_barrier_semaphore()
    z_steps = (1, -1)
    z_next = [shifted("gz", step)["gz"] for step in z_steps]
    z_lower = [z < me["gz"] for z in z_next]
    y_steps = (1, -1) if count_y > 2 else (1,)
    sides_used = len(y_steps)

    def greet(place):
        pl.semaphore_signal(barrier, inc=1, device_id=place, device_id_type=MESH)

    for step in (1, -1):
        greet(shifted("gx", step))
    for step in y_steps:
        greet(shifted("gy", step))
    for step, lower in zip(z_steps, z_lower):
        @pl.when(jnp.logical_not(lower))
        def _(step=step):
            greet(shifted("gz", step))

    @pl.when(is_root)
    def _():
        def greet_one(i, carry):
            @pl.when(i != rank)
            def _():
                greet(place_of(i))
            return carry
        lax.fori_loop(0, total, greet_one, 0)

    greeters = 2 + sides_used + len(roots) - is_root.astype(jnp.int32)
    for lower in z_lower:
        greeters = greeters + lower.astype(jnp.int32)

    lane = lax.broadcasted_iota(jnp.int32, (1, 2 * HALF), 1)
    kx, ky, kz = packed_index(lax.rem(lane, HALF))
    quarter = (lane >= HALF).astype(jnp.float32)
    kx, ky, kz = [k.astype(jnp.float32) for k in (kx, ky, kz)]

    def quarters(k, place, axis, size):
        part = k * place.astype(jnp.float32) / (size * sizes[axis])
        return 4.0 * (part - jnp.floor(part))

    shift = quarters(kz, me["gz"] * size_z, "gz", size_z) - quarter
    rows_y = me["gy"] * size_y + lax.broadcasted_iota(jnp.int32, (size_y, 1), 0)
    angle_y = quarters(ky, rows_y, "gy", size_y) + shift
    for x in range(size_x):
        c, s = cos_sin(angle_y + quarters(kx, me["gx"] * size_x + x, "gx", size_x))
        cells[x * size_y : (x + 1) * size_y, 0 : 2 * HALF] = c
        cells[x * size_y : (x + 1) * size_y, 2 * HALF : 4 * HALF] = -s
    for z in range(0, size_z, 16):
        rows_at = z + lax.broadcasted_iota(jnp.int32, (16, 1), 0)
        for i, x in enumerate(cos_sin(quarters(kz, rows_at, "gz", size_z))):
            high, rest = split(x)
            along[z : z + 16, 2 * HALF * i : 2 * HALF * (i + 1)] = high.astype(jnp.bfloat16)
            along_low[z : z + 16, 2 * HALF * i : 2 * HALF * (i + 1)] = rest.astype(jnp.bfloat16)

    both_loaded = f.at[pl.ds(0, 2), own]
    pltpu.make_async_copy(both_loaded, both_loaded, load_sem).wait()
    load_fuel.start()
    load_late.start()
    flat = lambda i: f[i, own].reshape(rows, size_z)
    high, rest = split(flat(1) / flat(0))
    part = dot_split(jnp.concatenate([high, rest], 1), jnp.concatenate([along[...], along[...]], 0), ((1,), (0,)))
    part = part * cells[...] + dot_split(high, along_low[...], ((1,), (0,))) * cells[...]
    cube = column_sum(part[:, 0 : 2 * HALF] + part[:, 2 * HALF : 4 * HALF])
    own_sum[...] = cube
    got_sums[rank] = cube

    pl.semaphore_wait(barrier, greeters)
    def copy_out(src, dst, recv, place):
        return pltpu.make_async_remote_copy(
            src_ref=src, dst_ref=dst, send_sem=send_sem, recv_sem=recv, device_id=place, device_id_type=MESH)

    def spread(i):
        return copy_out(full_sum, full_sum, sum_recv, place_of(i))

    for r in root_ranks:
        @pl.when(rank != r)
        def _(r=r):
            copy_out(own_sum, got_sums.at[rank], sum_recv, place_of(r)).start()

    for step, lower in zip(z_steps, z_lower):
        @pl.when(lower)
        def _(step=step):
            pl.semaphore_signal(z_ready, inc=1, device_id=shifted("gz", step), device_id_type=MESH)

    both_loaded = measure.at[pl.ds(0, (fuel_hbm.size + late_hbm.size) // 1024)]
    pltpu.make_async_copy(both_loaded, both_loaded, load_sem).wait()
    load_modes.start()
    halos_x = [
        copy_out(f.at[:, pl.ds(size_x, REACH)], f.at[:, pl.ds(0, REACH)], halo_recv, shifted("gx", 1)),
        copy_out(f.at[:, pl.ds(REACH, REACH)], f.at[:, pl.ds(size_x + REACH, REACH)], halo_recv,
                 shifted("gx", -1)),
    ]
    for copy in halos_x:
        copy.start()
    band_at = 16
    pieces = []
    for i in range(2):
        ypack[i, :, 0:REACH] = f[1 + i, own, 0:REACH]
        ypack[i, :, REACH : 2 * REACH] = f[1 + i, own, size_y - REACH : size_y]
        high, rest = split(flat(1 + i))
        pieces += [high, *split(rest)]
    place = lax.broadcasted_iota(jnp.int32, (8, size_z), 0)
    place = jnp.where(place < REACH, place, place + size_z - 2 * REACH)
    edge = (lax.broadcasted_iota(jnp.int32, (8, size_z), 1) == place).astype(jnp.float32)
    ends = dot_split(edge, jnp.concatenate(pieces, 0), ((1,), (1,)))
    for i in range(2):
        zpack[i] = tree_sum([ends[:, (3 * i + j) * rows : (3 * i + j + 1) * rows] for j in range(3)])
    halos_y = [copy_out(ypack, sides.at[i], halo_recv, shifted("gy", step)) for i, step in enumerate(y_steps)]
    halos_z = [copy_out(zpack, ztile.at[i], z_recv, shifted("gz", step)) for i, step in enumerate(z_steps)]
    for copy, lower in zip(halos_z, z_lower):
        @pl.when(lower)
        def _(copy=copy):
            copy.start()
    for copy in halos_y:
        copy.start()

    lap = [dot_nn(flat(1 + i), late[band_at : band_at + size_z]).reshape(size_x, size_y, size_z) for i in range(2)]
    outs = (drate, mrate, hrate)
    mrate[...] = lap[0]
    hrate[...] = lap[1]

    load_modes.wait()
    count = modes.shape[1]
    code = (modes[0:1] * WIDTH + modes[1:2]) * WIDTH + modes[2:3]
    place = lax.rem(lax.broadcasted_iota(jnp.int32, (2 * HALF, 1), 0), HALF)
    px, py, pz = packed_index(place)
    mine = (px * WIDTH + py) * WIDTH + pz
    used = place < len(packed_modes())
    both_ways = jnp.where(used & (mine == code), 1.0, 0.0) + jnp.where(used & (mine == -code), 1.0, 0.0)
    chosen = dot_nt(jnp.ones((8, count), jnp.float32), both_ways)[0:1]

    chosen_out[...] = chosen
    dens_out[...] = f[0, own]
    for i in range(2):
        here = pl.ds(2 * HALF * i, 2 * HALF)
        across[here] = along[:, here].astype(jnp.float32).T.astype(jnp.bfloat16)
        across_low[here] = along_low[:, here].astype(jnp.float32).T.astype(jnp.bfloat16)

    arrived = [f.at[:, pl.ds(0, 2 * REACH)], sides.at[pl.ds(0, sides_used)]]
    higher = sum(jnp.logical_not(lower).astype(jnp.int32) for lower in z_lower)

    @pl.when(higher > 0)
    def _():
        pl.semaphore_wait(z_ready, higher)

    for copy, lower in zip(halos_z, z_lower):
        @pl.when(jnp.logical_not(lower))
        def _(copy=copy):
            copy.start()

    pltpu.make_async_copy(measure, measure, halo_recv).wait()
    for i in range(2):
        edges[i, :, 0:8] = sides[0, i]
        edges[i, :, 8 : 8 + size_y] = f[1 + i, own]
        edges[i, :, 8 + size_y : 16 + size_y] = sides[sides_used - 1, i]
        total_y = outs[1 + i][...]
        for offset, weight in enumerate(SECOND_COEFFS, 1):
            total_y = total_y + weight * (
                edges[i, :, 8 + offset : 8 + offset + size_y] + edges[i, :, 8 - offset : 8 - offset + size_y])
        outs[1 + i][...] = total_y

    def planes(x, offset):
        return x[REACH + offset : REACH + offset + size_x]

    def first_diff(x):
        result = None
        for offset, weight in enumerate(FIRST_COEFFS, 1):
            term = weight * (planes(x, offset) - planes(x, -offset))
            result = term if result is None else result + term
        return result

    def second_diff(x):
        return tree_sum([w * (planes(x, o) + planes(x, -o)) for o, w in enumerate(SECOND_COEFFS, 1)])

    mom = f[1]
    dens = f[0]
    fuel = f[2]
    vel_pad = mom / dens
    drate[...] = -first_diff(mom)
    mid_fuel = planes(fuel, 0)
    hrate[...] = (DIFFUSIVITY * (hrate[...] + second_diff(fuel)) - first_diff(fuel * vel_pad)
                  - mid_fuel * jnp.exp(-ACTIVATION * mid_fuel / planes(dens, 0)))
    mrate[...] = VISCOSITY * (mrate[...] + second_diff(mom)) - first_diff(mom * vel_pad + dens)

    pltpu.make_async_copy(ztile, ztile, z_recv).wait()
    for i, rate in enumerate((VISCOSITY, DIFFUSIVITY)):
        tile = jnp.concatenate([ztile[0, i], ztile[1, i]], 0)
        outs[1 + i][...] = outs[1 + i][...] + rate * dot_tn(tile, late[0:16]).reshape(size_x, size_y, size_z)

    leaves = [i for i in range(total) if i not in root_ranks]

    @pl.when(is_root)
    def _():
        got = got_sums.at[pl.ds(0, total - 1)]
        pltpu.make_async_copy(got, got, sum_recv).wait()

    @pl.when(jnp.logical_not(is_root))
    def _():
        pltpu.make_async_copy(full_sum, full_sum, sum_recv).wait()

    cube = jnp.where(is_root, tree_sum([got_sums[i] for i in range(total)]), full_sum[...])

    @pl.when(rank == root_ranks[-1])
    def _():
        full_sum[...] = cube
        for i in reversed(leaves):
            spread(i).start()

    total_out[...] = cube
    for sent in (arrived[0], arrived[1], ztile.at[:, :]):
        pltpu.make_async_copy(sent, sent, send_sem).wait()
    for r in root_ranks:
        @pl.when(rank != r)
        def _():
            pltpu.make_async_copy(own_sum, own_sum, send_sem).wait()
    if leaves:
        @pl.when(rank == root_ranks[-1])
        def _():
            sent = got_sums.at[pl.ds(0, len(leaves))]
            pltpu.make_async_copy(sent, sent, send_sem).wait()


def finish(ncell, drate, mrate, hrate, dens, cells, across, across_low, chosen, total,
           drate_hbm, mrate_hbm, hrate_hbm, result, sem):
    size_x, size_y, size_z = dens.shape
    rows = size_x * size_y
    early = [pltpu.make_async_copy(drate, drate_hbm, sem), pltpu.make_async_copy(hrate, hrate_hbm, sem)]
    for copy in early:
        copy.start()
    coef = total[...] / ncell
    energy = jnp.sum(chosen[...] * coef * coef, axis=1, keepdims=True)
    scale = 1.0 / (energy + ENERGY_EPS)
    lit = chosen[...] * (2.0 * FORCE_POWER / ncell) * total[...]
    high, rest = split(cells[...] * jnp.concatenate([lit, lit], 1))
    both = dot_split(high, jnp.concatenate([across[...], across_low[...]], 1), ((1,), (0,)))
    weight = dens[...].reshape(rows, size_z) * scale
    low = weight * (both[:, 0:size_z] + both[:, size_z:]) + weight * dot_split(rest, across[...], ((1,), (0,)))
    low = low.reshape(size_x, size_y, size_z)
    for at in range(0, size_x, size_x // 4):
        here = pl.ds(at, size_x // 4)
        result[here] = mrate[here] + low[at : at + size_x // 4]
        pltpu.make_async_copy(result.at[here], mrate_hbm.at[here], sem).start()
    for copy in early:
        copy.wait()
    pltpu.make_async_copy(result, mrate_hbm, sem).wait()


def solution(mesh):
    sizes = {a: mesh.shape[a] for a in ("gx", "gy", "gz")}

    def per_device(density, momentum, hydrogen, forced_modes):
        local = density.shape
        size_x, size_y, size_z = local
        rows = size_x * size_y
        late = tables(size_z)
        modes = forced_modes.T
        total = math.prod(sizes.values())
        halo_bytes = 4 * (3 * 2 * REACH * size_y + (1 + (sizes["gy"] > 2)) * 2 * size_x * 8) * size_z
        any_spec = pl.BlockSpec(memory_space=pl.ANY)
        f32 = jnp.float32
        rates = pl.pallas_call(
            functools.partial(kernel, sizes, local),
            out_shape=[pltpu.VMEM(local, f32)] * 4 + [
                pltpu.VMEM((rows, 4 * HALF), f32),
                pltpu.VMEM((4 * HALF, size_z), jnp.bfloat16),
                pltpu.VMEM((4 * HALF, size_z), jnp.bfloat16),
                pltpu.VMEM((1, 2 * HALF), f32),
                pltpu.VMEM((1, 2 * HALF), f32),
            ],
            in_specs=[any_spec] * 5,
            out_specs=[pl.BlockSpec(memory_space=pltpu.VMEM)] * 9,
            scratch_shapes=[
                pltpu.VMEM((3, size_x + 2 * REACH, size_y, size_z), f32),
                pltpu.VMEM(modes.shape, jnp.int32),
                pltpu.VMEM(late.shape, f32),
                pltpu.VMEM((size_z, 4 * HALF), jnp.bfloat16),
                pltpu.VMEM((size_z, 4 * HALF), jnp.bfloat16),
                pltpu.VMEM((2, size_x, size_y + 16, size_z), f32),
                pltpu.VMEM((2, 2, size_x, 8, size_z), f32),
                pltpu.VMEM((2, size_x, 8, size_z), f32),
                pltpu.VMEM((2, 8, rows), f32),
                pltpu.VMEM((2, 2, 8, rows), f32),
                pltpu.VMEM((1, 2 * HALF), f32),
                pltpu.VMEM((total, 1, 2 * HALF), f32),
                pltpu.VMEM((1, 2 * HALF), f32),
                pltpu.SemaphoreType.DMA,
                pltpu.SemaphoreType.DMA,
                pltpu.SemaphoreType.DMA,
                pltpu.SemaphoreType.DMA,
                pltpu.SemaphoreType.DMA,
                pltpu.SemaphoreType.REGULAR,
                pltpu.VMEM((halo_bytes // 4096, 8, 128), f32),
            ],
            compiler_params=pltpu.CompilerParams(collective_id=0, has_side_effects=True),
            name="flame",
        )(density, momentum, hydrogen, modes, jnp.asarray(late))
        return tuple(pl.pallas_call(
            functools.partial(finish, float(rows * size_z * total)),
            out_shape=[jax.ShapeDtypeStruct(local, f32)] * 3,
            in_specs=[pl.BlockSpec(memory_space=pltpu.VMEM)] * 9,
            out_specs=[any_spec] * 3,
            scratch_shapes=[pltpu.VMEM(local, f32), pltpu.SemaphoreType.DMA],
            name="write",
        )(*[pltpu.with_memory_space_constraint(r, pltpu.VMEM) for r in rates]))

    in_specs = (P("gx", "gy", "gz"), P("gx", "gy", "gz"), P("gx", "gy", "gz"), P())
    out_specs = (P("gx", "gy", "gz"), P("gx", "gy", "gz"), P("gx", "gy", "gz"))
    return jax.shard_map(
        per_device, mesh=mesh, in_specs=in_specs, out_specs=out_specs, check_vma=False
    )
```

```python
import functools
import math

import jax
import jax.numpy as jnp
import numpy as np
from jax import lax
from jax.experimental import pallas as pl
from jax.experimental.pallas import tpu as pltpu
from jax.sharding import PartitionSpec as P

KMAX = 3
WIDTH = 2 * KMAX + 1
HALF = 64
ROWS = KMAX + 1
REACH = 4
LOAD_PLANES = 4

FIRST_COEFFS = (0.8, -0.2, 4.0 / 105.0, -1.0 / 280.0)
SECOND_COEFFS = (1.6, -0.2, 8.0 / 315.0, -1.0 / 560.0)
CENTRE_COEFF = -205.0 / 72.0
VISCOSITY = 0.3
DIFFUSIVITY = 1.5
FORCE_POWER = 0.3
ENERGY_EPS = 1e-06
ACTIVATION = 2.0
HIGHEST = lax.Precision.HIGHEST
MESH = pl.DeviceIdType.MESH


def packed_modes():
    reach = range(-KMAX, KMAX + 1)
    cells = [(x, y, z) for z in range(ROWS) for x in reach for y in reach
             if x * x + y * y + z * z <= KMAX * KMAX and (z, x, y) > (0, 0, 0)]
    return cells


def packed_index(place):
    cells = packed_modes()
    result = []
    for part in range(3):
        value = jnp.full(place.shape, cells[0][part], jnp.int32)
        if part == 1:
            value = value + place
        for i in range(1, len(cells)):
            step = cells[i][part] - cells[i - 1][part] - (part == 1)
            if step:
                value = value + jnp.where(place >= i, step, 0)
        result.append(value)
    return result


def tables(size_z):
    band = np.zeros((size_z, size_z))
    halo = np.zeros((16, size_z))
    for z in range(size_z):
        band[z, z] = 3.0 * CENTRE_COEFF
        for offset, weight in enumerate(SECOND_COEFFS, 1):
            for q in (z - offset, z + offset):
                if 0 <= q < size_z:
                    band[q, z] = weight
                elif q < 0:
                    halo[8 + q, z] = weight
                else:
                    halo[8 + q - size_z, z] = weight
    return np.concatenate([halo, band], 0).astype(np.float32)


def polynomial(x, coeffs):
    result = coeffs[-1]
    for c in reversed(coeffs[:-1]):
        result = result * x + c
    return result


SIN_COEFFS = [(-1) ** n * (math.pi / 2) ** (2 * n + 1) / math.factorial(2 * n + 1) for n in range(5)]
COS_COEFFS = [(-1) ** n * (math.pi / 2) ** (2 * n) / math.factorial(2 * n) for n in range(6)]


def cos_sin(quarters):
    turns = jnp.floor(quarters + 0.5)
    d = quarters - turns
    square = d * d
    s = d * polynomial(square, SIN_COEFFS)
    c = polynomial(square, COS_COEFFS)
    half = jnp.floor(0.5 * turns)
    odd = turns - 2.0 * half
    turned = half - 2.0 * jnp.floor(0.5 * half)
    sin_sign = 1.0 - 2.0 * turned
    cos_sign = sin_sign - 2.0 * odd * sin_sign
    swap = odd > 0.5
    return jnp.where(swap, s, c) * cos_sign, jnp.where(swap, c, s) * sin_sign


def split(x):
    high = x.astype(jnp.bfloat16).astype(jnp.float32)
    return high, x - high


def dot_split(a, b, contract):
    return lax.dot_general(a.astype(jnp.bfloat16), b.astype(jnp.bfloat16), (contract, ((), ())),
                           preferred_element_type=jnp.float32)


def column_sum(x):
    x = tree_sum([x[i : i + 8] for i in range(0, x.shape[0], 8)])
    return jnp.sum(x, axis=0, keepdims=True)


def dot_nt(a, b):
    return lax.dot_general(a, b, (((1,), (1,)), ((), ())), precision=HIGHEST, preferred_element_type=jnp.float32)


def dot_nn(a, b):
    return lax.dot_general(a, b, (((1,), (0,)), ((), ())), precision=HIGHEST, preferred_element_type=jnp.float32)


def dot_tn(a, b):
    return lax.dot_general(a, b, (((0,), (0,)), ((), ())), precision=HIGHEST, preferred_element_type=jnp.float32)


def tree_sum(parts):
    parts = list(parts)
    while len(parts) > 1:
        parts = [sum(parts[i : i + 2][1:], parts[i]) for i in range(0, len(parts), 2)]
    return parts[0]


def root_places(sizes):
    places = [(0, 0), (1, 0), (1, max(0, sizes["gz"] // 2 - 1))]
    return [{"gx": x, "gy": 0, "gz": z} for i, (x, z) in enumerate(places) if (x, z) not in places[:i]]


def kernel(sizes, local, dens_hbm, mom_hbm, fuel_hbm, modes_hbm, late_hbm,
           drate, mrate, hrate, dens_out, cells, across, across_low, chosen_out, total_out,
           f, modes, late, along, along_low, edges, sides, ypack, zpack, ztile, own_sum, got_sums, full_sum,
           load_sem, send_sem, halo_recv, sum_recv, z_ready, measure):
    size_x, size_y, size_z = local
    rows = size_x * size_y
    me = {a: lax.axis_index(a) for a in sizes}
    count_x, count_y, count_z = sizes["gx"], sizes["gy"], sizes["gz"]
    total = count_x * count_y * count_z
    roots = root_places(sizes)
    rank_of = lambda p: (p["gz"] * count_x + p["gx"]) * count_y + p["gy"]
    rank = rank_of(me)
    root_ranks = [rank_of(r) for r in roots]
    is_root = functools.reduce(jnp.logical_or, [rank == r for r in root_ranks])

    def place_of(i):
        if isinstance(i, int):
            x, y, z = i // count_y % count_x, i % count_y, i // (count_x * count_y)
            return {"gx": jnp.int32(x), "gy": jnp.int32(y), "gz": jnp.int32(z)}
        return {"gx": lax.rem(lax.div(i, count_y), count_x), "gy": lax.rem(i, count_y),
                "gz": lax.div(i, count_x * count_y)}

    def shifted(axis, step):
        return {axis: lax.rem(me[axis] + step % sizes[axis], sizes[axis])}

    own = pl.ds(REACH, size_x)
    load_late = pltpu.make_async_copy(late_hbm, late, load_sem)
    for at in range(0, size_x, LOAD_PLANES):
        for i, src in enumerate((dens_hbm, mom_hbm)):
            pltpu.make_async_copy(
                src.at[pl.ds(at, LOAD_PLANES)], f.at[i, pl.ds(REACH + at, LOAD_PLANES)], load_sem).start()
    load_fuel = pltpu.make_async_copy(fuel_hbm, f.at[2, own], load_sem)
    load_modes = pltpu.make_async_copy(modes_hbm, modes, load_sem)

    barrier = pltpu.get_barrier_semaphore()
    z_steps = (1, -1)
    z_next = [shifted("gz", step)["gz"] for step in z_steps]
    z_lower = [z < me["gz"] for z in z_next]
    y_steps = (1, -1) if count_y > 2 else (1,)
    sides_used = len(y_steps)

    def greet(place):
        pl.semaphore_signal(barrier, inc=1, device_id=place, device_id_type=MESH)

    for step in (1, -1):
        greet(shifted("gx", step))
    for step in y_steps:
        greet(shifted("gy", step))
    for step, lower in zip(z_steps, z_lower):
        @pl.when(jnp.logical_not(lower))
        def _(step=step):
            greet(shifted("gz", step))

    @pl.when(is_root)
    def _():
        def greet_one(i, carry):
            @pl.when(i != rank)
            def _():
                greet(place_of(i))
            return carry
        lax.fori_loop(0, total, greet_one, 0)

    greeters = 2 + sides_used + len(roots) - is_root.astype(jnp.int32)
    for lower in z_lower:
        greeters = greeters + lower.astype(jnp.int32)

    lane = lax.broadcasted_iota(jnp.int32, (1, 2 * HALF), 1)
    kx, ky, kz = packed_index(lax.rem(lane, HALF))
    quarter = (lane >= HALF).astype(jnp.float32)
    kx, ky, kz = [k.astype(jnp.float32) for k in (kx, ky, kz)]

    def quarters(k, place, axis, size):
        part = k * place.astype(jnp.float32) / (size * sizes[axis])
        return 4.0 * (part - jnp.floor(part))

    shift = quarters(kz, me["gz"] * size_z, "gz", size_z) - quarter
    rows_y = me["gy"] * size_y + lax.broadcasted_iota(jnp.int32, (size_y, 1), 0)
    angle_y = quarters(ky, rows_y, "gy", size_y) + shift
    for x in range(size_x):
        c, s = cos_sin(angle_y + quarters(kx, me["gx"] * size_x + x, "gx", size_x))
        cells[x * size_y : (x + 1) * size_y, 0 : 2 * HALF] = c
        cells[x * size_y : (x + 1) * size_y, 2 * HALF : 4 * HALF] = -s
    for z in range(0, size_z, 16):
        rows_at = z + lax.broadcasted_iota(jnp.int32, (16, 1), 0)
        for i, x in enumerate(cos_sin(quarters(kz, rows_at, "gz", size_z))):
            high, rest = split(x)
            along[z : z + 16, 2 * HALF * i : 2 * HALF * (i + 1)] = high.astype(jnp.bfloat16)
            along_low[z : z + 16, 2 * HALF * i : 2 * HALF * (i + 1)] = rest.astype(jnp.bfloat16)

    both_loaded = f.at[pl.ds(0, 2), own]
    pltpu.make_async_copy(both_loaded, both_loaded, load_sem).wait()
    load_fuel.start()
    load_late.start()
    flat = lambda i: f[i, own].reshape(rows, size_z)
    high, rest = split(flat(1) / flat(0))
    part = dot_split(jnp.concatenate([high, rest], 1), jnp.concatenate([along[...], along[...]], 0), ((1,), (0,)))
    part = part * cells[...] + dot_split(high, along_low[...], ((1,), (0,))) * cells[...]
    cube = column_sum(part[:, 0 : 2 * HALF] + part[:, 2 * HALF : 4 * HALF])
    own_sum[...] = cube
    got_sums[rank] = cube

    pl.semaphore_wait(barrier, greeters)
    def copy_out(src, dst, recv, place):
        return pltpu.make_async_remote_copy(
            src_ref=src, dst_ref=dst, send_sem=send_sem, recv_sem=recv, device_id=place, device_id_type=MESH)

    def spread(i):
        return copy_out(full_sum, full_sum, sum_recv, place_of(i))

    for r in root_ranks:
        @pl.when(rank != r)
        def _(r=r):
            copy_out(own_sum, got_sums.at[rank], sum_recv, place_of(r)).start()

    for step, lower in zip(z_steps, z_lower):
        @pl.when(lower)
        def _(step=step):
            pl.semaphore_signal(z_ready, inc=1, device_id=shifted("gz", step), device_id_type=MESH)

    both_loaded = measure.at[pl.ds(0, (fuel_hbm.size + late_hbm.size) // 1024)]
    pltpu.make_async_copy(both_loaded, both_loaded, load_sem).wait()
    load_modes.start()
    halos_x = [
        copy_out(f.at[:, pl.ds(size_x, REACH)], f.at[:, pl.ds(0, REACH)], halo_recv, shifted("gx", 1)),
        copy_out(f.at[:, pl.ds(REACH, REACH)], f.at[:, pl.ds(size_x + REACH, REACH)], halo_recv,
                 shifted("gx", -1)),
    ]
    for copy in halos_x:
        copy.start()
    band_at = 16
    pieces = []
    for i in range(2):
        ypack[i, :, 0:REACH] = f[1 + i, own, 0:REACH]
        ypack[i, :, REACH : 2 * REACH] = f[1 + i, own, size_y - REACH : size_y]
        high, rest = split(flat(1 + i))
        pieces += [high, *split(rest)]
    place = lax.broadcasted_iota(jnp.int32, (8, size_z), 0)
    place = jnp.where(place < REACH, place, place + size_z - 2 * REACH)
    edge = (lax.broadcasted_iota(jnp.int32, (8, size_z), 1) == place).astype(jnp.float32)
    ends = dot_split(edge, jnp.concatenate(pieces, 0), ((1,), (1,)))
    for i in range(2):
        zpack[i] = tree_sum([ends[:, (3 * i + j) * rows : (3 * i + j + 1) * rows] for j in range(3)])
    halos_y = [copy_out(ypack, sides.at[i], halo_recv, shifted("gy", step)) for i, step in enumerate(y_steps)]
    halos_z = [copy_out(zpack, ztile.at[i], halo_recv, shifted("gz", step)) for i, step in enumerate(z_steps)]
    for copy, lower in zip(halos_z, z_lower):
        @pl.when(lower)
        def _(copy=copy):
            copy.start()
    for copy in halos_y:
        copy.start()

    lap = [dot_nn(flat(1 + i), late[band_at : band_at + size_z]).reshape(size_x, size_y, size_z) for i in range(2)]
    outs = (drate, mrate, hrate)
    mrate[...] = lap[0]
    hrate[...] = lap[1]

    load_modes.wait()
    count = modes.shape[1]
    code = (modes[0:1] * WIDTH + modes[1:2]) * WIDTH + modes[2:3]
    place = lax.rem(lax.broadcasted_iota(jnp.int32, (2 * HALF, 1), 0), HALF)
    px, py, pz = packed_index(place)
    mine = (px * WIDTH + py) * WIDTH + pz
    used = place < len(packed_modes())
    both_ways = jnp.where(used & (mine == code), 1.0, 0.0) + jnp.where(used & (mine == -code), 1.0, 0.0)
    chosen = dot_nt(jnp.ones((8, count), jnp.float32), both_ways)[0:1]

    chosen_out[...] = chosen
    dens_out[...] = f[0, own]
    for i in range(2):
        here = pl.ds(2 * HALF * i, 2 * HALF)
        across[here] = along[:, here].astype(jnp.float32).T.astype(jnp.bfloat16)
        across_low[here] = along_low[:, here].astype(jnp.float32).T.astype(jnp.bfloat16)

    arrived = [f.at[:, pl.ds(0, 2 * REACH)], sides.at[pl.ds(0, sides_used)]]
    higher = sum(jnp.logical_not(lower).astype(jnp.int32) for lower in z_lower)

    @pl.when(higher > 0)
    def _():
        pl.semaphore_wait(z_ready, higher)

    for copy, lower in zip(halos_z, z_lower):
        @pl.when(jnp.logical_not(lower))
        def _(copy=copy):
            copy.start()

    pltpu.make_async_copy(measure, measure, halo_recv).wait()
    for i in range(2):
        edges[i, :, 0:8] = sides[0, i]
        edges[i, :, 8 : 8 + size_y] = f[1 + i, own]
        edges[i, :, 8 + size_y : 16 + size_y] = sides[sides_used - 1, i]
        total_y = outs[1 + i][...]
        for offset, weight in enumerate(SECOND_COEFFS, 1):
            total_y = total_y + weight * (
                edges[i, :, 8 + offset : 8 + offset + size_y] + edges[i, :, 8 - offset : 8 - offset + size_y])
        outs[1 + i][...] = total_y

    def planes(x, offset):
        return x[REACH + offset : REACH + offset + size_x]

    def first_diff(x):
        result = None
        for offset, weight in enumerate(FIRST_COEFFS, 1):
            term = weight * (planes(x, offset) - planes(x, -offset))
            result = term if result is None else result + term
        return result

    def second_diff(x):
        return tree_sum([w * (planes(x, o) + planes(x, -o)) for o, w in enumerate(SECOND_COEFFS, 1)])

    mom = f[1]
    dens = f[0]
    fuel = f[2]
    vel_pad = mom / dens
    drate[...] = -first_diff(mom)
    mid_fuel = planes(fuel, 0)
    hrate[...] = (DIFFUSIVITY * (hrate[...] + second_diff(fuel)) - first_diff(fuel * vel_pad)
                  - mid_fuel * jnp.exp(-ACTIVATION * mid_fuel / planes(dens, 0)))
    mrate[...] = VISCOSITY * (mrate[...] + second_diff(mom)) - first_diff(mom * vel_pad + dens)

    for i, rate in enumerate((VISCOSITY, DIFFUSIVITY)):
        tile = jnp.concatenate([ztile[0, i], ztile[1, i]], 0)
        outs[1 + i][...] = outs[1 + i][...] + rate * dot_tn(tile, late[0:16]).reshape(size_x, size_y, size_z)

    leaves = [i for i in range(total) if i not in root_ranks]

    @pl.when(is_root)
    def _():
        got = got_sums.at[pl.ds(0, total - 1)]
        pltpu.make_async_copy(got, got, sum_recv).wait()

    @pl.when(jnp.logical_not(is_root))
    def _():
        pltpu.make_async_copy(full_sum, full_sum, sum_recv).wait()

    cube = jnp.where(is_root, tree_sum([got_sums[i] for i in range(total)]), full_sum[...])

    @pl.when(rank == root_ranks[-1])
    def _():
        full_sum[...] = cube
        for i in reversed(leaves):
            spread(i).start()

    total_out[...] = cube
    for sent in (arrived[0], arrived[1], ztile.at[:, :]):
        pltpu.make_async_copy(sent, sent, send_sem).wait()
    for r in root_ranks:
        @pl.when(rank != r)
        def _():
            pltpu.make_async_copy(own_sum, own_sum, send_sem).wait()
    if leaves:
        @pl.when(rank == root_ranks[-1])
        def _():
            sent = got_sums.at[pl.ds(0, len(leaves))]
            pltpu.make_async_copy(sent, sent, send_sem).wait()


def finish(ncell, drate, mrate, hrate, dens, cells, across, across_low, chosen, total,
           drate_hbm, mrate_hbm, hrate_hbm, result, sem):
    size_x, size_y, size_z = dens.shape
    rows = size_x * size_y
    early = [pltpu.make_async_copy(drate, drate_hbm, sem), pltpu.make_async_copy(hrate, hrate_hbm, sem)]
    for copy in early:
        copy.start()
    coef = total[...] / ncell
    energy = jnp.sum(chosen[...] * coef * coef, axis=1, keepdims=True)
    scale = 1.0 / (energy + ENERGY_EPS)
    lit = chosen[...] * (2.0 * FORCE_POWER / ncell) * total[...]
    high, rest = split(cells[...] * jnp.concatenate([lit, lit], 1))
    both = dot_split(high, jnp.concatenate([across[...], across_low[...]], 1), ((1,), (0,)))
    weight = dens[...].reshape(rows, size_z) * scale
    low = weight * (both[:, 0:size_z] + both[:, size_z:]) + weight * dot_split(rest, across[...], ((1,), (0,)))
    low = low.reshape(size_x, size_y, size_z)
    for at in range(0, size_x, size_x // 4):
        here = pl.ds(at, size_x // 4)
        result[here] = mrate[here] + low[at : at + size_x // 4]
        pltpu.make_async_copy(result.at[here], mrate_hbm.at[here], sem).start()
    for copy in early:
        copy.wait()
    pltpu.make_async_copy(result, mrate_hbm, sem).wait()


def solution(mesh):
    sizes = {a: mesh.shape[a] for a in ("gx", "gy", "gz")}

    def per_device(density, momentum, hydrogen, forced_modes):
        local = density.shape
        size_x, size_y, size_z = local
        rows = size_x * size_y
        late = tables(size_z)
        modes = forced_modes.T
        total = math.prod(sizes.values())
        halo_bytes = 4 * (3 * 2 * REACH * size_y + (1 + (sizes["gy"] > 2)) * 2 * size_x * 8) * size_z + 4 * 2 * 2 * 8 * rows
        any_spec = pl.BlockSpec(memory_space=pl.ANY)
        f32 = jnp.float32
        rates = pl.pallas_call(
            functools.partial(kernel, sizes, local),
            out_shape=[pltpu.VMEM(local, f32)] * 4 + [
                pltpu.VMEM((rows, 4 * HALF), f32),
                pltpu.VMEM((4 * HALF, size_z), jnp.bfloat16),
                pltpu.VMEM((4 * HALF, size_z), jnp.bfloat16),
                pltpu.VMEM((1, 2 * HALF), f32),
                pltpu.VMEM((1, 2 * HALF), f32),
            ],
            in_specs=[any_spec] * 5,
            out_specs=[pl.BlockSpec(memory_space=pltpu.VMEM)] * 9,
            scratch_shapes=[
                pltpu.VMEM((3, size_x + 2 * REACH, size_y, size_z), f32),
                pltpu.VMEM(modes.shape, jnp.int32),
                pltpu.VMEM(late.shape, f32),
                pltpu.VMEM((size_z, 4 * HALF), jnp.bfloat16),
                pltpu.VMEM((size_z, 4 * HALF), jnp.bfloat16),
                pltpu.VMEM((2, size_x, size_y + 16, size_z), f32),
                pltpu.VMEM((2, 2, size_x, 8, size_z), f32),
                pltpu.VMEM((2, size_x, 8, size_z), f32),
                pltpu.VMEM((2, 8, rows), f32),
                pltpu.VMEM((2, 2, 8, rows), f32),
                pltpu.VMEM((1, 2 * HALF), f32),
                pltpu.VMEM((total, 1, 2 * HALF), f32),
                pltpu.VMEM((1, 2 * HALF), f32),
                pltpu.SemaphoreType.DMA,
                pltpu.SemaphoreType.DMA,
                pltpu.SemaphoreType.DMA,
                pltpu.SemaphoreType.DMA,
                pltpu.SemaphoreType.REGULAR,
                pltpu.VMEM((halo_bytes // 4096, 8, 128), f32),
            ],
            compiler_params=pltpu.CompilerParams(collective_id=0, has_side_effects=True),
            name="flame",
        )(density, momentum, hydrogen, modes, jnp.asarray(late))
        return tuple(pl.pallas_call(
            functools.partial(finish, float(rows * size_z * total)),
            out_shape=[jax.ShapeDtypeStruct(local, f32)] * 3,
            in_specs=[pl.BlockSpec(memory_space=pltpu.VMEM)] * 9,
            out_specs=[any_spec] * 3,
            scratch_shapes=[pltpu.VMEM(local, f32), pltpu.SemaphoreType.DMA],
            name="write",
        )(*[pltpu.with_memory_space_constraint(r, pltpu.VMEM) for r in rates]))

    in_specs = (P("gx", "gy", "gz"), P("gx", "gy", "gz"), P("gx", "gy", "gz"), P())
    out_specs = (P("gx", "gy", "gz"), P("gx", "gy", "gz"), P("gx", "gy", "gz"))
    return jax.shard_map(
        per_device, mesh=mesh, in_specs=in_specs, out_specs=out_specs, check_vma=False
    )
```
